32 devices in a mesh: gx: 2 (over core), gy: 4 (over y, x), gz: 4 (over z).
Axes of the slice: x: 2, y: 2, z: 4, core: 2. Of those that a mesh axis runs over, the one named last changes fastest.
Arguments:
- right_side: float32 [3, 32, 64, 512], P(None, 'gx', 'gy', 'gz'), may hold values from -64 to 64
- damage: int32 [32, 64, 512], P('gx', 'gy', 'gz'), may hold values from 0 to 15
Outputs:
- displacement: float32 [3, 32, 64, 512], P(None, 'gx', 'gy', 'gz')
- norms: float32 [2], replicated
The draws below stay inside these ranges and needn't reach their ends.
All inputs are finite; a program needn't handle non-finite values.
Results may differ from the reference program's by a relative error of at most 0.0003.
Values sent between devices are 32-bit elements; how exact they have to be, the bound alone decides.
A program may use at most 64 MiB of HBM per device.

```python
import math
import jax
import jax.numpy as jnp
from jax import lax

BLOCK = 16
COARSE = 8
NX = 32
NY = 64
NZ = 512


def draw_right_side(key, part):
    key_noise = jax.random.fold_in(key, 11)
    key_rows = jax.random.fold_in(key, 12)
    key_cols = jax.random.fold_in(key, 13)
    ramp = 1.0 + 2.0 * jnp.arange(NX, dtype=jnp.float32) / NX
    rough_rows = jnp.exp(jax.random.uniform(key_rows, (NX,), jnp.float32, 0.0, math.log(3.0)))
    rough_cols = jnp.exp(jax.random.uniform(key_cols, (NY,), jnp.float32, 0.0, math.log(3.0)))
    scale = (ramp * rough_rows)[:, None, None] * rough_cols[None, :, None]
    noise = jnp.clip(jax.random.normal(key_noise, (3, NX, NY, NZ), jnp.float32), -6.0, 6.0)
    return jnp.clip(noise * scale, -64.0, 64.0)


def place_ends(drawn, key, low, high):
    dims = drawn.shape
    index_at = [jax.random.randint(jax.random.fold_in(key, axis), (), 0, dims[axis]) for axis in range(len(dims))]
    drawn = drawn.at[tuple(index_at)].set(low)
    longest = dims.index(max(dims))
    index_at[longest] = (index_at[longest] + 1) % dims[longest]
    return drawn.at[tuple(index_at)].set(high)


def setup_inputs(seed: int = 0) -> dict:
    splits = jax.random.split(jax.random.key(seed), 3)
    return {
        "right_side": draw_right_side(jax.random.fold_in(splits[2], 71), 0),
        "damage": place_ends(jax.random.randint(splits[1], (NX, NY, NZ), 0, 16), jax.random.fold_in(splits[1], 1), 0, 15).astype(jnp.int32),
    }


FLOOR_STIFFNESS = 0.05
MASS_TERM = 0.001
COUPLING = 2.5
RELAXATION = 0.6

def stiffness_of(damage):
    damage_level = damage.astype(jnp.float32) / 15.0
    return (1.0 - damage_level) ** 2 * (1.0 - FLOOR_STIFFNESS) + FLOOR_STIFFNESS

def diagonal_of(coefficient, mass_term):
    return coefficient * (6.0 + 2.0 * COUPLING) + mass_term

def stencil(padded, coefficient, mass_term):
    extent = (padded.shape[1] - 2, padded.shape[2] - 2, padded.shape[3] - 2)

    def neighbour(component, offset):
        return padded[component, 1 + offset[0]:1 + offset[0] + extent[0], 1 + offset[1]:1 + offset[1] + extent[1], 1 + offset[2]:1 + offset[2] + extent[2]]

    def joined(first, second, factor):
        return tuple((first[number] + factor * second[number] for number in range(3)))
    unit_steps = ((1, 0, 0), (0, 1, 0), (0, 0, 1))
    images = []
    for component in range(3):
        centre = neighbour(component, (0, 0, 0))
        beside_all = jnp.zeros_like(centre)
        for partner in range(3):
            step_up = unit_steps[partner]
            step_down = joined((0, 0, 0), step_up, -1)
            beside_all = beside_all + neighbour(component, step_up) + neighbour(component, step_down)
        own_up = unit_steps[component]
        own_down = joined((0, 0, 0), own_up, -1)
        axial_part = 2.0 * centre - neighbour(component, own_up) - neighbour(component, own_down)
        mixed_part = jnp.zeros_like(centre)
        for partner in range(3):
            if partner != component:
                other_up = unit_steps[partner]
                mixed_part = mixed_part + neighbour(partner, joined(own_up, other_up, 1)) - neighbour(partner, joined(own_up, other_up, -1)) - neighbour(partner, joined(own_down, other_up, 1)) + neighbour(partner, joined(own_down, other_up, -1))
        images.append(coefficient * (6.0 * centre - beside_all + COUPLING * (axial_part - 0.25 * mixed_part)) + mass_term * centre)
    return jnp.stack(images)

def apply_whole(displacement, coefficient):
    padded = jnp.pad(displacement, ((0, 0), (1, 1), (1, 1), (1, 1)))
    block_count = displacement.shape[1] // BLOCK

    def one_block(block_no):
        start = (block_no * BLOCK).astype(jnp.int32)
        slab_piece = lax.dynamic_slice_in_dim(padded, start, BLOCK + 2, 1)
        slab_stiff = lax.dynamic_slice_in_dim(coefficient, start, BLOCK, 0)
        return stencil(slab_piece, slab_stiff, MASS_TERM)
    blocks_out = lax.map(one_block, jnp.arange(block_count, dtype=jnp.int32))
    return jnp.moveaxis(blocks_out, 0, 1).reshape(displacement.shape)

def block_sums(source):
    channels, size_x, size_y, size_z = source.shape
    return lax.optimization_barrier(jnp.sum(source.reshape(channels, size_x // BLOCK, BLOCK, size_y // BLOCK, BLOCK, size_z // BLOCK, BLOCK), axis=(2, 4, 6)))

def spread(block_field):
    channels, size_x, size_y, size_z = block_field.shape
    widened = jnp.broadcast_to(block_field[:, :, None, :, None, :, None], (channels, size_x, BLOCK, size_y, BLOCK, size_z, BLOCK))
    return widened.reshape(channels, size_x * BLOCK, size_y * BLOCK, size_z * BLOCK)

def coarse_sweeps(coarse_load, mean_stiffness):
    coarse_coefficient = BLOCK ** 2 * mean_stiffness
    coarse_mass = BLOCK ** 3 * MASS_TERM
    coarse_diagonal = diagonal_of(coarse_coefficient, coarse_mass)
    correction = RELAXATION * coarse_load / coarse_diagonal
    for repeat in range(COARSE - 1):
        padded = jnp.pad(correction, ((0, 0), (1, 1), (1, 1), (1, 1)))
        coarse_image = stencil(padded, coarse_coefficient, coarse_mass)
        correction = correction + RELAXATION * (coarse_load - coarse_image) / coarse_diagonal
    return correction

def reference(right_side, damage):
    coefficient = stiffness_of(damage)
    diagonal = diagonal_of(coefficient, MASS_TERM)
    displacement = RELAXATION * right_side / diagonal
    displacement = displacement + RELAXATION * (right_side - apply_whole(displacement, coefficient)) / diagonal
    residual = right_side - apply_whole(displacement, coefficient)
    coarse_load = block_sums(residual)
    mean_stiffness = (block_sums(coefficient[None]) / BLOCK ** 3)[0]
    correction = coarse_sweeps(coarse_load, mean_stiffness)
    displacement = displacement + spread(correction)
    for repeat in range(2):
        displacement = displacement + RELAXATION * (right_side - apply_whole(displacement, coefficient)) / diagonal
    residual = right_side - apply_whole(displacement, coefficient)
    total_count = 3 * NX * NY * NZ
    load_sum = jnp.sum(right_side * right_side)
    residual_sum = jnp.sum(residual * residual)
    norms = jnp.stack([jnp.sqrt(load_sum / total_count), jnp.sqrt(residual_sum / total_count)])
    return (displacement, norms)
```

```python
import functools

import jax
import jax.numpy as jnp
from jax import lax
from jax.experimental import pallas as pl
from jax.experimental.pallas import tpu as pltpu
from jax.sharding import PartitionSpec as P

BLOCK = 16
COARSE = 8
FLOOR_STIFFNESS = 0.05
MASS_TERM = 0.001
COUPLING = 2.5
RELAXATION = 0.6
DIAGONAL = 6.0 + 2.0 * COUPLING
OWN = 1.0 + COUPLING
CROSS = 0.25 * COUPLING
AXES = ("gx", "gy", "gz")
HALO = 4
LANES = 128
MESH = pl.DeviceIdType.MESH
EXACT = lax.Precision.HIGHEST


def messages():
    out = []
    for dx in (-1, 1):
        for part in range(HALO):
            out.append(("x", dx, 0, 0, part))
    for part in range(2):
        for dy in (-1, 1):
            out.append(("y", 0, dy, 0, part))
        for dx in (-1, 1):
            for dy in (-1, 1):
                if part == 1:
                    out.append(("xy", dx, dy, 0, part))
                out.append(("xyn", dx, dy, 0, part))
        if part == 0:
            for dz in (-1, 1):
                for dx in (-1, 0, 1):
                    for dy in (-1, 0, 1):
                        out.append(("z" if dx == 0 else "xz", dx, dy, dz, 0))
    return out


MESSAGES = messages()


def by_two(low, high, body, carry):
    pairs = (high - low) // 2

    def both(trip, carry):
        carry = body(low + 2 * trip, carry)
        return body(low + 2 * trip + 1, carry)

    carry = lax.fori_loop(0, pairs, both, carry)
    return body(high - 1, carry) if (high - low) % 2 else carry


def kernel(
    counts,
    extent,
    load_ref,
    damage_ref,
    out_ref,
    norms_ref,
    base,
    inverse,
    field_a,
    field_b,
    harm,
    y_send,
    y_recv,
    xy_send,
    xy_recv,
    xyn_send,
    xyn_recv,
    yz_send,
    yz_recv,
    xyz_send,
    xyz_recv,
    z_send,
    z_recv,
    xz_send,
    xz_recv,
    coarse_send,
    coarse_recv,
    coarse_w,
    spread_w,
    image_w,
    norm_send,
    norm_recv,
    local_sem,
    send_sem,
    recv_sem,
    coarse_send_sem,
    coarse_recv_sem,
    norm_send_sem,
    norm_recv_sem,
    hello_sem,
):
    count_x, count_y, count_z = counts
    ex, ey, ez = extent
    cz = ez // BLOCK
    total = count_x * count_y * count_z
    wide_x = ex + 2 * HALO
    ypad = 8
    rows = ey + 2 * ypad
    wide_y = ey + 2 * HALO
    first_y = ypad - HALO
    me = tuple(lax.axis_index(axis) for axis in AXES)
    my_id = (me[0] * count_y + me[1]) * count_z + me[2]

    def place(index):
        return (
            index // (count_y * count_z),
            lax.rem(index // count_z, count_y),
            lax.rem(index, count_z),
        )

    load_copies = []
    for x in range(ex):
        target = pl.ds((HALO + x) * rows + ypad, ey)
        load_copies.append(
            pltpu.make_async_copy(load_ref.at[:, x], base.at[0, 0:3, target], local_sem.at[x])
        )
    harm_copy = pltpu.make_async_copy(damage_ref, harm, local_sem.at[ex])
    harm_copy.start()
    for copy in load_copies:
        copy.start()

    barrier = pltpu.get_barrier_semaphore()

    reach = -(-COARSE // cz)
    window = 2 * reach + 1

    def peers(act):
        for dz in range(-reach, reach + 1):
            z = me[2] + dz

            @pl.when((z >= 0) & (z < count_z))
            def _():
                def one(step, carry):
                    if dz == 0:
                        step = step + 1
                    index = lax.rem(me[0] * count_y + me[1] + step, count_x * count_y)
                    act(index // count_y, lax.rem(index, count_y), z, dz)
                    return carry

                lax.fori_loop(0, count_x * count_y - (1 if dz == 0 else 0), one, 0)

    def greet(x, y, z, dz):
        pl.semaphore_signal(barrier, inc=1, device_id=(x, y, z), device_id_type=MESH)

    peers(greet)
    levels = jnp.minimum(me[2] + reach, count_z - 1) - jnp.maximum(me[2] - reach, 0) + 1

    harm_copy.wait()
    for x in range(ex):
        level = 1.0 - harm[x].astype(jnp.float32) / 15.0
        base[0, 3, pl.ds((HALO + x) * rows + ypad, ey)] = (
            level * level * (1.0 - FLOOR_STIFFNESS) + FLOOR_STIFFNESS
        )
    for copy in load_copies:
        copy.wait()

    lane = lax.broadcasted_iota(jnp.int32, (ey, LANES), 1)
    for side in range(2):
        for part in range(2):
            for layer in range(2):
                y = 2 * part + layer if side == 0 else ey - 2 - 2 * part + layer
                for f in range(4):
                    start = HALO * rows + ypad + y
                    for half in range(ex // 8):
                        y_send[side, part, f, layer, pl.ds(8 * half, 8)] = base[
                            0, f, pl.ds(start + 8 * half * rows, 8, stride=rows)
                        ]
                    for xs in range(2):
                        x0 = 0 if xs == 0 else ex - HALO
                        if part == 1:
                            xy_send[xs, side, f, layer] = base[
                                0, f, pl.ds(start + x0 * rows, HALO, stride=rows)
                            ]
                            continue
                        for which in range(2):
                            x0 = 2 * which if xs == 0 else ex - 2 - 2 * which
                            xyn_send[xs, side, which, f, layer] = base[
                                0, f, pl.ds(start + x0 * rows, 2, stride=rows)
                            ]
    for f in range(4):
        packed = None
        for k in range(ex):
            row = base[0, f, pl.ds((HALO + k) * rows + ypad, ey)]
            moved = pltpu.roll(row, (8 * k + HALO) % LANES, 1)
            packed = moved if packed is None else jnp.where(lane // 8 == k, moved, packed)
        z_send[f] = packed
        yz_send[0, f] = packed[:HALO]
        yz_send[1, f] = packed[ey - HALO :]
    for xs in range(2):
        packed = None
        for f in range(4):
            for j in range(HALO):
                x = j if xs == 0 else ex - HALO + j
                k = f * HALO + j
                row = base[0, f, pl.ds((HALO + x) * rows + ypad, ey)]
                moved = pltpu.roll(row, (8 * k + HALO) % LANES, 1)
                packed = moved if packed is None else jnp.where(lane // 8 == k, moved, packed)
        xz_send[xs] = packed
        xyz_send[xs, 0] = packed[:HALO]
        xyz_send[xs, 1] = packed[ey - HALO :]

    pl.semaphore_wait(barrier, levels * count_x * count_y - 1)

    def exists(dx, dy, dz):
        ok = None
        for axis, step in enumerate((dx, dy, dz)):
            if step == 0:
                continue
            here = me[axis] + step
            good = (here >= 0) & (here < counts[axis])
            ok = good if ok is None else ok & good
        return ok

    def describe(number):
        kind, dx, dy, dz, part = MESSAGES[number]
        target = (me[0] + dx, me[1] + dy, me[2] + dz)
        xs, ys, zs = (dx + 1) // 2, (dy + 1) // 2, (dz + 1) // 2
        if kind == "x":
            src_x = HALO + part if dx < 0 else ex + part
            dst_x = HALO + ex + part if dx < 0 else part
            src = base.at[0, :, pl.ds(src_x * rows + ypad, ey)]
            dst = base.at[0, :, pl.ds(dst_x * rows + ypad, ey)]
        elif kind == "y":
            src, dst = y_send.at[ys, part], y_recv.at[1 - ys, part]
        elif kind == "xy":
            src, dst = xy_send.at[xs, ys], xy_recv.at[1 - xs, 1 - ys]
        elif kind == "xyn":
            src, dst = xyn_send.at[xs, ys, part], xyn_recv.at[1 - xs, 1 - ys, part]
        else:
            own = pl.ds(ypad, ey)
            if kind == "z" and dy == 0:
                src, dst = z_send, z_recv.at[1 - zs, :, own]
            elif kind == "z":
                src, dst = yz_send.at[ys], yz_recv.at[1 - zs, 1 - ys]
            elif dy == 0:
                src, dst = xz_send.at[xs], xz_recv.at[1 - xs, 1 - zs, own]
            else:
                src, dst = xyz_send.at[xs, ys], xyz_recv.at[1 - xs, 1 - zs, 1 - ys]
        copy = pltpu.make_async_remote_copy(
            src_ref=src,
            dst_ref=dst,
            send_sem=send_sem.at[number],
            recv_sem=recv_sem.at[number],
            device_id=target,
            device_id_type=MESH,
        )
        return copy, exists(dx, dy, dz), exists(-dx, -dy, -dz)

    for number in range(len(MESSAGES)):
        copy, to_there, _ = describe(number)

        @pl.when(to_there)
        def _():
            copy.start()

    rounds = []
    radius = reach
    while radius < count_z - 1:
        rounds.append(radius)
        radius *= 2

    def hello(number):
        for side, step in enumerate((-rounds[number], rounds[number])):

            @pl.when(exists(0, 0, step))
            def _():
                pl.semaphore_signal(
                    hello_sem.at[number, 1 - side],
                    inc=1,
                    device_id=(me[0], me[1], me[2] + step),
                    device_id_type=MESH,
                )

    def hear(number):
        for side, step in enumerate((-rounds[number], rounds[number])):

            @pl.when(exists(0, 0, step))
            def _():
                pl.semaphore_wait(hello_sem.at[number, side], 1)

    if rounds:
        hello(0)

    def wait_for(part, send):
        for number, message in enumerate(MESSAGES):
            far = message[0] in ("y", "xy", "xyn") and message[4] == 1
            if send and (message[0] == "x") != (part == 0):
                continue
            if not send and far != (part == 1):
                continue
            copy, to_there, from_there = describe(number)

            @pl.when(to_there if send else from_there)
            def _():
                if send:
                    copy.wait_send()
                else:
                    copy.wait_recv()

    def unpack_y(part):
        for side in range(2):
            for layer in range(2):
                y = (
                    ypad - 2 - 2 * part + layer
                    if side == 0
                    else ypad + ey + 2 * part + layer
                )
                for f in range(4):
                    for half in range(ex // 8):
                        base[
                            0, f, pl.ds((HALO + 8 * half) * rows + y, 8, stride=rows)
                        ] = y_recv[side, part, f, layer, pl.ds(8 * half, 8)]
                    near_y = ypad - 2 + layer if side == 0 else ypad + ey + layer
                    for xs in range(2):
                        x0 = 0 if xs == 0 else HALO + ex
                        if part == 1:
                            base[0, f, pl.ds(x0 * rows + y, HALO, stride=rows)] = xy_recv[
                                xs, side, f, layer
                            ]
                        x0 = 2 - 2 * part if xs == 0 else HALO + ex + 2 * part
                        base[0, f, pl.ds(x0 * rows + near_y, 2, stride=rows)] = xyn_recv[
                            xs, side, part, f, layer
                        ]

    def unpack_z():
        lane_rows = lax.broadcasted_iota(jnp.int32, (rows, LANES), 1)
        lower = lax.rem(lane_rows, 8) < HALO
        for zs in range(2):
            for ys in range(2):
                edge = pl.ds(first_y if ys == 0 else ypad + ey, HALO)
                for f in range(4):
                    z_recv[zs, f, edge] = yz_recv[zs, ys, f]
                for xs in range(2):
                    xz_recv[xs, zs, edge] = xyz_recv[xs, zs, ys]
        for f in range(4):
            merged = jnp.where(lower, z_recv[0, f], z_recv[1, f])
            for k in range(ex):
                base[1, f, pl.ds((HALO + k) * rows, rows)] = pltpu.roll(
                    merged, (2 * LANES - 8 * k - HALO) % LANES, 1
                )
        for xs in range(2):
            merged = jnp.where(lower, xz_recv[xs, 0], xz_recv[xs, 1])
            for f in range(4):
                for j in range(HALO):
                    k = f * HALO + j
                    x = j if xs == 0 else HALO + ex + j
                    base[1, f, pl.ds(x * rows, rows)] = pltpu.roll(
                        merged, (2 * LANES - 8 * k - HALO) % LANES, 1
                    )

    lane = lax.broadcasted_iota(jnp.int32, (wide_y, LANES), 1)
    row_y = lax.broadcasted_iota(jnp.int32, (wide_y, LANES), 0)
    at_y = me[1] * ey + row_y - HALO
    good_y = (at_y >= 0) & (at_y < ey * count_y)
    good_halo = (
        good_y
        & ((me[2] > 0) | (lane < LANES // 2))
        & ((me[2] < count_z - 1) | (lane >= LANES // 2))
    )
    goods = (good_y, good_halo)

    def at(x, dy=0, own=False):
        if own:
            return pl.ds(x * rows + ypad + dy, ey)
        return pl.ds(x * rows + first_y + dy, wide_y)

    def prepare(x, carry):
        at_x = me[0] * ex + x - HALO
        good_x = (at_x >= 0) & (at_x < ex * count_x)
        for t in range(2):
            good = goods[t] & good_x
            g = jnp.where(good, base[t, 3, at(x)], 1.0)
            base[t, 3, at(x)] = g
            inv = jnp.where(good, RELAXATION / (g * DIAGONAL + MASS_TERM), 0.0)
            inverse[t, at(x)] = inv
            for c in range(3):
                load = jnp.where(good, base[t, c, at(x)], 0.0)
                base[t, c, at(x)] = load
                field_a[t, c, at(x)] = load * inv
        return carry

    def image(field, x, own=False):
        parts = [[None] * 3, [None] * 3]
        ups = [[None] * 3, [None] * 3]
        downs = [[None] * 3, [None] * 3]
        for t in range(2):

            def load(c, ox, oy):
                return field[t, c, at(x + ox, oy, own)]

            centre = [load(c, 0, 0) for c in range(3)]
            x_up = [load(c, 1, 0) for c in range(3)]
            x_down = [load(c, -1, 0) for c in range(3)]
            y_up = [load(c, 0, 1) for c in range(3)]
            y_down = [load(c, 0, -1) for c in range(3)]

            def corners(c):
                return (load(c, 1, 1) - load(c, 1, -1)) - (load(c, -1, 1) - load(c, -1, -1))

            sum_x = [x_up[c] + x_down[c] for c in range(3)]
            sum_y = [y_up[c] + y_down[c] for c in range(3)]
            parts[t][0] = DIAGONAL * centre[0] - OWN * sum_x[0] - sum_y[0] - CROSS * corners(1)
            parts[t][1] = DIAGONAL * centre[1] - sum_x[1] - OWN * sum_y[1] - CROSS * corners(0)
            parts[t][2] = DIAGONAL * centre[2] - sum_x[2] - sum_y[2]
            tilt_x = CROSS * (x_up[2] - x_down[2])
            tilt_y = CROSS * (y_up[2] - y_down[2])
            tilt_z = CROSS * ((x_up[0] - x_down[0]) + (y_up[1] - y_down[1]))
            own_z = OWN * centre[2]
            ups[t] = [centre[0] + tilt_x, centre[1] + tilt_y, own_z + tilt_z]
            downs[t] = [centre[0] - tilt_x, centre[1] - tilt_y, own_z - tilt_z]
        out = [[None] * 3, [None] * 3]
        lanes = lax.broadcasted_iota(jnp.int32, parts[0][0].shape, 1)
        first_lane = lanes == 0
        last_lane = lanes == LANES - 1
        for c in range(3):
            up = [pltpu.roll(ups[t][c], LANES - 1, 1) for t in range(2)]
            down = [pltpu.roll(downs[t][c], 1, 1) for t in range(2)]
            for t in range(2):
                beside = jnp.where(last_lane, up[1 - t], up[t]) + jnp.where(
                    first_lane, down[1 - t], down[t]
                )
                out[t][c] = parts[t][c] - beside
        return out

    def residual(field, x, tiles, own=False):
        images = image(field, x, own)
        out = []
        here = at(x, 0, own)
        for t in tiles:
            g = base[t, 3, here]
            out.append(
                [
                    base[t, c, here] - (g * images[t][c] + MASS_TERM * field[t, c, here])
                    for c in range(3)
                ]
            )
        return out

    def sweep(source, target, low, high):
        def one(x, carry):
            left = residual(source, x, (0, 1))
            for t in range(2):
                inv = inverse[t, at(x)]
                for c in range(3):
                    target[t, c, at(x)] = source[t, c, at(x)] + inv * left[t][c]
            return carry

        by_two(low, high, one, 0)

    def fold(value):
        return jnp.sum(value.reshape(ey // 8, 8, LANES), axis=0)

    zero = jnp.zeros((8, LANES), jnp.float32)

    wait_for(0, False)
    wait_for(0, True)
    unpack_y(0)
    unpack_z()
    by_two(2, wide_x - 2, prepare, 0)
    sweep(field_a, field_b, 3, wide_x - 3)

    def restrict(x, carry):
        left = residual(field_b, x, (0,), True)[0]
        sums = [carry[c] + fold(left[c]) for c in range(3)]
        sums.append(carry[3] + fold(base[0, 3, at(x, 0, True)]))
        return tuple(sums)

    sums = by_two(HALO, HALO + ex, restrict, (zero,) * 4)
    stacked = jnp.concatenate([jnp.sum(s, axis=0, keepdims=True) for s in sums] + [zero[:4]], axis=0)
    source_lane = lax.broadcasted_iota(jnp.int32, (LANES, LANES), 0)
    target_lane = lax.broadcasted_iota(jnp.int32, (LANES, LANES), 1)
    gather = (source_lane // BLOCK == lax.rem(target_lane, cz)).astype(jnp.float32)
    grouped = jnp.dot(stacked, gather, precision=EXACT, preferred_element_type=jnp.float32)
    coarse_send[...] = grouped[:4]

    def coarse_copy(x, y, z, dz):
        return pltpu.make_async_remote_copy(
            src_ref=coarse_send,
            dst_ref=coarse_recv.at[reach - dz, me[0] * count_y + me[1]],
            send_sem=coarse_send_sem.at[reach + dz],
            recv_sem=coarse_recv_sem.at[reach - dz],
            device_id=(x, y, z),
            device_id_type=MESH,
        )

    def coarse_wait():
        for dz in range(-reach, reach + 1):
            z = me[2] + dz
            slots = coarse_recv.at[reach + dz, pl.ds(0, count_x * count_y - (1 if dz == 0 else 0))]

            @pl.when((z >= 0) & (z < count_z))
            def _():
                for sem in (coarse_send_sem, coarse_recv_sem):
                    pltpu.make_async_copy(slots, slots, sem.at[reach + dz]).wait()

    peers(lambda x, y, z, dz: coarse_copy(x, y, z, dz).start())
    coarse_recv[reach, me[0] * count_y + me[1]] = grouped[:4]

    wait_for(1, False)
    unpack_y(1)
    by_two(0, wide_x, prepare, 0)
    sweep(field_a, field_b, 1, wide_x - 1)
    sweep(field_b, field_a, 2, wide_x - 2)

    def load_squares(x, carry):
        loads = [base[0, c, at(x, 0, True)] for c in range(3)]
        return carry + fold(sum(value * value for value in loads))

    load_sum = by_two(HALO, HALO + ex, load_squares, zero)
    wait_for(1, True)
    for number in range(len(rounds)):
        if number > 0:
            hello(number)
        hear(number)
    coarse_wait()

    coarse_rows = -(-(count_y + 1) // 8) * 8
    lane_c = lax.broadcasted_iota(jnp.int32, (coarse_rows, LANES), 1)
    row_c = lax.broadcasted_iota(jnp.int32, (coarse_rows, LANES), 0)
    at_z = me[2] * cz - reach * cz + lane_c
    valid = (
        (row_c < count_y) & (at_z >= 0) & (at_z < cz * count_z) & (lane_c < window * cz)
    )
    slab = [[None] * 4 for _ in range(count_x)]
    for x in range(count_x):
        for c in range(4):
            value = None
            for w in range(window):
                column = jnp.concatenate(
                    [coarse_recv[w, x * count_y + y, c : c + 1] for y in range(count_y)]
                    + [jnp.zeros((coarse_rows - count_y, LANES), jnp.float32)],
                    axis=0,
                )
                value = column if value is None else jnp.where(lane_c // cz == w, column, value)
            slab[x][c] = jnp.where(valid, value, 0.0)
    mass = BLOCK**3 * MASS_TERM
    factor = [slab[x][3] * (BLOCK**2 / BLOCK**3) for x in range(count_x)]
    relax = [
        jnp.where(valid, RELAXATION / (factor[x] * DIAGONAL + mass), 0.0) for x in range(count_x)
    ]
    nothing = jnp.zeros((coarse_rows, LANES), jnp.float32)
    w = [[slab[x][c] * relax[x] for c in range(3)] for x in range(count_x)]

    def y_shift(value, step):
        return pltpu.roll(value, step % coarse_rows, 0)

    def z_shift(value, step):
        return pltpu.roll(value, step % LANES, 1)

    for repeat in range(COARSE - 1):
        fresh = []
        for x in range(count_x):
            here = w[x]
            above = w[x + 1] if x + 1 < count_x else [nothing] * 3
            below = w[x - 1] if x > 0 else [nothing] * 3
            sum_x = [above[c] + below[c] for c in range(3)]
            diff_x = [above[c] - below[c] for c in range(3)]
            y_up = [y_shift(here[c], -1) for c in range(3)]
            y_down = [y_shift(here[c], 1) for c in range(3)]
            sum_y = [y_up[c] + y_down[c] for c in range(3)]
            diff_y = [y_up[c] - y_down[c] for c in range(3)]
            corner_x = y_shift(diff_x[1], -1) - y_shift(diff_x[1], 1)
            corner_y = y_shift(diff_x[0], -1) - y_shift(diff_x[0], 1)
            tilt = [CROSS * diff_x[2], CROSS * diff_y[2], CROSS * (diff_x[0] + diff_y[1])]
            own = [here[0], here[1], OWN * here[2]]
            beside = [z_shift(own[c] + tilt[c], -1) + z_shift(own[c] - tilt[c], 1) for c in range(3)]
            flat = [
                DIAGONAL * here[0] - OWN * sum_x[0] - sum_y[0] - CROSS * corner_x - beside[0],
                DIAGONAL * here[1] - sum_x[1] - OWN * sum_y[1] - CROSS * corner_y - beside[1],
                DIAGONAL * here[2] - sum_x[2] - sum_y[2] - beside[2],
            ]
            fresh.append(
                [
                    here[c] + relax[x] * (slab[x][c] - (factor[x] * flat[c] + mass * here[c]))
                    for c in range(3)
                ]
            )
        w = fresh

    for x in range(count_x + 2):
        for c in range(3):
            inside = 1 <= x <= count_x
            coarse_w[x, c, pl.ds(0, 8)] = jnp.zeros((8, LANES), jnp.float32)
            coarse_w[x, c, pl.ds(8, coarse_rows)] = w[x - 1][c] if inside else nothing
    widen_core = (source_lane == reach * cz + target_lane // BLOCK).astype(jnp.float32)
    widen_halo = (
        source_lane == jnp.where(target_lane < LANES // 2, (reach + 1) * cz, reach * cz - 1)
    ).astype(jnp.float32)
    for xc in range(3):
        for c in range(3):
            cells = [coarse_w[me[0] + xc, c, pl.ds(7 + me[1] + k, 1)] for k in range(3)]
            stacked = jnp.concatenate(cells + [zero[:5]], axis=0)
            for t, matrix in enumerate((widen_core, widen_halo)):
                wide = jnp.dot(stacked, matrix, precision=EXACT, preferred_element_type=jnp.float32)
                low = jnp.broadcast_to(wide[0:1], (wide_y, LANES))
                mid = jnp.broadcast_to(wide[1:2], (wide_y, LANES))
                top = jnp.broadcast_to(wide[2:3], (wide_y, LANES))
                wide = jnp.where(row_y < HALO, low, jnp.where(row_y < HALO + ey, mid, top))
                for plane in range(3):
                    spread_w[t, c, pl.ds((3 * xc + plane) * rows + first_y, wide_y)] = wide
    for plane in range(1, 8):
        images = image(spread_w, plane)
        for t in range(2):
            for c in range(3):
                image_w[t, c, at(plane)] = images[t][c]

    def correct(x, carry):
        kind = (
            1
            + (x >= HALO - 1).astype(jnp.int32)
            + (x >= HALO).astype(jnp.int32)
            + (x >= HALO + 1).astype(jnp.int32)
            + (x >= HALO + ex - 1).astype(jnp.int32)
            + (x >= HALO + ex).astype(jnp.int32)
            + (x >= HALO + ex + 1).astype(jnp.int32)
        )
        for t in range(2):
            inv = inverse[t, at(x)]
            g = base[t, 3, at(x)]
            for c in range(3):
                added = spread_w[t, c, at(kind)]
                field_a[t, c, at(x)] = (
                    field_a[t, c, at(x)]
                    + added
                    - inv * (g * image_w[t, c, at(kind)] + MASS_TERM * added)
                )
        return carry

    by_two(2, wide_x - 2, correct, 0)
    sweep(field_a, field_b, 3, wide_x - 3)

    def squares(x, carry):
        left = residual(field_b, x, (0,), True)[0]
        for c in range(3):
            out_ref[c, x - HALO] = field_b[0, c, at(x, 0, True)]
        return carry + fold(sum(value * value for value in left))

    left_sum = by_two(HALO, HALO + ex, squares, zero)
    load_total = jnp.sum(jnp.sum(load_sum, axis=0, keepdims=True), axis=1, keepdims=True)
    left_total = jnp.sum(jnp.sum(left_sum, axis=0, keepdims=True), axis=1, keepdims=True)
    first = lax.broadcasted_iota(jnp.int32, (1, LANES), 1) == 0
    mine = jnp.where(first, load_total, left_total)
    norm_send[...] = mine

    def norm_start(step, carry):
        pltpu.make_async_remote_copy(
            src_ref=norm_send,
            dst_ref=norm_recv.at[my_id],
            send_sem=norm_send_sem.at[0],
            recv_sem=norm_recv_sem.at[0],
            device_id=place(lax.rem(my_id + step, total)),
            device_id_type=MESH,
        ).start()
        return carry

    lax.fori_loop(1, total, norm_start, 0)
    norm_recv[my_id] = mine
    others = norm_recv.at[pl.ds(0, total - 1)]
    for sem in (norm_send_sem, norm_recv_sem):
        pltpu.make_async_copy(others, others, sem.at[0]).wait()
    summed = jnp.sum(norm_recv[...], axis=0)
    nodes = 3 * ex * ey * ez * total
    norms_ref[...] = jnp.sqrt(summed / nodes)


def on_device(counts, right_side, damage):
    _, ex, ey, ez = right_side.shape
    cz = ez // BLOCK
    wide_x = ex + 2 * HALO
    rows = ey + 16
    flat = wide_x * rows
    wide_y = ey + 2 * HALO
    total = counts[0] * counts[1] * counts[2]
    window = 2 * (-(-COARSE // cz)) + 1
    coarse_rows = -(-(counts[1] + 1) // 8) * 8
    rounds = 0
    while window // 2 << rounds < counts[2] - 1:
        rounds += 1
    f32 = jnp.float32
    vmem = pltpu.VMEM
    dma = pltpu.SemaphoreType.DMA
    displacement, norms = pl.pallas_call(
        functools.partial(kernel, counts, (ex, ey, ez)),
        out_shape=(
            pltpu.VMEM(right_side.shape, f32),
            pltpu.VMEM((1, LANES), f32),
        ),
        in_specs=[pl.BlockSpec(memory_space=pl.ANY)] * 2,
        out_specs=(
            pl.BlockSpec(memory_space=pltpu.VMEM),
            pl.BlockSpec(memory_space=pltpu.VMEM),
        ),
        scratch_shapes=[
            vmem((2, 4, flat, LANES), f32),
            vmem((2, flat, LANES), f32),
            vmem((2, 3, flat, LANES), f32),
            vmem((2, 3, flat, LANES), f32),
            vmem((ex, ey, LANES), jnp.int32),
            vmem((2, 2, 4, 2, ex, LANES), f32),
            vmem((2, 2, 4, 2, ex, LANES), f32),
            vmem((2, 2, 4, 2, HALO, LANES), f32),
            vmem((2, 2, 4, 2, HALO, LANES), f32),
            vmem((2, 2, 2, 4, 2, 2, LANES), f32),
            vmem((2, 2, 2, 4, 2, 2, LANES), f32),
            vmem((2, 4, HALO, LANES), f32),
            vmem((2, 2, 4, HALO, LANES), f32),
            vmem((2, 2, HALO, LANES), f32),
            vmem((2, 2, 2, HALO, LANES), f32),
            vmem((4, ey, LANES), f32),
            vmem((2, 4, rows, LANES), f32),
            vmem((2, ey, LANES), f32),
            vmem((2, 2, rows, LANES), f32),
            vmem((4, LANES), f32),
            vmem((window, counts[0] * counts[1], 4, LANES), f32),
            vmem((counts[0] + 2, 3, 8 + coarse_rows, LANES), f32),
            vmem((2, 3, 9 * rows, LANES), f32),
            vmem((2, 3, 9 * rows, LANES), f32),
            vmem((1, LANES), f32),
            vmem((total, 1, LANES), f32),
            dma((ex + 1,)),
            dma((len(MESSAGES),)),
            dma((len(MESSAGES),)),
            dma((window,)),
            dma((window,)),
            dma((1,)),
            dma((1,)),
            pltpu.SemaphoreType.REGULAR((max(1, rounds), 2)),
        ],
        compiler_params=pltpu.CompilerParams(collective_id=0, has_side_effects=True),
    )(right_side, damage)
    return displacement, norms[0, :2]


def solution(mesh):
    counts = tuple(mesh.shape[axis] for axis in AXES)
    placed = (P(None, "gx", "gy", "gz"), P("gx", "gy", "gz"))
    return jax.shard_map(
        functools.partial(on_device, counts),
        mesh=mesh,
        in_specs=placed,
        out_specs=(P(None, "gx", "gy", "gz"), P()),
        check_vma=False,
    )
```

```python
import functools

import jax
import jax.numpy as jnp
from jax import lax
from jax.experimental import pallas as pl
from jax.experimental.pallas import tpu as pltpu
from jax.sharding import PartitionSpec as P

BLOCK = 16
COARSE = 8
FLOOR_STIFFNESS = 0.05
MASS_TERM = 0.001
COUPLING = 2.5
RELAXATION = 0.6
KEEP = 1.0 - RELAXATION
DIAGONAL = 6.0 + 2.0 * COUPLING
OWN = 1.0 + COUPLING
CROSS = 0.25 * COUPLING
AXES = ("gx", "gy", "gz")
HALO = 4
EDGE = 2 * HALO
LANES = 128
YPAD = 8
MESH = pl.DeviceIdType.MESH
EXACT = lax.Precision.HIGHEST
NEAR = ((0, 1), (1, 1), (2, 1), (3, 1), (0, 2), (1, 2), (2, 2))
FAR = ((3, 2), (0, 3), (1, 3), (2, 3), (3, 3), (0, 4), (1, 4), (2, 4))
LAYERS = NEAR + FAR


def directions():
    out = []
    for dx in (-1, 0, 1):
        for dy in (-1, 0, 1):
            for dz in (-1, 0, 1):
                if (dx, dy, dz) != (0, 0, 0):
                    out.append((dx, dy, dz))
    return sorted(out, key=lambda d: -sum(abs(step) for step in d))


DIRECTIONS = directions()
FAR_DIRECTIONS = [d for d in DIRECTIONS if d[1] != 0]


UNROLL = 24


def by_two(low, high, body, carry):
    trips = -(-(high - low) // UNROLL)
    size = -(-(high - low) // trips)
    whole = (high - low) // size

    def several(trip, carry):
        for k in range(size):
            carry = body(low + size * trip + k, carry)
        return carry

    if whole > 1:
        carry = lax.fori_loop(0, whole, several, carry)
    else:
        carry = several(0, carry)
    for k in range(low + whole * size, high):
        carry = body(k, carry)
    return carry


def kernel(
    counts,
    extent,
    load_ref,
    damage_ref,
    out_ref,
    norms_ref,
    raw,
    stiff,
    harm,
    base,
    field_a,
    field_b,
    edge_base,
    edge_a,
    edge_b,
    sides,
    y_send,
    y_recv,
    xyn_send,
    xyn_recv,
    xy_send,
    xy_recv,
    p_all,
    q_send,
    q_all,
    py_send,
    py_recv,
    qy_send,
    qy_recv,
    coarse_send,
    coarse_recv,
    coarse_w,
    stack_w,
    spread_w,
    image_w,
    norm_send,
    norm_recv,
    amount,
    local_sem,
    send_sem,
    near_sem,
    far_sem,
    coarse_send_sem,
    coarse_recv_sem,
    norm_sem,
    hello_sem,
):
    count_x, count_y, count_z = counts
    ex, ey, ez = extent
    cz = ez // BLOCK
    total = count_x * count_y * count_z
    wide_x = ex + 2 * HALO
    ypad = YPAD
    rows = ey + 2 * ypad
    wide_y = ey + 2 * HALO
    first_y = ypad - HALO
    me = tuple(lax.axis_index(axis) for axis in AXES)
    my_id = (me[0] * count_y + me[1]) * count_z + me[2]

    def place(index):
        return (
            index // (count_y * count_z),
            lax.rem(index // count_z, count_y),
            lax.rem(index, count_z),
        )

    harm_copy = pltpu.make_async_copy(damage_ref, harm, local_sem.at[0])
    load_copy = pltpu.make_async_copy(load_ref, raw, local_sem.at[1])
    harm_copy.start()
    load_copy.start()
    barrier = pltpu.get_barrier_semaphore()

    reach = -(-COARSE // cz)
    window = 2 * reach + 1

    def peers(act):
        for dz in range(-reach, reach + 1):
            z = me[2] + dz

            @pl.when((z >= 0) & (z < count_z))
            def _():
                def one(step, carry):
                    if dz == 0:
                        step = step + 1
                    index = lax.rem(me[0] * count_y + me[1] + step, count_x * count_y)
                    act(index // count_y, lax.rem(index, count_y), z, dz)
                    return carry

                lax.fori_loop(0, count_x * count_y - (1 if dz == 0 else 0), one, 0)

    def greet(x, y, z, dz):
        pl.semaphore_signal(barrier, inc=1, device_id=(x, y, z), device_id_type=MESH)

    peers(greet)
    levels = jnp.minimum(me[2] + reach, count_z - 1) - jnp.maximum(me[2] - reach, 0) + 1

    def exists(dx, dy, dz):
        ok = None
        for axis, step in enumerate((dx, dy, dz)):
            if step == 0:
                continue
            here = me[axis] + step
            good = (here >= 0) & (here < counts[axis])
            ok = good if ok is None else ok & good
        return ok

    def block(x):
        return pl.ds((HALO + x) * rows + ypad, ey)

    for xs in range(2):

        @pl.when(jnp.logical_not(exists(2 * xs - 1, 0, 0)))
        def _():
            for part in range(HALO):
                for f in range(4):
                    x = part - HALO if xs == 0 else ex + part
                    base[f, block(x)] = jnp.zeros((ey, LANES), jnp.float32)

        for ys in range(2):

            @pl.when(jnp.logical_not(exists(2 * xs - 1, 2 * ys - 1, 0)))
            def _():
                xyn_recv[xs, ys] = jnp.zeros((len(NEAR), 2, LANES), jnp.float32)
                xy_recv[xs, ys] = jnp.zeros((len(LAYERS), HALO, LANES), jnp.float32)

    for ys in range(2):

        @pl.when(jnp.logical_not(exists(0, 2 * ys - 1, 0)))
        def _():
            y_recv[ys] = jnp.zeros((len(LAYERS), ex, LANES), jnp.float32)

    lane_own = lax.broadcasted_iota(jnp.int32, (ey, LANES), 1)
    lane = lax.broadcasted_iota(jnp.int32, (wide_y, LANES), 1)
    row_y = lax.broadcasted_iota(jnp.int32, (wide_y, LANES), 0)
    lower = lax.rem(lane, EDGE) < HALO
    at_y = me[1] * ey + row_y - HALO
    good_y = (at_y >= 0) & (at_y < ey * count_y)
    has_back, has_front = me[2] > 0, me[2] < count_z - 1
    upper_x = lax.rem(lane // (HALO * EDGE), 2) == 0
    high_z = lane >= LANES // 2
    good_x = (upper_x & (me[0] < count_x - 1)) | (~upper_x & (me[0] > 0))
    good_z = (high_z & (lower | has_front)) | (~high_z & (~lower | has_back))
    goods = (
        good_y & (~lower | has_back),
        good_y & (lower | has_front),
        good_y & good_x & good_z,
    )

    def fold(value):
        return jnp.sum(value.reshape(ey // 8, 8, LANES), axis=0)

    zero = jnp.zeros((8, LANES), jnp.float32)

    harm_copy.wait()
    load_copy.wait()

    def own_rows(x):
        return pl.ds(x * ey, ey)

    load_sum = zero
    stiff_sum = zero
    packed = [None] * 4
    for x in range(ex):
        level = 1.0 - harm[x].astype(jnp.float32) / 15.0
        g = level * level * (1.0 - FLOOR_STIFFNESS) + FLOOR_STIFFNESS
        inv = RELAXATION / (g * DIAGONAL + MASS_TERM)
        stiff[own_rows(x)] = g
        stiff_sum = stiff_sum + fold(g)
        values = []
        squared = None
        for c in range(3):
            load = raw[c, x]
            values.append(load * inv)
            squared = load * load if squared is None else squared + load * load
        load_sum = load_sum + fold(squared)
        values.append(g * inv)
        for f in range(4):
            base[f, block(x)] = values[f]
            moved = pltpu.roll(values[f], (EDGE * x + HALO) % LANES, 1)
            packed[f] = moved if x == 0 else jnp.where(lane_own // EDGE == x, moved, packed[f])
    for f in range(4):
        p_all[1, f, pl.ds(ypad, ey)] = packed[f]
        for phase in range(2):
            py_send[phase, 0, f] = packed[f][2 * phase : 2 * phase + 2]
            py_send[phase, 1, f] = packed[f][ey - 2 - 2 * phase : ey - 2 * phase]
    width = HALO * EDGE
    for xs in range(2):
        joined = None
        for f in range(4):
            shift = width * f - (0 if xs == 0 else (ex - HALO) * EDGE)
            moved = pltpu.roll(packed[f], shift % LANES, 1)
            joined = moved if f == 0 else jnp.where(lane_own // width == f, moved, joined)
        q_send[xs] = joined
        for phase in range(2):
            qy_send[phase, xs, 0] = joined[2 * phase : 2 * phase + 2]
            qy_send[phase, xs, 1] = joined[ey - 2 - 2 * phase : ey - 2 * phase]
    for side in range(2):
        for i, (f, layer) in enumerate(LAYERS):
            start = HALO * rows + ypad + (layer - 1 if side == 0 else ey - layer)
            for half in range(ex // 8):
                y_send[side, i, pl.ds(8 * half, 8)] = base[
                    f, pl.ds(start + 8 * half * rows, 8, stride=rows)
                ]
            for xs in range(2):
                x0 = 0 if xs == 0 else ex - HALO
                xy_send[xs, side, i] = base[f, pl.ds(start + x0 * rows, HALO, stride=rows)]
                if i < len(NEAR):
                    x0 = 0 if xs == 0 else ex - 2
                    xyn_send[xs, side, i] = base[f, pl.ds(start + x0 * rows, 2, stride=rows)]

    pl.semaphore_wait(barrier, levels * count_x * count_y - 1)

    def pieces(d, phase):
        dx, dy, dz = d
        xs, ys = (dx + 1) // 2, (dy + 1) // 2
        out = []
        near, far = pl.ds(0, len(NEAR)), pl.ds(len(NEAR), len(FAR))
        own = pl.ds(ypad, ey)
        if dy == 0:
            if phase == 1:
                return out
            if dz == 0:
                for part in range(HALO):
                    src_x = part if dx < 0 else ex - HALO + part
                    dst_x = ex + part if dx < 0 else part - HALO
                    out.append((base.at[:, block(src_x)], base.at[:, block(dst_x)], 4 * ey))
            if dx == 0:
                out.append((p_all.at[1, :, own], p_all.at[1 - dz, :, own], 4 * ey))
            else:
                out.append((q_send.at[xs], q_all.at[1 - xs, 1 - dz, own], ey))
            return out
        if dx == 0:
            out.append((py_send.at[phase, ys], py_recv.at[phase, 1 - ys, 1 - dz], 8))
        else:
            out.append((qy_send.at[phase, xs, ys], qy_recv.at[phase, 1 - xs, 1 - ys, 1 - dz], 2))
        if dz == 0 and dx == 0:
            part = near if phase == 0 else far
            size = len(NEAR) if phase == 0 else len(FAR)
            out.append((y_send.at[ys, part], y_recv.at[1 - ys, part], size * ex))
        elif dz == 0 and phase == 0:
            out.append((xyn_send.at[xs, ys], xyn_recv.at[1 - xs, 1 - ys], 2 * len(NEAR)))
        elif dz == 0:
            out.append((xy_send.at[xs, ys], xy_recv.at[1 - xs, 1 - ys], HALO * len(LAYERS)))
        return out

    def arrival(number, phase):
        if phase == 0:
            return near_sem.at[number]
        return far_sem.at[FAR_DIRECTIONS.index(DIRECTIONS[number])]

    def start_sends(phase):
        for number, d in enumerate(DIRECTIONS):
            parts = pieces(d, phase)
            if not parts:
                continue

            @pl.when(exists(*d))
            def _():
                for src, dst, _ in parts:
                    pltpu.make_async_remote_copy(
                        src_ref=src,
                        dst_ref=dst,
                        send_sem=send_sem.at[number],
                        recv_sem=arrival(number, phase),
                        device_id=tuple(me[axis] + d[axis] for axis in range(3)),
                        device_id_type=MESH,
                    ).start()

    start_sends(0)
    start_sends(1)

    def wait_bytes(size, sem):
        span = amount.at[pl.ds(0, size)]
        pltpu.make_async_copy(span, span, sem).wait()

    def wait_near_or_far(phase):
        for number, d in enumerate(DIRECTIONS):
            size = sum(part[2] for part in pieces(d, phase))
            if size:

                @pl.when(exists(*(-step for step in d)))
                def _():
                    wait_bytes(size, arrival(number, phase))

    def wait_sends():
        for number, d in enumerate(DIRECTIONS):
            size = sum(part[2] for phase in range(2) for part in pieces(d, phase))

            @pl.when(exists(*d))
            def _():
                wait_bytes(size, send_sem.at[number])

    rounds = []
    radius = reach
    while radius < count_z - 1:
        rounds.append(radius)
        radius *= 2

    def hello(number):
        for side, step in enumerate((-rounds[number], rounds[number])):

            @pl.when(exists(0, 0, step))
            def _():
                pl.semaphore_signal(
                    hello_sem.at[number, 1 - side],
                    inc=1,
                    device_id=(me[0], me[1], me[2] + step),
                    device_id_type=MESH,
                )

    def hear(number):
        for side, step in enumerate((-rounds[number], rounds[number])):

            @pl.when(exists(0, 0, step))
            def _():
                pl.semaphore_wait(hello_sem.at[number, side], 1)

    if rounds:
        hello(0)

    def unpack(phase):
        for side in range(2):
            for i, (f, layer) in enumerate(LAYERS):
                y = ypad - layer if side == 0 else ypad + ey + layer - 1
                if (i < len(NEAR)) == (phase == 0):
                    for half in range(ex // 8):
                        base[f, pl.ds((HALO + 8 * half) * rows + y, 8, stride=rows)] = y_recv[
                            side, i, pl.ds(8 * half, 8)
                        ]
                for xs in range(2):
                    if phase == 1:
                        x0 = 0 if xs == 0 else HALO + ex
                        base[f, pl.ds(x0 * rows + y, HALO, stride=rows)] = xy_recv[xs, side, i]
                    elif i < len(NEAR):
                        x0 = HALO - 2 if xs == 0 else HALO + ex
                        base[f, pl.ds(x0 * rows + y, 2, stride=rows)] = xyn_recv[xs, side, i]
            start = ypad - 2 - 2 * phase if side == 0 else ypad + ey + 2 * phase
            for dz in range(3):
                for f in range(4):
                    p_all[dz, f, pl.ds(start, 2)] = py_recv[phase, side, dz, f]
                for xs in range(2):
                    q_all[xs, dz, pl.ds(start, 2)] = qy_recv[phase, xs, side, dz]
        wide = pl.ds(first_y, wide_y)
        for f in range(4):
            back, here, front = (p_all[dz, f, wide] for dz in range(3))
            edge_base[f, 0, wide] = jnp.where(goods[0], jnp.where(lower, back, here), 0.0)
            edge_base[f, 1, wide] = jnp.where(goods[1], jnp.where(lower, here, front), 0.0)
        low, high = [], []
        for xs in range(2):
            back, here, front = (q_all[xs, dz, wide] for dz in range(3))
            low.append(jnp.where(lower, back, here))
            high.append(jnp.where(lower, here, front))
        for f in range(4):
            quarter = [
                pltpu.roll(value, (width * (k - f)) % LANES, 1)
                for k, value in enumerate((low[1], low[0], high[1], high[0]))
            ]
            merged = jnp.where(
                high_z,
                jnp.where(upper_x, quarter[2], quarter[3]),
                jnp.where(upper_x, quarter[0], quarter[1]),
            )
            edge_base[f, 2, wide] = jnp.where(goods[2], merged, 0.0)

    def at(p, dy=0, own=False):
        if own:
            return pl.ds(p * rows + ypad + dy, ey)
        return pl.ds(p * rows + first_y + dy, wide_y)

    cell = lane // EDGE
    last_cell = cell == LANES // EDGE - 1
    first_cell = cell == 0
    half_cell = LANES // EDGE // 2

    def turn(value, step):
        return pltpu.roll(value, step % LANES, 1)

    def edge_shift(values, step):
        low, high, outer = values
        near = [turn(value, -step * EDGE) for value in values]
        half = LANES // 2
        if step > 0:
            return [
                jnp.where(last_cell, near[2], near[0]),
                jnp.where(last_cell, turn(outer, half - EDGE), near[1]),
                jnp.where(
                    last_cell,
                    near[1],
                    jnp.where(cell == half_cell - 1, turn(low, half - EDGE), near[2]),
                ),
            ]
        return [
            jnp.where(first_cell, turn(outer, half + EDGE), near[0]),
            jnp.where(first_cell, near[2], near[1]),
            jnp.where(
                first_cell, near[0], jnp.where(cell == half_cell, turn(high, half + EDGE), near[2])
            ),
        ]

    def edge_stage(field, stage, sums=True):
        wide = pl.ds(first_y, wide_y)

        def load(c, oy):
            return [field[c, k, pl.ds(first_y + oy, wide_y)] for k in range(3)]

        centre = [load(c, 0) for c in range(3)]
        y_up = [load(c, 1) for c in range(3)]
        y_down = [load(c, -1) for c in range(3)]
        slope = [[CROSS * (y_up[c][k] - y_down[c][k]) for k in range(3)] for c in range(3)]
        used = range(3) if sums else (0, 2)
        x_up = {c: edge_shift(centre[c], 1) for c in used}
        x_down = {c: edge_shift(centre[c], -1) for c in used}
        ups, downs = [], []
        for k in range(3):
            tilt = [
                CROSS * (x_up[2][k] - x_down[2][k]),
                slope[2][k],
                CROSS * (x_up[0][k] - x_down[0][k]) + slope[1][k],
            ]
            mine = [centre[0][k], centre[1][k], OWN * centre[2][k]]
            ups.append([mine[c] + tilt[c] for c in range(3)])
            downs.append([mine[c] - tilt[c] for c in range(3)])
        front = lax.rem(lane, EDGE) == HALO
        for c in range(3):
            sides[stage, c, pl.ds(first_y, wide_y)] = jnp.where(front, ups[1][c], turn(downs[0][c], 2))
            sides[stage, c, pl.ds(rows + first_y, wide_y)] = jnp.where(
                front, turn(ups[2][c], LANES // 2), turn(downs[2][c], 2)
            )
        if not sums:
            return None
        slope_up = [edge_shift(slope[c], 1) for c in range(2)]
        slope_down = [edge_shift(slope[c], -1) for c in range(2)]
        out = []
        for k in range(3):
            sum_x = [x_up[c][k] + x_down[c][k] for c in range(3)]
            sum_y = [y_up[c][k] + y_down[c][k] for c in range(3)]
            sum_z = [turn(ups[k][c], -1) + turn(downs[k][c], 1) for c in range(3)]
            out.append(
                [
                    OWN * sum_x[0] + sum_y[0] + (slope_up[1][k] - slope_down[1][k]) + sum_z[0],
                    sum_x[1] + OWN * sum_y[1] + (slope_up[0][k] - slope_down[0][k]) + sum_z[1],
                    sum_x[2] + sum_y[2] + sum_z[2],
                ]
            )
        return out

    def edge_sweep(source, target, stage):
        beside = edge_stage(source, stage)
        wide = pl.ds(first_y, wide_y)
        for k in range(3):
            share = edge_base[3, k, wide]
            for c in range(3):
                target[c, k, wide] = (
                    KEEP * source[c, k, wide] + edge_base[c, k, wide] + share * beside[k][c]
                )

    def neighbours(field, p, x, stage, own=False):
        def load(c, ox, oy):
            return field[c, at(p + ox, oy, own)]

        if isinstance(x, int):
            ring = (x + 2 * HALO) % wide_x
            outside = ring < 2 * HALO
            where_x = ring if outside else ring - 2 * HALO
            shift = (LANES - 1 - HALO - EDGE * where_x) % LANES
            start = (rows if outside else 0) + (ypad if own else first_y)
        else:
            ring = lax.rem(x + 2 * HALO, wide_x)
            outside = ring < 2 * HALO
            where_x = jnp.where(outside, ring, ring - 2 * HALO)
            shift = lax.rem(2 * LANES - 1 - HALO - EDGE * where_x, LANES)
            start = jnp.where(outside, rows, 0) + (ypad if own else first_y)
        height = ey if own else wide_y
        centre = [load(c, 0, 0) for c in range(3)]
        x_up = [load(c, 1, 0) for c in range(3)]
        x_down = [load(c, -1, 0) for c in range(3)]
        y_up = [load(c, 0, 1) for c in range(3)]
        y_down = [load(c, 0, -1) for c in range(3)]
        slope = [CROSS * (y_up[c] - y_down[c]) for c in range(3)]
        corner = [
            CROSS * (load(c, 1, 1) - load(c, 1, -1)) - CROSS * (load(c, -1, 1) - load(c, -1, -1))
            for c in range(2)
        ]
        tilt = [
            CROSS * (x_up[2] - x_down[2]),
            slope[2],
            CROSS * (x_up[0] - x_down[0]) + slope[1],
        ]
        mine = [centre[0], centre[1], OWN * centre[2]]
        lanes = lax.broadcasted_iota(jnp.int32, (height, LANES), 1)
        sum_z = []
        for c in range(3):
            end = pltpu.roll(sides[stage, c, pl.ds(start, height)], shift, 1)
            up = jnp.where(lanes == LANES - 1, end, turn(mine[c] + tilt[c], -1))
            down = jnp.where(lanes == 0, end, turn(mine[c] - tilt[c], 1))
            sum_z.append(up + down)
        return [
            OWN * (x_up[0] + x_down[0]) + (y_up[0] + y_down[0]) + corner[1] + sum_z[0],
            (x_up[1] + x_down[1]) + OWN * (y_up[1] + y_down[1]) + corner[0] + sum_z[1],
            (x_up[2] + x_down[2]) + (y_up[2] + y_down[2]) + sum_z[2],
        ]

    def sweep(source, target, low, high, stage):
        def one(p, carry):
            beside = neighbours(source, p, p - HALO, stage)
            share = base[3, at(p)]
            for c in range(3):
                target[c, at(p)] = KEEP * source[c, at(p)] + base[c, at(p)] + share * beside[c]
            return carry

        by_two(low, high, one, 0)

    def residual(field, x, stage):
        p = x + HALO
        beside = neighbours(field, p, x, stage, True)
        g = stiff[own_rows(x)]
        heavy = g * DIAGONAL + MASS_TERM
        return [
            raw[c, x] - heavy * field[c, at(p, 0, True)] + g * beside[c] for c in range(3)
        ]

    wait_near_or_far(0)
    greeted = min(1, len(rounds) - 1)
    for number in range(greeted):
        hear(number)
        hello(number + 1)
    unpack(0)
    edge_sweep(edge_base, edge_a, 0)
    edge_stage(edge_a, 1, False)
    sweep(base, field_b, HALO - 1, HALO + ex + 1, 0)

    def restrict(x, carry):
        left = residual(field_b, x, 1)
        return tuple(carry[c] + left[c] for c in range(3))

    sums = by_two(0, ex, restrict, (jnp.zeros((ey, LANES), jnp.float32),) * 3)
    sums = [fold(s) for s in sums] + [stiff_sum]
    stacked = jnp.concatenate([jnp.sum(s, axis=0, keepdims=True) for s in sums] + [zero[:4]], axis=0)
    source_lane = lax.broadcasted_iota(jnp.int32, (LANES, LANES), 0)
    target_lane = lax.broadcasted_iota(jnp.int32, (LANES, LANES), 1)
    gather = (source_lane // BLOCK == lax.rem(target_lane, cz)).astype(jnp.float32)
    grouped = jnp.dot(stacked, gather, precision=EXACT, preferred_element_type=jnp.float32)
    coarse_send[...] = grouped[:4]

    def coarse_copy(x, y, z, dz):
        return pltpu.make_async_remote_copy(
            src_ref=coarse_send,
            dst_ref=coarse_recv.at[reach - dz, me[0] * count_y + me[1]],
            send_sem=coarse_send_sem.at[reach + dz],
            recv_sem=coarse_recv_sem.at[reach - dz],
            device_id=(x, y, z),
            device_id_type=MESH,
        )

    def coarse_wait():
        for dz in range(-reach, reach + 1):
            z = me[2] + dz
            slots = coarse_recv.at[reach + dz, pl.ds(0, count_x * count_y - (1 if dz == 0 else 0))]

            @pl.when((z >= 0) & (z < count_z))
            def _():
                for sem in (coarse_send_sem, coarse_recv_sem):
                    pltpu.make_async_copy(slots, slots, sem.at[reach + dz]).wait()

    peers(lambda x, y, z, dz: coarse_copy(x, y, z, dz).start())
    coarse_recv[reach, me[0] * count_y + me[1]] = grouped[:4]

    wait_near_or_far(1)
    unpack(1)
    edge_sweep(edge_base, edge_a, 0)
    edge_sweep(edge_a, edge_b, 1)
    sweep(base, field_a, 1, wide_x - 1, 0)
    sweep(field_a, field_b, 2, wide_x - 2, 1)
    wait_sends()
    coarse_wait()

    coarse_rows = -(-(count_y + 1) // 8) * 8
    lane_c = lax.broadcasted_iota(jnp.int32, (coarse_rows, LANES), 1)
    row_c = lax.broadcasted_iota(jnp.int32, (coarse_rows, LANES), 0)
    at_z = me[2] * cz - reach * cz + lane_c
    valid = (
        (row_c < count_y) & (at_z >= 0) & (at_z < cz * count_z) & (lane_c < window * cz)
    )
    slab = [[None] * 4 for _ in range(count_x)]
    for x in range(count_x):
        for c in range(4):
            value = None
            for w in range(window):
                column = jnp.concatenate(
                    [coarse_recv[w, x * count_y + y, c : c + 1] for y in range(count_y)]
                    + [jnp.zeros((coarse_rows - count_y, LANES), jnp.float32)],
                    axis=0,
                )
                value = column if value is None else jnp.where(lane_c // cz == w, column, value)
            slab[x][c] = jnp.where(valid, value, 0.0)
    mass = BLOCK**3 * MASS_TERM
    factor = [slab[x][3] * (BLOCK**2 / BLOCK**3) for x in range(count_x)]
    relax = [
        jnp.where(valid, RELAXATION / (factor[x] * DIAGONAL + mass), 0.0) for x in range(count_x)
    ]
    nothing = jnp.zeros((coarse_rows, LANES), jnp.float32)
    start_w = [[slab[x][c] * relax[x] for c in range(3)] for x in range(count_x)]
    share_w = [factor[x] * relax[x] for x in range(count_x)]
    w = start_w

    def y_shift(value, step):
        return pltpu.roll(value, step % coarse_rows, 0)

    for repeat in range(COARSE - 1):
        fresh = []
        for x in range(count_x):
            here = w[x]
            above = w[x + 1] if x + 1 < count_x else [nothing] * 3
            below = w[x - 1] if x > 0 else [nothing] * 3
            sum_x = [above[c] + below[c] for c in range(3)]
            diff_x = [above[c] - below[c] for c in range(3)]
            y_up = [y_shift(here[c], -1) for c in range(3)]
            y_down = [y_shift(here[c], 1) for c in range(3)]
            sum_y = [y_up[c] + y_down[c] for c in range(3)]
            diff_y = [y_up[c] - y_down[c] for c in range(3)]
            corner_x = y_shift(diff_x[1], -1) - y_shift(diff_x[1], 1)
            corner_y = y_shift(diff_x[0], -1) - y_shift(diff_x[0], 1)
            tilt = [CROSS * diff_x[2], CROSS * diff_y[2], CROSS * (diff_x[0] + diff_y[1])]
            own = [here[0], here[1], OWN * here[2]]
            sum_z = [turn(own[c] + tilt[c], -1) + turn(own[c] - tilt[c], 1) for c in range(3)]
            beside = [
                OWN * sum_x[0] + sum_y[0] + CROSS * corner_x + sum_z[0],
                sum_x[1] + OWN * sum_y[1] + CROSS * corner_y + sum_z[1],
                sum_x[2] + sum_y[2] + sum_z[2],
            ]
            fresh.append(
                [
                    KEEP * here[c] + start_w[x][c] + share_w[x] * beside[c]
                    for c in range(3)
                ]
            )
        w = fresh

    for x in range(count_x + 2):
        for c in range(3):
            inside = 1 <= x <= count_x
            coarse_w[x, c, pl.ds(0, 8)] = jnp.zeros((8, LANES), jnp.float32)
            coarse_w[x, c, pl.ds(8, coarse_rows)] = w[x - 1][c] if inside else nothing
    stack_w[pl.ds(24, 8)] = zero
    for xc in range(3):
        for c in range(3):
            stack_w[pl.ds(3 * (3 * xc + c), 3)] = coarse_w[me[0] + xc, c, pl.ds(7 + me[1], 3)]
    inner = lax.rem(target_lane, EDGE) < HALO
    first_cell_z, last_cell_z = reach * cz, (reach + 1) * cz - 1
    pick_low = jnp.where(inner, first_cell_z - 1, first_cell_z)
    pick_high = jnp.where(inner, last_cell_z, last_cell_z + 1)
    picks = (
        first_cell_z + target_lane // BLOCK,
        pick_low,
        pick_high,
        jnp.where(target_lane < LANES // 2, pick_low, pick_high),
    )
    widen = jnp.concatenate([(source_lane == pick).astype(jnp.float32) for pick in picks], axis=1)
    wide_all = jnp.dot(stack_w[...], widen, precision=EXACT, preferred_element_type=jnp.float32)

    def drawn(xc, c, k):
        parts = []
        for j in range(3):
            line = 3 * (3 * xc + c) + j
            piece = wide_all[line : line + 1, k * LANES : (k + 1) * LANES]
            parts.append(jnp.broadcast_to(piece, (wide_y, LANES)))
        return jnp.where(row_y < HALO, parts[0], jnp.where(row_y < HALO + ey, parts[1], parts[2]))

    wide = pl.ds(first_y, wide_y)
    for c in range(3):
        for xc in range(3):
            value = drawn(xc, c, 0)
            for plane in range(3):
                spread_w[c, pl.ds((3 * xc + plane) * rows + first_y, wide_y)] = value
        edge_a[c, 0, wide] = drawn(1, c, 1)
        edge_a[c, 1, wide] = drawn(1, c, 2)
        edge_a[c, 2, wide] = jnp.where(upper_x, drawn(2, c, 3), drawn(0, c, 3))
    beside = edge_stage(edge_a, 0)
    for k in range(3):
        share = edge_base[3, k, wide]
        for c in range(3):
            edge_b[c, k, wide] = (
                edge_b[c, k, wide] + KEEP * edge_a[c, k, wide] + share * beside[k][c]
            )
    edge_sweep(edge_b, edge_a, 1)
    edge_stage(edge_a, 2, False)
    for plane, x in ((1, -2), (2, -1), (3, 0), (4, ex // 2), (5, ex - 1), (6, ex), (7, ex + 1)):
        images = neighbours(spread_w, plane, x, 0)
        for c in range(3):
            image_w[c, at(plane)] = images[c]

    def correct(p, carry):
        kind = (
            jnp.int32(1)
            + jnp.int32(p >= HALO - 1)
            + jnp.int32(p >= HALO)
            + jnp.int32(p >= HALO + 1)
            + jnp.int32(p >= HALO + ex - 1)
            + jnp.int32(p >= HALO + ex)
            + jnp.int32(p >= HALO + ex + 1)
        )
        share = base[3, at(p)]
        for c in range(3):
            field_b[c, at(p)] = (
                field_b[c, at(p)] + KEEP * spread_w[c, at(kind)] + share * image_w[c, at(kind)]
            )
        return carry

    by_two(2, wide_x - 2, correct, 0)
    sweep(field_b, field_a, 3, wide_x - 3, 1)

    def squares(x, carry):
        left = residual(field_a, x, 2)
        for c in range(3):
            out_ref[c, x] = field_a[c, at(x + HALO, 0, True)]
        return carry + fold(sum(value * value for value in left))

    left_sum = by_two(0, ex, squares, zero)
    load_total = jnp.sum(jnp.sum(load_sum, axis=0, keepdims=True), axis=1, keepdims=True)
    left_total = jnp.sum(jnp.sum(left_sum, axis=0, keepdims=True), axis=1, keepdims=True)
    first = lax.broadcasted_iota(jnp.int32, (1, LANES), 1) == 0
    mine = jnp.where(first, load_total, left_total)
    norm_send[...] = mine

    def norm_start(step, carry):
        pltpu.make_async_remote_copy(
            src_ref=norm_send,
            dst_ref=norm_recv.at[my_id],
            send_sem=norm_sem.at[0],
            recv_sem=norm_sem.at[1],
            device_id=place(lax.rem(my_id + step, total)),
            device_id_type=MESH,
        ).start()
        return carry

    for number in range(greeted, len(rounds)):
        if number > greeted:
            hello(number)
        hear(number)
    lax.fori_loop(1, total, norm_start, 0)
    norm_recv[my_id] = mine
    others = norm_recv.at[pl.ds(0, total - 1)]
    for k in range(2):
        pltpu.make_async_copy(others, others, norm_sem.at[k]).wait()
    summed = jnp.sum(norm_recv[...], axis=0)
    nodes = 3 * ex * ey * ez * total
    norms_ref[...] = jnp.sqrt(summed / nodes)


def on_device(counts, right_side, damage):
    _, ex, ey, ez = right_side.shape
    assert ez == LANES and ex * EDGE == LANES and 2 * EDGE * EDGE == LANES
    assert ex % BLOCK == 0 and ey == BLOCK and ex == BLOCK
    cz = ez // BLOCK
    wide_x = ex + 2 * HALO
    rows = ey + 2 * YPAD
    flat = wide_x * rows
    total = counts[0] * counts[1] * counts[2]
    window = 2 * (-(-COARSE // cz)) + 1
    coarse_rows = -(-(counts[1] + 1) // 8) * 8
    rounds = 0
    while window // 2 << rounds < counts[2] - 1:
        rounds += 1
    f32 = jnp.float32

    def vmem(*shape):
        return pltpu.VMEM(shape + (LANES,), f32)

    dma = pltpu.SemaphoreType.DMA
    near, layers = len(NEAR), len(LAYERS)
    displacement, norms = pl.pallas_call(
        functools.partial(kernel, counts, (ex, ey, ez)),
        out_shape=(
            pltpu.VMEM(right_side.shape, f32),
            pltpu.VMEM((1, LANES), f32),
        ),
        in_specs=[pl.BlockSpec(memory_space=pl.ANY)] * 2,
        out_specs=(
            pl.BlockSpec(memory_space=pltpu.VMEM),
            pl.BlockSpec(memory_space=pltpu.VMEM),
        ),
        scratch_shapes=[
            vmem(3, ex, ey),
            vmem(ex * ey),
            pltpu.VMEM((ex, ey, LANES), jnp.int32),
            vmem(4, flat),
            vmem(3, flat),
            vmem(3, flat),
            vmem(4, 3, rows),
            vmem(3, 3, rows),
            vmem(3, 3, rows),
            vmem(3, 3, 2 * rows),
            vmem(2, layers, ex),
            vmem(2, layers, ex),
            vmem(2, 2, near, 2),
            vmem(2, 2, near, 2),
            vmem(2, 2, layers, HALO),
            vmem(2, 2, layers, HALO),
            vmem(3, 4, rows),
            vmem(2, ey),
            vmem(2, 3, rows),
            vmem(2, 2, 4, 2),
            vmem(2, 2, 3, 4, 2),
            vmem(2, 2, 2, 2),
            vmem(2, 2, 2, 3, 2),
            vmem(4),
            vmem(window, counts[0] * counts[1], 4),
            vmem(counts[0] + 2, 3, 8 + coarse_rows),
            vmem(32),
            vmem(3, 9 * rows),
            vmem(3, 9 * rows),
            vmem(1),
            vmem(total, 1),
            vmem(4 * HALO * ey + ey, 1),
            dma((2,)),
            dma((len(DIRECTIONS),)),
            dma((len(DIRECTIONS),)),
            dma((len(FAR_DIRECTIONS),)),
            dma((window,)),
            dma((window,)),
            dma((2,)),
            pltpu.SemaphoreType.REGULAR((max(1, rounds), 2)),
        ],
        compiler_params=pltpu.CompilerParams(collective_id=0, has_side_effects=True),
    )(right_side, damage)
    return displacement, norms[0, :2]


def solution(mesh):
    counts = tuple(mesh.shape[axis] for axis in AXES)
    placed = (P(None, "gx", "gy", "gz"), P("gx", "gy", "gz"))
    return jax.shard_map(
        functools.partial(on_device, counts),
        mesh=mesh,
        in_specs=placed,
        out_specs=(P(None, "gx", "gy", "gz"), P()),
        check_vma=False,
    )
```

```python
import functools

import jax
import jax.numpy as jnp
from jax import lax
from jax.experimental import pallas as pl
from jax.experimental.pallas import tpu as pltpu
from jax.sharding import PartitionSpec as P

BLOCK = 16
COARSE = 8
FLOOR_STIFFNESS = 0.05
MASS_TERM = 0.001
COUPLING = 2.5
RELAXATION = 0.6
KEEP = 1.0 - RELAXATION
DIAGONAL = 6.0 + 2.0 * COUPLING
OWN = 1.0 + COUPLING
CROSS = 0.25 * COUPLING
AXES = ("gx", "gy", "gz")
HALO = 4
EDGE = 2 * HALO
LANES = 128
YPAD = 8
MESH = pl.DeviceIdType.MESH
EXACT = lax.Precision.HIGHEST
NEAR = ((0, 1), (1, 1), (2, 1), (3, 1), (0, 2), (1, 2), (2, 2))
FAR = ((3, 2), (0, 3), (1, 3), (2, 3), (3, 3), (0, 4), (1, 4), (2, 4))
LAYERS = NEAR + FAR


def directions():
    out = []
    for dx in (-1, 0, 1):
        for dy in (-1, 0, 1):
            for dz in (-1, 0, 1):
                if (dx, dy, dz) != (0, 0, 0):
                    out.append((dx, dy, dz))
    return sorted(out, key=lambda d: -sum(abs(step) for step in d))


DIRECTIONS = directions()


UNROLL = 24


def by_two(low, high, body, carry):
    trips = -(-(high - low) // UNROLL)
    size = -(-(high - low) // trips)
    whole = (high - low) // size

    def several(trip, carry):
        for k in range(size):
            carry = body(low + size * trip + k, carry)
        return carry

    if whole > 1:
        carry = lax.fori_loop(0, whole, several, carry)
    else:
        carry = several(0, carry)
    for k in range(low + whole * size, high):
        carry = body(k, carry)
    return carry


def kernel(
    counts,
    extent,
    load_ref,
    damage_ref,
    out_ref,
    norms_ref,
    raw,
    stiff,
    harm,
    base,
    field_a,
    field_b,
    edge_base,
    edge_a,
    edge_b,
    sides,
    y_send,
    y_recv,
    xyn_send,
    xyn_recv,
    xy_send,
    xy_recv,
    p_all,
    q_send,
    q_all,
    py_send,
    py_recv,
    qy_send,
    qy_recv,
    coarse_send,
    coarse_recv,
    coarse_w,
    stack_w,
    spread_w,
    image_w,
    norm_send,
    norm_recv,
    amount,
    local_sem,
    halo_sem,
    coarse_sem,
    norm_sem,
    hello_sem,
):
    count_x, count_y, count_z = counts
    ex, ey, ez = extent
    cz = ez // BLOCK
    total = count_x * count_y * count_z
    wide_x = ex + 2 * HALO
    ypad = YPAD
    rows = ey + 2 * ypad
    wide_y = ey + 2 * HALO
    first_y = ypad - HALO
    me = tuple(lax.axis_index(axis) for axis in AXES)
    my_id = (me[0] * count_y + me[1]) * count_z + me[2]

    def place(index):
        return (
            index // (count_y * count_z),
            lax.rem(index // count_z, count_y),
            lax.rem(index, count_z),
        )

    harm_copy = pltpu.make_async_copy(damage_ref, harm, local_sem.at[0])
    load_copy = pltpu.make_async_copy(load_ref, raw, local_sem.at[1])
    harm_copy.start()
    load_copy.start()
    barrier = pltpu.get_barrier_semaphore()

    reach = -(-COARSE // cz)
    window = 2 * reach + 1

    def around(here, count):
        out = [here]
        for step in range(1, count):
            there = here + step
            out.append(jnp.where(there >= count, there - count, there))
        return out

    ring_x, ring_y, ring_z = (around(me[axis], counts[axis]) for axis in range(3))

    def peers(act):
        for dz in sorted(range(-reach, reach + 1), key=lambda step: -abs(step)):
            z = me[2] + dz

            @pl.when((z >= 0) & (z < count_z))
            def _():
                for x in reversed(ring_x):
                    for y in reversed(ring_y):
                        if dz != 0 or x is not me[0] or y is not me[1]:
                            act(x, y, z, dz)

    def greet(x, y, z, dz):
        pl.semaphore_signal(barrier, inc=1, device_id=(x, y, z), device_id_type=MESH)

    peers(greet)
    levels = jnp.minimum(me[2] + reach, count_z - 1) - jnp.maximum(me[2] - reach, 0) + 1

    def exists(dx, dy, dz):
        ok = None
        for axis, step in enumerate((dx, dy, dz)):
            if step == 0:
                continue
            here = me[axis] + step
            good = (here >= 0) & (here < counts[axis])
            ok = good if ok is None else ok & good
        return ok

    def block(x):
        return pl.ds((HALO + x) * rows + ypad, ey)

    for xs in range(2):

        @pl.when(jnp.logical_not(exists(2 * xs - 1, 0, 0)))
        def _():
            for part in range(HALO):
                for f in range(4):
                    x = part - HALO if xs == 0 else ex + part
                    base[f, block(x)] = jnp.zeros((ey, LANES), jnp.float32)

        for ys in range(2):

            @pl.when(jnp.logical_not(exists(2 * xs - 1, 2 * ys - 1, 0)))
            def _():
                xyn_recv[xs, ys] = jnp.zeros((len(NEAR), 2, LANES), jnp.float32)
                xy_recv[xs, ys] = jnp.zeros((len(LAYERS), HALO, LANES), jnp.float32)

    for ys in range(2):

        @pl.when(jnp.logical_not(exists(0, 2 * ys - 1, 0)))
        def _():
            y_recv[ys] = jnp.zeros((len(LAYERS), ex, LANES), jnp.float32)

    lane_own = lax.broadcasted_iota(jnp.int32, (ey, LANES), 1)
    lane = lax.broadcasted_iota(jnp.int32, (wide_y, LANES), 1)
    row_y = lax.broadcasted_iota(jnp.int32, (wide_y, LANES), 0)
    lower = lax.rem(lane, EDGE) < HALO
    at_y = me[1] * ey + row_y - HALO
    good_y = (at_y >= 0) & (at_y < ey * count_y)
    has_back, has_front = me[2] > 0, me[2] < count_z - 1
    upper_x = lax.rem(lane // (HALO * EDGE), 2) == 0
    high_z = lane >= LANES // 2
    good_x = (upper_x & (me[0] < count_x - 1)) | (~upper_x & (me[0] > 0))
    good_z = (high_z & (lower | has_front)) | (~high_z & (~lower | has_back))
    goods = (
        good_y & (~lower | has_back),
        good_y & (lower | has_front),
        good_y & good_x & good_z,
    )

    def fold(value):
        return jnp.sum(value.reshape(ey // 8, 8, LANES), axis=0)

    zero = jnp.zeros((8, LANES), jnp.float32)

    harm_copy.wait()
    load_copy.wait()

    def own_rows(x):
        return pl.ds(x * ey, ey)

    load_sum = zero
    stiff_sum = zero
    packed = [None] * 4
    for x in range(ex):
        level = 1.0 - harm[x].astype(jnp.float32) / 15.0
        g = level * level * (1.0 - FLOOR_STIFFNESS) + FLOOR_STIFFNESS
        inv = RELAXATION / (g * DIAGONAL + MASS_TERM)
        stiff[own_rows(x)] = g
        stiff_sum = stiff_sum + fold(g)
        values = []
        squared = None
        for c in range(3):
            load = raw[c, x]
            values.append(load * inv)
            squared = load * load if squared is None else squared + load * load
        load_sum = load_sum + fold(squared)
        values.append(g * inv)
        for f in range(4):
            base[f, block(x)] = values[f]
            moved = pltpu.roll(values[f], (EDGE * x + HALO) % LANES, 1)
            packed[f] = moved if x == 0 else jnp.where(lane_own // EDGE == x, moved, packed[f])
    for f in range(4):
        p_all[1, f, pl.ds(ypad, ey)] = packed[f]
        for phase in range(2):
            py_send[phase, 0, f] = packed[f][2 * phase : 2 * phase + 2]
            py_send[phase, 1, f] = packed[f][ey - 2 - 2 * phase : ey - 2 * phase]
    width = HALO * EDGE
    for xs in range(2):
        joined = None
        for f in range(4):
            shift = width * f - (0 if xs == 0 else (ex - HALO) * EDGE)
            moved = pltpu.roll(packed[f], shift % LANES, 1)
            joined = moved if f == 0 else jnp.where(lane_own // width == f, moved, joined)
        q_send[xs] = joined
        for phase in range(2):
            qy_send[phase, xs, 0] = joined[2 * phase : 2 * phase + 2]
            qy_send[phase, xs, 1] = joined[ey - 2 - 2 * phase : ey - 2 * phase]
    for side in range(2):
        for i, (f, layer) in enumerate(LAYERS):
            start = HALO * rows + ypad + (layer - 1 if side == 0 else ey - layer)
            for half in range(ex // 8):
                y_send[side, i, pl.ds(8 * half, 8)] = base[
                    f, pl.ds(start + 8 * half * rows, 8, stride=rows)
                ]
            for xs in range(2):
                x0 = 0 if xs == 0 else ex - HALO
                xy_send[xs, side, i] = base[f, pl.ds(start + x0 * rows, HALO, stride=rows)]
                if i < len(NEAR):
                    x0 = 0 if xs == 0 else ex - 2
                    xyn_send[xs, side, i] = base[f, pl.ds(start + x0 * rows, 2, stride=rows)]

    pl.semaphore_wait(barrier, levels * count_x * count_y - 1)

    def pieces(d, phase):
        dx, dy, dz = d
        xs, ys = (dx + 1) // 2, (dy + 1) // 2
        out = []
        near, far = pl.ds(0, len(NEAR)), pl.ds(len(NEAR), len(FAR))
        own = pl.ds(ypad, ey)
        if dy == 0:
            if phase == 1:
                return out
            if dz == 0:
                for part in range(HALO):
                    src_x = part if dx < 0 else ex - HALO + part
                    dst_x = ex + part if dx < 0 else part - HALO
                    out.append((base.at[:, block(src_x)], base.at[:, block(dst_x)], 4 * ey))
            if dx == 0:
                out.append((p_all.at[1, :, own], p_all.at[1 - dz, :, own], 4 * ey))
            else:
                out.append((q_send.at[xs], q_all.at[1 - xs, 1 - dz, own], ey))
            return out
        if dx == 0:
            out.append((py_send.at[phase, ys], py_recv.at[phase, 1 - ys, 1 - dz], 8))
        else:
            out.append((qy_send.at[phase, xs, ys], qy_recv.at[phase, 1 - xs, 1 - ys, 1 - dz], 2))
        if dz == 0 and dx == 0:
            part = near if phase == 0 else far
            size = len(NEAR) if phase == 0 else len(FAR)
            out.append((y_send.at[ys, part], y_recv.at[1 - ys, part], size * ex))
        elif dz == 0 and phase == 0:
            out.append((xyn_send.at[xs, ys], xyn_recv.at[1 - xs, 1 - ys], 2 * len(NEAR)))
        elif dz == 0:
            out.append((xy_send.at[xs, ys], xy_recv.at[1 - xs, 1 - ys], HALO * len(LAYERS)))
        return out

    def start_sends(phase):
        odd = lax.rem(me[1], 2) == 1
        ordered = []
        for turn_number in range(2):
            for number, d in enumerate(DIRECTIONS):
                if d[1] != 0:
                    ordered.append((number, d, odd == ((d[1] > 0) == (turn_number == 0))))
        ordered += [(number, d, None) for number, d in enumerate(DIRECTIONS) if d[1] == 0]
        for number, d, condition in ordered:
            parts = pieces(d, phase)
            if not parts:
                continue

            @pl.when(exists(*d) if condition is None else exists(*d) & condition)
            def _():
                for src, dst, _ in parts:
                    pltpu.make_async_remote_copy(
                        src_ref=src,
                        dst_ref=dst,
                        send_sem=halo_sem.at[2],
                        recv_sem=halo_sem.at[phase],
                        device_id=tuple(me[axis] + d[axis] for axis in range(3)),
                        device_id_type=MESH,
                    ).start()

    start_sends(0)
    start_sends(1)

    def wait_bytes(size, sem):
        span = amount.at[pl.ds(0, size)]
        pltpu.make_async_copy(span, span, sem).wait()

    sides_of = [
        (here > 0).astype(jnp.int32) + (here < count - 1).astype(jnp.int32)
        for here, count in zip(me, counts)
    ]
    most = [min(2, count - 1) for count in counts]

    def wait_halo(phases, sem):
        for number_x in range(min(1, most[0]), most[0] + 1):
            for number_y in range(min(1, most[1]), most[1] + 1):
                for number_z in range(min(1, most[2]), most[2] + 1):
                    have = (number_x, number_y, number_z)
                    size = 0
                    for d in DIRECTIONS:
                        if d == tuple(-abs(step) for step in d):
                            times = 1
                            for step, number in zip(d, have):
                                times *= number if step else 1
                            for phase in phases:
                                size += times * sum(part[2] for part in pieces(d, phase))

                    @pl.when(
                        (sides_of[0] == number_x)
                        & (sides_of[1] == number_y)
                        & (sides_of[2] == number_z)
                    )
                    def _():
                        wait_bytes(size, sem)

    rounds = []
    radius = reach
    while radius < count_z - 1:
        rounds.append(radius)
        radius *= 2

    def hello(number):
        for side, step in enumerate((-rounds[number], rounds[number])):

            @pl.when(exists(0, 0, step))
            def _():
                pl.semaphore_signal(
                    hello_sem.at[number, 1 - side],
                    inc=1,
                    device_id=(me[0], me[1], me[2] + step),
                    device_id_type=MESH,
                )

    def hear(number):
        for side, step in enumerate((-rounds[number], rounds[number])):

            @pl.when(exists(0, 0, step))
            def _():
                pl.semaphore_wait(hello_sem.at[number, side], 1)

    if rounds:
        hello(0)

    def unpack(phase):
        for side in range(2):
            for i, (f, layer) in enumerate(LAYERS):
                y = ypad - layer if side == 0 else ypad + ey + layer - 1
                if (i < len(NEAR)) == (phase == 0):
                    for half in range(ex // 8):
                        base[f, pl.ds((HALO + 8 * half) * rows + y, 8, stride=rows)] = y_recv[
                            side, i, pl.ds(8 * half, 8)
                        ]
                for xs in range(2):
                    if phase == 1:
                        x0 = 0 if xs == 0 else HALO + ex
                        base[f, pl.ds(x0 * rows + y, HALO, stride=rows)] = xy_recv[xs, side, i]
                    elif i < len(NEAR):
                        x0 = HALO - 2 if xs == 0 else HALO + ex
                        base[f, pl.ds(x0 * rows + y, 2, stride=rows)] = xyn_recv[xs, side, i]
            start = ypad - 2 - 2 * phase if side == 0 else ypad + ey + 2 * phase
            for dz in range(3):
                for f in range(4):
                    p_all[dz, f, pl.ds(start, 2)] = py_recv[phase, side, dz, f]
                for xs in range(2):
                    q_all[xs, dz, pl.ds(start, 2)] = qy_recv[phase, xs, side, dz]
        wide = pl.ds(first_y, wide_y)
        for f in range(4):
            back, here, front = (p_all[dz, f, wide] for dz in range(3))
            edge_base[f, 0, wide] = jnp.where(goods[0], jnp.where(lower, back, here), 0.0)
            edge_base[f, 1, wide] = jnp.where(goods[1], jnp.where(lower, here, front), 0.0)
        low, high = [], []
        for xs in range(2):
            back, here, front = (q_all[xs, dz, wide] for dz in range(3))
            low.append(jnp.where(lower, back, here))
            high.append(jnp.where(lower, here, front))
        for f in range(4):
            quarter = [
                pltpu.roll(value, (width * (k - f)) % LANES, 1)
                for k, value in enumerate((low[1], low[0], high[1], high[0]))
            ]
            merged = jnp.where(
                high_z,
                jnp.where(upper_x, quarter[2], quarter[3]),
                jnp.where(upper_x, quarter[0], quarter[1]),
            )
            edge_base[f, 2, wide] = jnp.where(goods[2], merged, 0.0)

    def at(p, dy=0, own=False):
        if own:
            return pl.ds(p * rows + ypad + dy, ey)
        return pl.ds(p * rows + first_y + dy, wide_y)

    cell = lane // EDGE
    last_cell = cell == LANES // EDGE - 1
    first_cell = cell == 0
    half_cell = LANES // EDGE // 2

    def turn(value, step):
        return pltpu.roll(value, step % LANES, 1)

    def edge_shift(values, step):
        low, high, outer = values
        near = [turn(value, -step * EDGE) for value in values]
        half = LANES // 2
        if step > 0:
            return [
                jnp.where(last_cell, near[2], near[0]),
                jnp.where(last_cell, turn(outer, half - EDGE), near[1]),
                jnp.where(
                    last_cell,
                    near[1],
                    jnp.where(cell == half_cell - 1, turn(low, half - EDGE), near[2]),
                ),
            ]
        return [
            jnp.where(first_cell, turn(outer, half + EDGE), near[0]),
            jnp.where(first_cell, near[2], near[1]),
            jnp.where(
                first_cell, near[0], jnp.where(cell == half_cell, turn(high, half + EDGE), near[2])
            ),
        ]

    def edge_stage(field, stage, sums=True):
        wide = pl.ds(first_y, wide_y)

        def load(c, oy):
            return [field[c, k, pl.ds(first_y + oy, wide_y)] for k in range(3)]

        centre = [load(c, 0) for c in range(3)]
        y_up = [load(c, 1) for c in range(3)]
        y_down = [load(c, -1) for c in range(3)]
        slope = [[CROSS * (y_up[c][k] - y_down[c][k]) for k in range(3)] for c in range(3)]
        used = range(3) if sums else (0, 2)
        x_up = {c: edge_shift(centre[c], 1) for c in used}
        x_down = {c: edge_shift(centre[c], -1) for c in used}
        ups, downs = [], []
        for k in range(3):
            tilt = [
                CROSS * (x_up[2][k] - x_down[2][k]),
                slope[2][k],
                CROSS * (x_up[0][k] - x_down[0][k]) + slope[1][k],
            ]
            mine = [centre[0][k], centre[1][k], OWN * centre[2][k]]
            ups.append([mine[c] + tilt[c] for c in range(3)])
            downs.append([mine[c] - tilt[c] for c in range(3)])
        front = lax.rem(lane, EDGE) == HALO
        for c in range(3):
            sides[stage, c, pl.ds(first_y, wide_y)] = jnp.where(front, ups[1][c], turn(downs[0][c], 2))
            sides[stage, c, pl.ds(rows + first_y, wide_y)] = jnp.where(
                front, turn(ups[2][c], LANES // 2), turn(downs[2][c], 2)
            )
        if not sums:
            return None
        slope_up = [edge_shift(slope[c], 1) for c in range(2)]
        slope_down = [edge_shift(slope[c], -1) for c in range(2)]
        out = []
        for k in range(3):
            sum_x = [x_up[c][k] + x_down[c][k] for c in range(3)]
            sum_y = [y_up[c][k] + y_down[c][k] for c in range(3)]
            sum_z = [turn(ups[k][c], -1) + turn(downs[k][c], 1) for c in range(3)]
            out.append(
                [
                    OWN * sum_x[0] + sum_y[0] + (slope_up[1][k] - slope_down[1][k]) + sum_z[0],
                    sum_x[1] + OWN * sum_y[1] + (slope_up[0][k] - slope_down[0][k]) + sum_z[1],
                    sum_x[2] + sum_y[2] + sum_z[2],
                ]
            )
        return out

    def edge_sweep(source, target, stage):
        beside = edge_stage(source, stage)
        wide = pl.ds(first_y, wide_y)
        for k in range(3):
            share = edge_base[3, k, wide]
            for c in range(3):
                target[c, k, wide] = (
                    KEEP * source[c, k, wide] + edge_base[c, k, wide] + share * beside[k][c]
                )

    def neighbours(field, p, x, stage, own=False):
        def load(c, ox, oy):
            return field[c, at(p + ox, oy, own)]

        if isinstance(x, int):
            ring = (x + 2 * HALO) % wide_x
            outside = ring < 2 * HALO
            where_x = ring if outside else ring - 2 * HALO
            shift = (LANES - 1 - HALO - EDGE * where_x) % LANES
            start = (rows if outside else 0) + (ypad if own else first_y)
        else:
            ring = lax.rem(x + 2 * HALO, wide_x)
            outside = ring < 2 * HALO
            where_x = jnp.where(outside, ring, ring - 2 * HALO)
            shift = lax.rem(2 * LANES - 1 - HALO - EDGE * where_x, LANES)
            start = jnp.where(outside, rows, 0) + (ypad if own else first_y)
        height = ey if own else wide_y
        centre = [load(c, 0, 0) for c in range(3)]
        x_up = [load(c, 1, 0) for c in range(3)]
        x_down = [load(c, -1, 0) for c in range(3)]
        y_up = [load(c, 0, 1) for c in range(3)]
        y_down = [load(c, 0, -1) for c in range(3)]
        slope = [CROSS * (y_up[c] - y_down[c]) for c in range(3)]
        corner = [
            CROSS * (load(c, 1, 1) - load(c, 1, -1)) - CROSS * (load(c, -1, 1) - load(c, -1, -1))
            for c in range(2)
        ]
        tilt = [
            CROSS * (x_up[2] - x_down[2]),
            slope[2],
            CROSS * (x_up[0] - x_down[0]) + slope[1],
        ]
        mine = [centre[0], centre[1], OWN * centre[2]]
        lanes = lax.broadcasted_iota(jnp.int32, (height, LANES), 1)
        sum_z = []
        for c in range(3):
            end = pltpu.roll(sides[stage, c, pl.ds(start, height)], shift, 1)
            up = jnp.where(lanes == LANES - 1, end, turn(mine[c] + tilt[c], -1))
            down = jnp.where(lanes == 0, end, turn(mine[c] - tilt[c], 1))
            sum_z.append(up + down)
        return [
            OWN * (x_up[0] + x_down[0]) + (y_up[0] + y_down[0]) + corner[1] + sum_z[0],
            (x_up[1] + x_down[1]) + OWN * (y_up[1] + y_down[1]) + corner[0] + sum_z[1],
            (x_up[2] + x_down[2]) + (y_up[2] + y_down[2]) + sum_z[2],
        ]

    def sweep(source, target, low, high, stage):
        def one(p, carry):
            beside = neighbours(source, p, p - HALO, stage)
            share = base[3, at(p)]
            for c in range(3):
                target[c, at(p)] = KEEP * source[c, at(p)] + base[c, at(p)] + share * beside[c]
            return carry

        by_two(low, high, one, 0)

    def residual(field, x, stage):
        p = x + HALO
        beside = neighbours(field, p, x, stage, True)
        g = stiff[own_rows(x)]
        heavy = g * DIAGONAL + MASS_TERM
        return [
            raw[c, x] - heavy * field[c, at(p, 0, True)] + g * beside[c] for c in range(3)
        ]

    wait_halo((0,), halo_sem.at[0])
    greeted = min(1, len(rounds) - 1)
    for number in range(greeted):
        hear(number)
        hello(number + 1)
    unpack(0)
    edge_sweep(edge_base, edge_a, 0)
    edge_stage(edge_a, 1, False)
    sweep(base, field_b, HALO - 1, HALO + ex + 1, 0)

    def restrict(x, carry):
        left = residual(field_b, x, 1)
        return tuple(carry[c] + left[c] for c in range(3))

    sums = by_two(0, ex, restrict, (jnp.zeros((ey, LANES), jnp.float32),) * 3)
    sums = [fold(s) for s in sums] + [stiff_sum]
    stacked = jnp.concatenate([jnp.sum(s, axis=0, keepdims=True) for s in sums] + [zero[:4]], axis=0)
    source_lane = lax.broadcasted_iota(jnp.int32, (LANES, LANES), 0)
    target_lane = lax.broadcasted_iota(jnp.int32, (LANES, LANES), 1)
    gather = (source_lane // BLOCK == lax.rem(target_lane, cz)).astype(jnp.float32)
    grouped = jnp.dot(stacked, gather, precision=EXACT, preferred_element_type=jnp.float32)
    coarse_send[...] = grouped[:4]

    def coarse_copy(x, y, z, dz):
        return pltpu.make_async_remote_copy(
            src_ref=coarse_send,
            dst_ref=coarse_recv.at[reach - dz, me[0] * count_y + me[1]],
            send_sem=coarse_sem.at[0],
            recv_sem=coarse_sem.at[1],
            device_id=(x, y, z),
            device_id_type=MESH,
        )

    def coarse_wait():
        for number in range(1, window + 1):

            @pl.when(levels == number)
            def _():
                for k in range(2):
                    wait_bytes(4 * (number * count_x * count_y - 1), coarse_sem.at[k])

    peers(lambda x, y, z, dz: coarse_copy(x, y, z, dz).start())
    coarse_recv[reach, me[0] * count_y + me[1]] = grouped[:4]

    wait_halo((1,), halo_sem.at[1])
    unpack(1)
    edge_sweep(edge_base, edge_a, 0)
    edge_sweep(edge_a, edge_b, 1)
    sweep(base, field_a, 1, wide_x - 1, 0)
    sweep(field_a, field_b, 2, wide_x - 2, 1)
    wait_halo((0, 1), halo_sem.at[2])
    coarse_wait()

    coarse_rows = -(-(count_y + 1) // 8) * 8
    lane_c = lax.broadcasted_iota(jnp.int32, (coarse_rows, LANES), 1)
    row_c = lax.broadcasted_iota(jnp.int32, (coarse_rows, LANES), 0)
    at_z = me[2] * cz - reach * cz + lane_c
    valid = (
        (row_c < count_y) & (at_z >= 0) & (at_z < cz * count_z) & (lane_c < window * cz)
    )
    slab = [[None] * 4 for _ in range(count_x)]
    for x in range(count_x):
        for c in range(4):
            value = None
            for w in range(window):
                column = jnp.concatenate(
                    [coarse_recv[w, x * count_y + y, c : c + 1] for y in range(count_y)]
                    + [jnp.zeros((coarse_rows - count_y, LANES), jnp.float32)],
                    axis=0,
                )
                value = column if value is None else jnp.where(lane_c // cz == w, column, value)
            slab[x][c] = jnp.where(valid, value, 0.0)
    mass = BLOCK**3 * MASS_TERM
    factor = [slab[x][3] * (BLOCK**2 / BLOCK**3) for x in range(count_x)]
    relax = [
        jnp.where(valid, RELAXATION / (factor[x] * DIAGONAL + mass), 0.0) for x in range(count_x)
    ]
    nothing = jnp.zeros((coarse_rows, LANES), jnp.float32)
    start_w = [[slab[x][c] * relax[x] for c in range(3)] for x in range(count_x)]
    share_w = [factor[x] * relax[x] for x in range(count_x)]
    w = start_w

    def y_shift(value, step):
        return pltpu.roll(value, step % coarse_rows, 0)

    for repeat in range(COARSE - 1):
        fresh = []
        for x in range(count_x):
            here = w[x]
            above = w[x + 1] if x + 1 < count_x else [nothing] * 3
            below = w[x - 1] if x > 0 else [nothing] * 3
            sum_x = [above[c] + below[c] for c in range(3)]
            diff_x = [above[c] - below[c] for c in range(3)]
            y_up = [y_shift(here[c], -1) for c in range(3)]
            y_down = [y_shift(here[c], 1) for c in range(3)]
            sum_y = [y_up[c] + y_down[c] for c in range(3)]
            diff_y = [y_up[c] - y_down[c] for c in range(3)]
            corner_x = y_shift(diff_x[1], -1) - y_shift(diff_x[1], 1)
            corner_y = y_shift(diff_x[0], -1) - y_shift(diff_x[0], 1)
            tilt = [CROSS * diff_x[2], CROSS * diff_y[2], CROSS * (diff_x[0] + diff_y[1])]
            own = [here[0], here[1], OWN * here[2]]
            sum_z = [turn(own[c] + tilt[c], -1) + turn(own[c] - tilt[c], 1) for c in range(3)]
            beside = [
                OWN * sum_x[0] + sum_y[0] + CROSS * corner_x + sum_z[0],
                sum_x[1] + OWN * sum_y[1] + CROSS * corner_y + sum_z[1],
                sum_x[2] + sum_y[2] + sum_z[2],
            ]
            fresh.append(
                [
                    KEEP * here[c] + start_w[x][c] + share_w[x] * beside[c]
                    for c in range(3)
                ]
            )
        w = fresh

    for x in range(count_x + 2):
        for c in range(3):
            inside = 1 <= x <= count_x
            coarse_w[x, c, pl.ds(0, 8)] = jnp.zeros((8, LANES), jnp.float32)
            coarse_w[x, c, pl.ds(8, coarse_rows)] = w[x - 1][c] if inside else nothing
    stack_w[pl.ds(24, 8)] = zero
    for xc in range(3):
        for c in range(3):
            stack_w[pl.ds(3 * (3 * xc + c), 3)] = coarse_w[me[0] + xc, c, pl.ds(7 + me[1], 3)]
    inner = lax.rem(target_lane, EDGE) < HALO
    first_cell_z, last_cell_z = reach * cz, (reach + 1) * cz - 1
    pick_low = jnp.where(inner, first_cell_z - 1, first_cell_z)
    pick_high = jnp.where(inner, last_cell_z, last_cell_z + 1)
    picks = (
        first_cell_z + target_lane // BLOCK,
        pick_low,
        pick_high,
        jnp.where(target_lane < LANES // 2, pick_low, pick_high),
    )
    widen = jnp.concatenate([(source_lane == pick).astype(jnp.float32) for pick in picks], axis=1)
    wide_all = jnp.dot(stack_w[...], widen, precision=EXACT, preferred_element_type=jnp.float32)

    def drawn(xc, c, k):
        parts = []
        for j in range(3):
            line = 3 * (3 * xc + c) + j
            piece = wide_all[line : line + 1, k * LANES : (k + 1) * LANES]
            parts.append(jnp.broadcast_to(piece, (wide_y, LANES)))
        return jnp.where(row_y < HALO, parts[0], jnp.where(row_y < HALO + ey, parts[1], parts[2]))

    wide = pl.ds(first_y, wide_y)
    for c in range(3):
        for xc in range(3):
            value = drawn(xc, c, 0)
            for plane in range(3):
                spread_w[c, pl.ds((3 * xc + plane) * rows + first_y, wide_y)] = value
        edge_a[c, 0, wide] = drawn(1, c, 1)
        edge_a[c, 1, wide] = drawn(1, c, 2)
        edge_a[c, 2, wide] = jnp.where(upper_x, drawn(2, c, 3), drawn(0, c, 3))
    beside = edge_stage(edge_a, 0)
    for k in range(3):
        share = edge_base[3, k, wide]
        for c in range(3):
            edge_b[c, k, wide] = (
                edge_b[c, k, wide] + KEEP * edge_a[c, k, wide] + share * beside[k][c]
            )
    edge_sweep(edge_b, edge_a, 1)
    edge_stage(edge_a, 2, False)
    for plane, x in ((1, -2), (2, -1), (3, 0), (4, ex // 2), (5, ex - 1), (6, ex), (7, ex + 1)):
        images = neighbours(spread_w, plane, x, 0)
        for c in range(3):
            image_w[c, at(plane)] = images[c]

    def correct(p, carry):
        kind = (
            jnp.int32(1)
            + jnp.int32(p >= HALO - 1)
            + jnp.int32(p >= HALO)
            + jnp.int32(p >= HALO + 1)
            + jnp.int32(p >= HALO + ex - 1)
            + jnp.int32(p >= HALO + ex)
            + jnp.int32(p >= HALO + ex + 1)
        )
        share = base[3, at(p)]
        for c in range(3):
            field_b[c, at(p)] = (
                field_b[c, at(p)] + KEEP * spread_w[c, at(kind)] + share * image_w[c, at(kind)]
            )
        return carry

    by_two(2, wide_x - 2, correct, 0)
    sweep(field_b, field_a, 3, wide_x - 3, 1)

    def squares(x, carry):
        left = residual(field_a, x, 2)
        for c in range(3):
            out_ref[c, x] = field_a[c, at(x + HALO, 0, True)]
        return carry + fold(sum(value * value for value in left))

    left_sum = by_two(0, ex, squares, zero)
    load_total = jnp.sum(jnp.sum(load_sum, axis=0, keepdims=True), axis=1, keepdims=True)
    left_total = jnp.sum(jnp.sum(left_sum, axis=0, keepdims=True), axis=1, keepdims=True)
    first = lax.broadcasted_iota(jnp.int32, (1, LANES), 1) == 0
    mine = jnp.where(first, load_total, left_total)
    norm_send[...] = mine

    for number in range(greeted, len(rounds)):
        if number > greeted:
            hello(number)
        hear(number)
    for x in reversed(ring_x):
        for z in reversed(ring_z):
            for y in reversed(ring_y):
                if x is not me[0] or y is not me[1] or z is not me[2]:
                    pltpu.make_async_remote_copy(
                        src_ref=norm_send,
                        dst_ref=norm_recv.at[my_id],
                        send_sem=norm_sem.at[0],
                        recv_sem=norm_sem.at[1],
                        device_id=(x, y, z),
                        device_id_type=MESH,
                    ).start()
    norm_recv[my_id] = mine
    others = norm_recv.at[pl.ds(0, total - 1)]
    for k in range(2):
        pltpu.make_async_copy(others, others, norm_sem.at[k]).wait()
    summed = jnp.sum(norm_recv[...], axis=0)
    nodes = 3 * ex * ey * ez * total
    norms_ref[...] = jnp.sqrt(summed / nodes)


def on_device(counts, right_side, damage):
    _, ex, ey, ez = right_side.shape
    assert ez == LANES and ex * EDGE == LANES and 2 * EDGE * EDGE == LANES
    assert ex % BLOCK == 0 and ey == BLOCK and ex == BLOCK
    cz = ez // BLOCK
    wide_x = ex + 2 * HALO
    rows = ey + 2 * YPAD
    flat = wide_x * rows
    total = counts[0] * counts[1] * counts[2]
    window = 2 * (-(-COARSE // cz)) + 1
    coarse_rows = -(-(counts[1] + 1) // 8) * 8
    rounds = 0
    while window // 2 << rounds < counts[2] - 1:
        rounds += 1
    f32 = jnp.float32

    def vmem(*shape):
        return pltpu.VMEM(shape + (LANES,), f32)

    dma = pltpu.SemaphoreType.DMA
    near, layers = len(NEAR), len(LAYERS)
    displacement, norms = pl.pallas_call(
        functools.partial(kernel, counts, (ex, ey, ez)),
        out_shape=(
            pltpu.VMEM(right_side.shape, f32),
            pltpu.VMEM((1, LANES), f32),
        ),
        in_specs=[pl.BlockSpec(memory_space=pl.ANY)] * 2,
        out_specs=(
            pl.BlockSpec(memory_space=pltpu.VMEM),
            pl.BlockSpec(memory_space=pltpu.VMEM),
        ),
        scratch_shapes=[
            vmem(3, ex, ey),
            vmem(ex * ey),
            pltpu.VMEM((ex, ey, LANES), jnp.int32),
            vmem(4, flat),
            vmem(3, flat),
            vmem(3, flat),
            vmem(4, 3, rows),
            vmem(3, 3, rows),
            vmem(3, 3, rows),
            vmem(3, 3, 2 * rows),
            vmem(2, layers, ex),
            vmem(2, layers, ex),
            vmem(2, 2, near, 2),
            vmem(2, 2, near, 2),
            vmem(2, 2, layers, HALO),
            vmem(2, 2, layers, HALO),
            vmem(3, 4, rows),
            vmem(2, ey),
            vmem(2, 3, rows),
            vmem(2, 2, 4, 2),
            vmem(2, 2, 3, 4, 2),
            vmem(2, 2, 2, 2),
            vmem(2, 2, 2, 3, 2),
            vmem(4),
            vmem(window, counts[0] * counts[1], 4),
            vmem(counts[0] + 2, 3, 8 + coarse_rows),
            vmem(32),
            vmem(3, 9 * rows),
            vmem(3, 9 * rows),
            vmem(1),
            vmem(total, 1),
            vmem(4 * EDGE * LANES, 1),
            dma((2,)),
            dma((3,)),
            dma((2,)),
            dma((2,)),
            pltpu.SemaphoreType.REGULAR((max(1, rounds), 2)),
        ],
        compiler_params=pltpu.CompilerParams(collective_id=0, has_side_effects=True),
    )(right_side, damage)
    return displacement, norms[0, :2]


def solution(mesh):
    counts = tuple(mesh.shape[axis] for axis in AXES)
    placed = (P(None, "gx", "gy", "gz"), P("gx", "gy", "gz"))
    return jax.shard_map(
        functools.partial(on_device, counts),
        mesh=mesh,
        in_specs=placed,
        out_specs=(P(None, "gx", "gy", "gz"), P()),
        check_vma=False,
    )
```

```python
import functools

import jax
import jax.numpy as jnp
from jax import lax
from jax.experimental import pallas as pl
from jax.experimental.pallas import tpu as pltpu
from jax.sharding import PartitionSpec as P

BLOCK = 16
COARSE = 8
FLOOR_STIFFNESS = 0.05
MASS_TERM = 0.001
COUPLING = 2.5
RELAXATION = 0.6
KEEP = 1.0 - RELAXATION
DIAGONAL = 6.0 + 2.0 * COUPLING
OWN = 1.0 + COUPLING
CROSS = 0.25 * COUPLING
AXES = ("gx", "gy", "gz")
HALO = 4
EDGE = 2 * HALO
LANES = 128
YPAD = 8
MESH = pl.DeviceIdType.MESH
EXACT = lax.Precision.HIGHEST
NEAR = ((0, 1), (1, 1), (2, 1), (3, 1), (0, 2), (1, 2), (2, 2))
FAR = ((3, 2), (0, 3), (1, 3), (2, 3), (3, 3), (0, 4), (1, 4), (2, 4))
LAYERS = NEAR + FAR


def directions():
    out = []
    for dx in (-1, 0, 1):
        for dy in (-1, 0, 1):
            for dz in (-1, 0, 1):
                if (dx, dy, dz) != (0, 0, 0):
                    out.append((dx, dy, dz))
    return sorted(out, key=lambda d: -sum(abs(step) for step in d))


DIRECTIONS = directions()


UNROLL = 24


def by_two(low, high, body, carry):
    trips = -(-(high - low) // UNROLL)
    size = -(-(high - low) // trips)
    whole = (high - low) // size

    def several(trip, carry):
        for k in range(size):
            carry = body(low + size * trip + k, carry)
        return carry

    if whole > 1:
        carry = lax.fori_loop(0, whole, several, carry)
    else:
        carry = several(0, carry)
    for k in range(low + whole * size, high):
        carry = body(k, carry)
    return carry


def kernel(
    counts,
    extent,
    load_ref,
    damage_ref,
    out_ref,
    norms_ref,
    raw,
    stiff,
    harm,
    base,
    field_a,
    field_b,
    edge_base,
    edge_a,
    edge_b,
    sides,
    swung,
    y_send,
    y_recv,
    xyn_send,
    xyn_recv,
    xy_send,
    xy_recv,
    p_all,
    q_send,
    q_all,
    py_send,
    py_recv,
    qy_send,
    qy_recv,
    coarse_send,
    coarse_recv,
    coarse_w,
    stack_w,
    spread_w,
    image_w,
    norm_send,
    norm_recv,
    amount,
    local_sem,
    halo_sem,
    coarse_sem,
    norm_sem,
    hello_sem,
):
    count_x, count_y, count_z = counts
    ex, ey, ez = extent
    cz = ez // BLOCK
    total = count_x * count_y * count_z
    wide_x = ex + 2 * HALO
    ypad = YPAD
    rows = ey + 2 * ypad
    wide_y = ey + 2 * HALO
    first_y = ypad - HALO
    me = tuple(lax.axis_index(axis) for axis in AXES)
    my_id = (me[0] * count_y + me[1]) * count_z + me[2]

    def place(index):
        return (
            index // (count_y * count_z),
            lax.rem(index // count_z, count_y),
            lax.rem(index, count_z),
        )

    harm_copy = pltpu.make_async_copy(damage_ref, harm, local_sem.at[0])
    load_copy = pltpu.make_async_copy(load_ref, raw, local_sem.at[1])
    harm_copy.start()
    load_copy.start()
    barrier = pltpu.get_barrier_semaphore()

    reach = -(-COARSE // cz)
    window = 2 * reach + 1

    def around(here, count):
        out = [here]
        for step in range(1, count):
            there = here + step
            out.append(jnp.where(there >= count, there - count, there))
        return out

    ring_x, ring_y, ring_z = (around(me[axis], counts[axis]) for axis in range(3))

    def peers(act):
        for dz in sorted(range(-reach, reach + 1), key=lambda step: -abs(step)):
            z = me[2] + dz

            @pl.when((z >= 0) & (z < count_z))
            def _():
                for x in reversed(ring_x):
                    for y in reversed(ring_y):
                        if dz != 0 or x is not me[0] or y is not me[1]:
                            act(x, y, z, dz)

    def greet(x, y, z, dz):
        pl.semaphore_signal(barrier, inc=1, device_id=(x, y, z), device_id_type=MESH)

    peers(greet)
    levels = jnp.minimum(me[2] + reach, count_z - 1) - jnp.maximum(me[2] - reach, 0) + 1

    def exists(dx, dy, dz):
        ok = None
        for axis, step in enumerate((dx, dy, dz)):
            if step == 0:
                continue
            here = me[axis] + step
            good = (here >= 0) & (here < counts[axis])
            ok = good if ok is None else ok & good
        return ok

    def block(x):
        return pl.ds((HALO + x) * rows + ypad, ey)

    for xs in range(2):

        @pl.when(jnp.logical_not(exists(2 * xs - 1, 0, 0)))
        def _():
            for part in range(HALO):
                for f in range(4):
                    x = part - HALO if xs == 0 else ex + part
                    base[f, block(x)] = jnp.zeros((ey, LANES), jnp.float32)

        for ys in range(2):

            @pl.when(jnp.logical_not(exists(2 * xs - 1, 2 * ys - 1, 0)))
            def _():
                xyn_recv[xs, ys] = jnp.zeros((len(NEAR), 2, LANES), jnp.float32)
                xy_recv[xs, ys] = jnp.zeros((len(LAYERS), HALO, LANES), jnp.float32)

    for ys in range(2):

        @pl.when(jnp.logical_not(exists(0, 2 * ys - 1, 0)))
        def _():
            y_recv[ys] = jnp.zeros((len(LAYERS), ex, LANES), jnp.float32)

    lane_own = lax.broadcasted_iota(jnp.int32, (ey, LANES), 1)
    lane = lax.broadcasted_iota(jnp.int32, (wide_y, LANES), 1)
    row_y = lax.broadcasted_iota(jnp.int32, (wide_y, LANES), 0)
    lower = lax.rem(lane, EDGE) < HALO
    at_y = me[1] * ey + row_y - HALO
    good_y = (at_y >= 0) & (at_y < ey * count_y)
    has_back, has_front = me[2] > 0, me[2] < count_z - 1
    upper_x = lax.rem(lane // (HALO * EDGE), 2) == 0
    high_z = lane >= LANES // 2
    good_x = (upper_x & (me[0] < count_x - 1)) | (~upper_x & (me[0] > 0))
    good_z = (high_z & (lower | has_front)) | (~high_z & (~lower | has_back))
    goods = (
        good_y & (~lower | has_back),
        good_y & (lower | has_front),
        good_y & good_x & good_z,
    )

    def fold(value):
        return jnp.sum(value.reshape(ey // 8, 8, LANES), axis=0)

    zero = jnp.zeros((8, LANES), jnp.float32)

    harm_copy.wait()
    load_copy.wait()

    def own_rows(x):
        return pl.ds(x * ey, ey)

    load_sum = zero
    stiff_sum = zero
    packed = [None] * 4
    for x in range(ex):
        level = 1.0 - harm[x].astype(jnp.float32) / 15.0
        g = level * level * (1.0 - FLOOR_STIFFNESS) + FLOOR_STIFFNESS
        inv = RELAXATION / (g * DIAGONAL + MASS_TERM)
        stiff[own_rows(x)] = g
        stiff_sum = stiff_sum + fold(g)
        values = []
        squared = None
        for c in range(3):
            load = raw[c, x]
            values.append(load * inv)
            squared = load * load if squared is None else squared + load * load
        load_sum = load_sum + fold(squared)
        values.append(g * inv)
        for f in range(4):
            base[f, block(x)] = values[f]
            moved = pltpu.roll(values[f], (EDGE * x + HALO) % LANES, 1)
            packed[f] = moved if x == 0 else jnp.where(lane_own // EDGE == x, moved, packed[f])
    for f in range(4):
        p_all[1, f, pl.ds(ypad, ey)] = packed[f]
        for phase in range(2):
            py_send[phase, 0, f] = packed[f][2 * phase : 2 * phase + 2]
            py_send[phase, 1, f] = packed[f][ey - 2 - 2 * phase : ey - 2 * phase]
    width = HALO * EDGE
    for xs in range(2):
        joined = None
        for f in range(4):
            shift = width * f - (0 if xs == 0 else (ex - HALO) * EDGE)
            moved = pltpu.roll(packed[f], shift % LANES, 1)
            joined = moved if f == 0 else jnp.where(lane_own // width == f, moved, joined)
        q_send[xs] = joined
        for phase in range(2):
            qy_send[phase, xs, 0] = joined[2 * phase : 2 * phase + 2]
            qy_send[phase, xs, 1] = joined[ey - 2 - 2 * phase : ey - 2 * phase]
    for side in range(2):
        for i, (f, layer) in enumerate(LAYERS):
            start = HALO * rows + ypad + (layer - 1 if side == 0 else ey - layer)
            for half in range(ex // 8):
                y_send[side, i, pl.ds(8 * half, 8)] = base[
                    f, pl.ds(start + 8 * half * rows, 8, stride=rows)
                ]
            for xs in range(2):
                x0 = 0 if xs == 0 else ex - HALO
                xy_send[xs, side, i] = base[f, pl.ds(start + x0 * rows, HALO, stride=rows)]
                if i < len(NEAR):
                    x0 = 0 if xs == 0 else ex - 2
                    xyn_send[xs, side, i] = base[f, pl.ds(start + x0 * rows, 2, stride=rows)]

    pl.semaphore_wait(barrier, levels * count_x * count_y - 1)

    def pieces(d, phase):
        dx, dy, dz = d
        xs, ys = (dx + 1) // 2, (dy + 1) // 2
        out = []
        near, far = pl.ds(0, len(NEAR)), pl.ds(len(NEAR), len(FAR))
        own = pl.ds(ypad, ey)
        edges, late = phase % 2 == 0, phase // 2
        if dy == 0:
            if late:
                return out
            if dz == 0 and not edges:
                for part in range(HALO):
                    src_x = part if dx < 0 else ex - HALO + part
                    dst_x = ex + part if dx < 0 else part - HALO
                    out.append((base.at[:, block(src_x)], base.at[:, block(dst_x)], 4 * ey))
            if dx == 0 and edges:
                out.append((p_all.at[1, :, own], p_all.at[1 - dz, :, own], 4 * ey))
            elif edges:
                out.append((q_send.at[xs], q_all.at[1 - xs, 1 - dz, own], ey))
            return out
        if edges:
            if dx == 0:
                out.append((py_send.at[late, ys], py_recv.at[late, 1 - ys, 1 - dz], 8))
            else:
                out.append((qy_send.at[late, xs, ys], qy_recv.at[late, 1 - xs, 1 - ys, 1 - dz], 2))
        elif dz == 0 and dx == 0:
            part = far if late else near
            size = len(FAR) if late else len(NEAR)
            out.append((y_send.at[ys, part], y_recv.at[1 - ys, part], size * ex))
        elif dz == 0 and not late:
            out.append((xyn_send.at[xs, ys], xyn_recv.at[1 - xs, 1 - ys], 2 * len(NEAR)))
        elif dz == 0:
            out.append((xy_send.at[xs, ys], xy_recv.at[1 - xs, 1 - ys], HALO * len(LAYERS)))
        return out

    def start_sends(phase):
        odd = lax.rem(me[1], 2) == 1
        ordered = []
        for turn_number in range(2):
            for number, d in enumerate(DIRECTIONS):
                if d[1] != 0:
                    ordered.append((number, d, odd == ((d[1] > 0) == (turn_number == 0))))
        ordered += [(number, d, None) for number, d in enumerate(DIRECTIONS) if d[1] == 0]
        for number, d, condition in ordered:
            parts = pieces(d, phase)
            if not parts:
                continue

            @pl.when(exists(*d) if condition is None else exists(*d) & condition)
            def _():
                for src, dst, _ in parts:
                    pltpu.make_async_remote_copy(
                        src_ref=src,
                        dst_ref=dst,
                        send_sem=halo_sem.at[4],
                        recv_sem=halo_sem.at[phase],
                        device_id=tuple(me[axis] + d[axis] for axis in range(3)),
                        device_id_type=MESH,
                    ).start()

    for phase in range(4):
        start_sends(phase)

    def wait_bytes(size, sem):
        span = amount.at[pl.ds(0, size)]
        pltpu.make_async_copy(span, span, sem).wait()

    sides_of = [
        (here > 0).astype(jnp.int32) + (here < count - 1).astype(jnp.int32)
        for here, count in zip(me, counts)
    ]
    most = [min(2, count - 1) for count in counts]

    def wait_halo(phases, sem):
        for number_x in range(min(1, most[0]), most[0] + 1):
            for number_y in range(min(1, most[1]), most[1] + 1):
                for number_z in range(min(1, most[2]), most[2] + 1):
                    have = (number_x, number_y, number_z)
                    size = 0
                    for d in DIRECTIONS:
                        if d == tuple(-abs(step) for step in d):
                            times = 1
                            for step, number in zip(d, have):
                                times *= number if step else 1
                            for phase in phases:
                                size += times * sum(part[2] for part in pieces(d, phase))

                    @pl.when(
                        (sides_of[0] == number_x)
                        & (sides_of[1] == number_y)
                        & (sides_of[2] == number_z)
                    )
                    def _():
                        wait_bytes(size, sem)

    rounds = []
    radius = reach
    while radius < count_z - 1:
        rounds.append(radius)
        radius *= 2

    def hello(number):
        for side, step in enumerate((-rounds[number], rounds[number])):

            @pl.when(exists(0, 0, step))
            def _():
                pl.semaphore_signal(
                    hello_sem.at[number, 1 - side],
                    inc=1,
                    device_id=(me[0], me[1], me[2] + step),
                    device_id_type=MESH,
                )

    def hear(number):
        for side, step in enumerate((-rounds[number], rounds[number])):

            @pl.when(exists(0, 0, step))
            def _():
                pl.semaphore_wait(hello_sem.at[number, side], 1)

    if rounds:
        hello(0)

    def unpack_main(phase):
        for side in range(2):
            for i, (f, layer) in enumerate(LAYERS):
                y = ypad - layer if side == 0 else ypad + ey + layer - 1
                if (i < len(NEAR)) == (phase == 0):
                    for half in range(ex // 8):
                        base[f, pl.ds((HALO + 8 * half) * rows + y, 8, stride=rows)] = y_recv[
                            side, i, pl.ds(8 * half, 8)
                        ]
                for xs in range(2):
                    if phase == 1:
                        x0 = 0 if xs == 0 else HALO + ex
                        base[f, pl.ds(x0 * rows + y, HALO, stride=rows)] = xy_recv[xs, side, i]
                    elif i < len(NEAR):
                        x0 = HALO - 2 if xs == 0 else HALO + ex
                        base[f, pl.ds(x0 * rows + y, 2, stride=rows)] = xyn_recv[xs, side, i]

    def unpack_edges(phase):
        for side in range(2):
            start = ypad - 2 - 2 * phase if side == 0 else ypad + ey + 2 * phase
            for dz in range(3):
                for f in range(4):
                    p_all[dz, f, pl.ds(start, 2)] = py_recv[phase, side, dz, f]
                for xs in range(2):
                    q_all[xs, dz, pl.ds(start, 2)] = qy_recv[phase, xs, side, dz]
        wide = pl.ds(first_y, wide_y)
        for f in range(4):
            back, here, front = (p_all[dz, f, wide] for dz in range(3))
            edge_base[f, 0, wide] = jnp.where(goods[0], jnp.where(lower, back, here), 0.0)
            edge_base[f, 1, wide] = jnp.where(goods[1], jnp.where(lower, here, front), 0.0)
        low, high = [], []
        for xs in range(2):
            back, here, front = (q_all[xs, dz, wide] for dz in range(3))
            low.append(jnp.where(lower, back, here))
            high.append(jnp.where(lower, here, front))
        for f in range(4):
            quarter = [
                pltpu.roll(value, (width * (k - f)) % LANES, 1)
                for k, value in enumerate((low[1], low[0], high[1], high[0]))
            ]
            merged = jnp.where(
                high_z,
                jnp.where(upper_x, quarter[2], quarter[3]),
                jnp.where(upper_x, quarter[0], quarter[1]),
            )
            edge_base[f, 2, wide] = jnp.where(goods[2], merged, 0.0)

    def at(p, dy=0, own=False):
        if own:
            return pl.ds(p * rows + ypad + dy, ey)
        return pl.ds(p * rows + first_y + dy, wide_y)

    outer = lax.broadcasted_iota(jnp.int32, (EDGE, LANES), 0) < HALO

    def take(ref, index, start, dy, mode):
        if mode == "wide":
            return ref[index + (pl.ds(start + first_y + dy, wide_y),)]
        if mode == "own":
            return ref[index + (pl.ds(start + ypad + dy, ey),)]
        low = ref[index + (pl.ds(start + first_y + dy, EDGE),)]
        high = ref[index + (pl.ds(start + ypad + ey - HALO + dy, EDGE),)]
        return jnp.where(outer, low, high)

    def put(ref, index, start, mode, value):
        if mode == "wide":
            ref[index + (pl.ds(start + first_y, wide_y),)] = value
        elif mode == "own":
            ref[index + (pl.ds(start + ypad, ey),)] = value
        else:
            ref[index + (pl.ds(start + first_y, HALO),)] = value[:HALO]
            ref[index + (pl.ds(start + ypad + ey, HALO),)] = value[HALO:]

    cell = lane // EDGE
    last_cell = cell == LANES // EDGE - 1
    first_cell = cell == 0
    half_cell = LANES // EDGE // 2

    def turn(value, step):
        return pltpu.roll(value, step % LANES, 1)

    def edge_shift(values, step):
        low, high, outer = values
        near = [turn(value, -step * EDGE) for value in values]
        half = LANES // 2
        if step > 0:
            far = turn(jnp.where(cell == half_cell, outer, low), half - EDGE)
            return [
                jnp.where(last_cell, near[2], near[0]),
                jnp.where(last_cell, far, near[1]),
                jnp.where(last_cell, near[1], jnp.where(cell == half_cell - 1, far, near[2])),
            ]
        far = turn(jnp.where(cell == half_cell - 1, outer, high), half + EDGE)
        return [
            jnp.where(first_cell, far, near[0]),
            jnp.where(first_cell, near[2], near[1]),
            jnp.where(first_cell, near[0], jnp.where(cell == half_cell, far, near[2])),
        ]

    def edge_stage(field, stage, sums=True):
        wide = pl.ds(first_y, wide_y)

        def load(c, oy):
            return [field[c, k, pl.ds(first_y + oy, wide_y)] for k in range(3)]

        centre = [load(c, 0) for c in range(3)]
        y_up = [load(c, 1) for c in range(3)]
        y_down = [load(c, -1) for c in range(3)]
        slope = [[CROSS * (y_up[c][k] - y_down[c][k]) for k in range(3)] for c in range(3)]
        used = range(3) if sums else (0, 2)
        x_up = {c: edge_shift(centre[c], 1) for c in used}
        x_down = {c: edge_shift(centre[c], -1) for c in used}
        ups, downs = [], []
        for k in range(3):
            tilt = [
                CROSS * (x_up[2][k] - x_down[2][k]),
                slope[2][k],
                CROSS * (x_up[0][k] - x_down[0][k]) + slope[1][k],
            ]
            mine = [centre[0][k], centre[1][k], OWN * centre[2][k]]
            ups.append([mine[c] + tilt[c] for c in range(3)])
            downs.append([mine[c] - tilt[c] for c in range(3)])
        front = lax.rem(lane, EDGE) == HALO
        for c in range(3):
            sides[stage, c, pl.ds(first_y, wide_y)] = jnp.where(front, ups[1][c], turn(downs[0][c], 2))
            sides[stage, c, pl.ds(rows + first_y, wide_y)] = jnp.where(
                front, turn(ups[2][c], LANES // 2), turn(downs[2][c], 2)
            )
        if not sums:
            return None
        slope_up, slope_down = [], []
        for c in range(2):
            for shifted, out in ((x_up, slope_up), (x_down, slope_down)):
                slot = 2 * c + (0 if out is slope_up else 1)
                for k in range(3):
                    swung[slot, k, wide] = shifted[c][k]
                out.append(
                    [
                        CROSS
                        * (
                            swung[slot, k, pl.ds(first_y + 1, wide_y)]
                            - swung[slot, k, pl.ds(first_y - 1, wide_y)]
                        )
                        for k in range(3)
                    ]
                )
        out = []
        for k in range(3):
            sum_x = [x_up[c][k] + x_down[c][k] for c in range(3)]
            sum_y = [y_up[c][k] + y_down[c][k] for c in range(3)]
            sum_z = [turn(ups[k][c], -1) + turn(downs[k][c], 1) for c in range(3)]
            out.append(
                [
                    OWN * sum_x[0] + sum_y[0] + (slope_up[1][k] - slope_down[1][k]) + sum_z[0],
                    sum_x[1] + OWN * sum_y[1] + (slope_up[0][k] - slope_down[0][k]) + sum_z[1],
                    sum_x[2] + sum_y[2] + sum_z[2],
                ]
            )
        return out

    def edge_sweep(source, target, stage):
        beside = edge_stage(source, stage)
        wide = pl.ds(first_y, wide_y)
        for k in range(3):
            share = edge_base[3, k, wide]
            for c in range(3):
                target[c, k, wide] = (
                    KEEP * source[c, k, wide] + edge_base[c, k, wide] + share * beside[k][c]
                )

    def neighbours(field, p, x, stage, mode="wide"):
        def load(c, ox, oy):
            return take(field, (c,), (p + ox) * rows, oy, mode)

        ring = (x + 2 * HALO) % wide_x
        outside = ring < 2 * HALO
        where_x = ring if outside else ring - 2 * HALO
        shift = (LANES - 1 - HALO - EDGE * where_x) % LANES
        centre = [load(c, 0, 0) for c in range(3)]
        x_up = [load(c, 1, 0) for c in range(3)]
        x_down = [load(c, -1, 0) for c in range(3)]
        y_up = [load(c, 0, 1) for c in range(3)]
        y_down = [load(c, 0, -1) for c in range(3)]
        slope = [CROSS * (y_up[c] - y_down[c]) for c in range(3)]
        corner = [
            CROSS * (load(c, 1, 1) - load(c, 1, -1)) - CROSS * (load(c, -1, 1) - load(c, -1, -1))
            for c in range(2)
        ]
        tilt = [
            CROSS * (x_up[2] - x_down[2]),
            slope[2],
            CROSS * (x_up[0] - x_down[0]) + slope[1],
        ]
        mine = [centre[0], centre[1], OWN * centre[2]]
        lanes = lax.broadcasted_iota(jnp.int32, centre[0].shape, 1)
        sum_z = []
        for c in range(3):
            end = pltpu.roll(take(sides, (stage, c), rows if outside else 0, 0, mode), shift, 1)
            up = jnp.where(lanes == LANES - 1, end, turn(mine[c] + tilt[c], -1))
            down = jnp.where(lanes == 0, end, turn(mine[c] - tilt[c], 1))
            sum_z.append(up + down)
        return [
            OWN * (x_up[0] + x_down[0]) + (y_up[0] + y_down[0]) + corner[1] + sum_z[0],
            (x_up[1] + x_down[1]) + OWN * (y_up[1] + y_down[1]) + corner[0] + sum_z[1],
            (x_up[2] + x_down[2]) + (y_up[2] + y_down[2]) + sum_z[2],
        ]

    def sweep(source, target, low, high, stage, mode="wide"):
        for x in range(low, high):
            p = x + HALO
            beside = neighbours(source, p, x, stage, mode)
            share = take(base, (3,), p * rows, 0, mode)
            for c in range(3):
                kept = KEEP * take(source, (c,), p * rows, 0, mode)
                fresh = kept + take(base, (c,), p * rows, 0, mode) + share * beside[c]
                put(target, (c,), p * rows, mode, fresh)

    def residual(field, x, stage):
        p = x + HALO
        beside = neighbours(field, p, x, stage, "own")
        g = stiff[own_rows(x)]
        heavy = g * DIAGONAL + MASS_TERM
        return [
            raw[c, x] - heavy * field[c, at(p, 0, True)] + g * beside[c] for c in range(3)
        ]

    wait_halo((0,), halo_sem.at[0])
    unpack_edges(0)
    edge_sweep(edge_base, edge_a, 0)
    edge_stage(edge_a, 1, False)
    greeted = min(1, len(rounds) - 1)
    for number in range(greeted):
        hear(number)
        hello(number + 1)
    wait_halo((1,), halo_sem.at[1])
    unpack_main(0)
    sweep(base, field_a, -1, ex + 1, 0)

    def restrict(x, carry):
        left = residual(field_a, x, 1)
        return tuple(carry[c] + left[c] for c in range(3))

    sums = by_two(0, ex, restrict, (jnp.zeros((ey, LANES), jnp.float32),) * 3)
    sums = [fold(s) for s in sums] + [stiff_sum]
    stacked = jnp.concatenate([jnp.sum(s, axis=0, keepdims=True) for s in sums] + [zero[:4]], axis=0)
    source_lane = lax.broadcasted_iota(jnp.int32, (LANES, LANES), 0)
    target_lane = lax.broadcasted_iota(jnp.int32, (LANES, LANES), 1)
    gather = (source_lane // BLOCK == lax.rem(target_lane, cz)).astype(jnp.float32)
    grouped = jnp.dot(stacked, gather, precision=EXACT, preferred_element_type=jnp.float32)
    coarse_send[...] = grouped[:4]

    def coarse_copy(x, y, z, dz):
        return pltpu.make_async_remote_copy(
            src_ref=coarse_send,
            dst_ref=coarse_recv.at[reach - dz, me[0] * count_y + me[1]],
            send_sem=coarse_sem.at[0],
            recv_sem=coarse_sem.at[1],
            device_id=(x, y, z),
            device_id_type=MESH,
        )

    def coarse_wait():
        for number in range(1, window + 1):

            @pl.when(levels == number)
            def _():
                for k in range(2):
                    wait_bytes(4 * (number * count_x * count_y - 1), coarse_sem.at[k])

    peers(lambda x, y, z, dz: coarse_copy(x, y, z, dz).start())
    coarse_recv[reach, me[0] * count_y + me[1]] = grouped[:4]

    sweep(field_a, field_b, 0, ex, 1, "own")
    wait_halo((2,), halo_sem.at[2])
    unpack_edges(1)
    edge_sweep(edge_base, edge_a, 0)
    edge_sweep(edge_a, edge_b, 1)
    wait_halo((3,), halo_sem.at[3])
    unpack_main(1)
    for low, high in ((1 - HALO, -1), (ex + 1, ex + HALO - 1)):
        sweep(base, field_a, low, high, 0)
    sweep(base, field_a, -1, ex + 1, 0, "rim")
    for low, high in ((-2, 0), (ex, ex + 2)):
        sweep(field_a, field_b, low, high, 1)
    sweep(field_a, field_b, 0, ex, 1, "rim")
    wait_halo(range(4), halo_sem.at[4])
    coarse_wait()

    coarse_rows = -(-(count_y + 1) // 8) * 8
    lane_c = lax.broadcasted_iota(jnp.int32, (coarse_rows, LANES), 1)
    row_c = lax.broadcasted_iota(jnp.int32, (coarse_rows, LANES), 0)
    at_z = me[2] * cz - reach * cz + lane_c
    valid = (
        (row_c < count_y) & (at_z >= 0) & (at_z < cz * count_z) & (lane_c < window * cz)
    )
    slab = [[None] * 4 for _ in range(count_x)]
    for x in range(count_x):
        for c in range(4):
            value = None
            for w in range(window):
                column = jnp.concatenate(
                    [coarse_recv[w, x * count_y + y, c : c + 1] for y in range(count_y)]
                    + [jnp.zeros((coarse_rows - count_y, LANES), jnp.float32)],
                    axis=0,
                )
                value = column if value is None else jnp.where(lane_c // cz == w, column, value)
            slab[x][c] = jnp.where(valid, value, 0.0)
    mass = BLOCK**3 * MASS_TERM
    factor = [slab[x][3] * (BLOCK**2 / BLOCK**3) for x in range(count_x)]
    relax = [
        jnp.where(valid, RELAXATION / (factor[x] * DIAGONAL + mass), 0.0) for x in range(count_x)
    ]
    nothing = jnp.zeros((coarse_rows, LANES), jnp.float32)
    start_w = [[slab[x][c] * relax[x] for c in range(3)] for x in range(count_x)]
    share_w = [factor[x] * relax[x] for x in range(count_x)]
    w = start_w

    def y_shift(value, step):
        return pltpu.roll(value, step % coarse_rows, 0)

    for repeat in range(COARSE - 1):
        fresh = []
        for x in range(count_x):
            here = w[x]
            above = w[x + 1] if x + 1 < count_x else [nothing] * 3
            below = w[x - 1] if x > 0 else [nothing] * 3
            sum_x = [above[c] + below[c] for c in range(3)]
            diff_x = [above[c] - below[c] for c in range(3)]
            y_up = [y_shift(here[c], -1) for c in range(3)]
            y_down = [y_shift(here[c], 1) for c in range(3)]
            sum_y = [y_up[c] + y_down[c] for c in range(3)]
            diff_y = [y_up[c] - y_down[c] for c in range(3)]
            corner_x = y_shift(diff_x[1], -1) - y_shift(diff_x[1], 1)
            corner_y = y_shift(diff_x[0], -1) - y_shift(diff_x[0], 1)
            tilt = [CROSS * diff_x[2], CROSS * diff_y[2], CROSS * (diff_x[0] + diff_y[1])]
            own = [here[0], here[1], OWN * here[2]]
            sum_z = [turn(own[c] + tilt[c], -1) + turn(own[c] - tilt[c], 1) for c in range(3)]
            beside = [
                OWN * sum_x[0] + sum_y[0] + CROSS * corner_x + sum_z[0],
                sum_x[1] + OWN * sum_y[1] + CROSS * corner_y + sum_z[1],
                sum_x[2] + sum_y[2] + sum_z[2],
            ]
            fresh.append(
                [
                    KEEP * here[c] + start_w[x][c] + share_w[x] * beside[c]
                    for c in range(3)
                ]
            )
        w = fresh

    for x in range(count_x + 2):
        for c in range(3):
            inside = 1 <= x <= count_x
            coarse_w[x, c, pl.ds(0, 8)] = jnp.zeros((8, LANES), jnp.float32)
            coarse_w[x, c, pl.ds(8, coarse_rows)] = w[x - 1][c] if inside else nothing
    stack_w[pl.ds(24, 8)] = zero
    for xc in range(3):
        for c in range(3):
            stack_w[pl.ds(3 * (3 * xc + c), 3)] = coarse_w[me[0] + xc, c, pl.ds(7 + me[1], 3)]
    inner = lax.rem(target_lane, EDGE) < HALO
    first_cell_z, last_cell_z = reach * cz, (reach + 1) * cz - 1
    pick_low = jnp.where(inner, first_cell_z - 1, first_cell_z)
    pick_high = jnp.where(inner, last_cell_z, last_cell_z + 1)
    picks = (
        first_cell_z + target_lane // BLOCK,
        pick_low,
        pick_high,
        jnp.where(target_lane < LANES // 2, pick_low, pick_high),
    )
    widen = jnp.concatenate([(source_lane == pick).astype(jnp.float32) for pick in picks], axis=1)
    wide_all = jnp.dot(stack_w[...], widen, precision=EXACT, preferred_element_type=jnp.float32)

    def drawn(xc, c, k):
        parts = []
        for j in range(3):
            line = 3 * (3 * xc + c) + j
            piece = wide_all[line : line + 1, k * LANES : (k + 1) * LANES]
            parts.append(jnp.broadcast_to(piece, (wide_y, LANES)))
        return jnp.where(row_y < HALO, parts[0], jnp.where(row_y < HALO + ey, parts[1], parts[2]))

    wide = pl.ds(first_y, wide_y)
    for c in range(3):
        for xc in range(3):
            value = drawn(xc, c, 0)
            for plane in range(3):
                spread_w[c, pl.ds((3 * xc + plane) * rows + first_y, wide_y)] = value
        edge_a[c, 0, wide] = drawn(1, c, 1)
        edge_a[c, 1, wide] = drawn(1, c, 2)
        edge_a[c, 2, wide] = jnp.where(upper_x, drawn(2, c, 3), drawn(0, c, 3))
    beside = edge_stage(edge_a, 0)
    for k in range(3):
        share = edge_base[3, k, wide]
        for c in range(3):
            edge_b[c, k, wide] = (
                edge_b[c, k, wide] + KEEP * edge_a[c, k, wide] + share * beside[k][c]
            )
    edge_sweep(edge_b, edge_a, 1)
    edge_stage(edge_a, 2, False)
    for plane, x in ((1, -2), (2, -1), (3, 0), (4, ex // 2), (5, ex - 1), (6, ex), (7, ex + 1)):
        images = neighbours(spread_w, plane, x, 0)
        for c in range(3):
            image_w[c, at(plane)] = images[c]

    def correct(p, carry):
        kind = (
            jnp.int32(1)
            + jnp.int32(p >= HALO - 1)
            + jnp.int32(p >= HALO)
            + jnp.int32(p >= HALO + 1)
            + jnp.int32(p >= HALO + ex - 1)
            + jnp.int32(p >= HALO + ex)
            + jnp.int32(p >= HALO + ex + 1)
        )
        share = base[3, at(p)]
        for c in range(3):
            field_b[c, at(p)] = (
                field_b[c, at(p)] + KEEP * spread_w[c, at(kind)] + share * image_w[c, at(kind)]
            )
        return carry

    by_two(2, wide_x - 2, correct, 0)
    sweep(field_b, field_a, -1, ex + 1, 1)

    def squares(x, carry):
        left = residual(field_a, x, 2)
        for c in range(3):
            out_ref[c, x] = field_a[c, at(x + HALO, 0, True)]
        return carry + fold(sum(value * value for value in left))

    left_sum = by_two(0, ex, squares, zero)
    load_total = jnp.sum(jnp.sum(load_sum, axis=0, keepdims=True), axis=1, keepdims=True)
    left_total = jnp.sum(jnp.sum(left_sum, axis=0, keepdims=True), axis=1, keepdims=True)
    first = lax.broadcasted_iota(jnp.int32, (1, LANES), 1) == 0
    mine = jnp.where(first, load_total, left_total)
    norm_send[...] = mine

    for number in range(greeted, len(rounds)):
        if number > greeted:
            hello(number)
        hear(number)
    for x in reversed(ring_x):
        for z in reversed(ring_z):
            for y in reversed(ring_y):
                if x is not me[0] or y is not me[1] or z is not me[2]:
                    pltpu.make_async_remote_copy(
                        src_ref=norm_send,
                        dst_ref=norm_recv.at[my_id],
                        send_sem=norm_sem.at[0],
                        recv_sem=norm_sem.at[1],
                        device_id=(x, y, z),
                        device_id_type=MESH,
                    ).start()
    norm_recv[my_id] = mine
    others = norm_recv.at[pl.ds(0, total - 1)]
    for k in range(2):
        pltpu.make_async_copy(others, others, norm_sem.at[k]).wait()
    summed = jnp.sum(norm_recv[...], axis=0)
    nodes = 3 * ex * ey * ez * total
    norms_ref[...] = jnp.sqrt(summed / nodes)


def on_device(counts, right_side, damage):
    _, ex, ey, ez = right_side.shape
    assert ez == LANES and ex * EDGE == LANES and 2 * EDGE * EDGE == LANES
    assert ex % BLOCK == 0 and ey == BLOCK and ex == BLOCK
    cz = ez // BLOCK
    wide_x = ex + 2 * HALO
    rows = ey + 2 * YPAD
    flat = wide_x * rows
    total = counts[0] * counts[1] * counts[2]
    window = 2 * (-(-COARSE // cz)) + 1
    coarse_rows = -(-(counts[1] + 1) // 8) * 8
    rounds = 0
    while window // 2 << rounds < counts[2] - 1:
        rounds += 1
    f32 = jnp.float32

    def vmem(*shape):
        return pltpu.VMEM(shape + (LANES,), f32)

    dma = pltpu.SemaphoreType.DMA
    near, layers = len(NEAR), len(LAYERS)
    displacement, norms = pl.pallas_call(
        functools.partial(kernel, counts, (ex, ey, ez)),
        out_shape=(
            pltpu.VMEM(right_side.shape, f32),
            pltpu.VMEM((1, LANES), f32),
        ),
        in_specs=[pl.BlockSpec(memory_space=pl.ANY)] * 2,
        out_specs=(
            pl.BlockSpec(memory_space=pltpu.VMEM),
            pl.BlockSpec(memory_space=pltpu.VMEM),
        ),
        scratch_shapes=[
            vmem(3, ex, ey),
            vmem(ex * ey),
            pltpu.VMEM((ex, ey, LANES), jnp.int32),
            vmem(4, flat),
            vmem(3, flat),
            vmem(3, flat),
            vmem(4, 3, rows),
            vmem(3, 3, rows),
            vmem(3, 3, rows),
            vmem(3, 3, 2 * rows),
            vmem(4, 3, rows),
            vmem(2, layers, ex),
            vmem(2, layers, ex),
            vmem(2, 2, near, 2),
            vmem(2, 2, near, 2),
            vmem(2, 2, layers, HALO),
            vmem(2, 2, layers, HALO),
            vmem(3, 4, rows),
            vmem(2, ey),
            vmem(2, 3, rows),
            vmem(2, 2, 4, 2),
            vmem(2, 2, 3, 4, 2),
            vmem(2, 2, 2, 2),
            vmem(2, 2, 2, 3, 2),
            vmem(4),
            vmem(window, counts[0] * counts[1], 4),
            vmem(counts[0] + 2, 3, 8 + coarse_rows),
            vmem(32),
            vmem(3, 9 * rows),
            vmem(3, 9 * rows),
            vmem(1),
            vmem(total, 1),
            vmem(4 * EDGE * LANES, 1),
            dma((2,)),
            dma((5,)),
            dma((2,)),
            dma((2,)),
            pltpu.SemaphoreType.REGULAR((max(1, rounds), 2)),
        ],
        compiler_params=pltpu.CompilerParams(collective_id=0, has_side_effects=True),
    )(right_side, damage)
    return displacement, norms[0, :2]


def solution(mesh):
    counts = tuple(mesh.shape[axis] for axis in AXES)
    placed = (P(None, "gx", "gy", "gz"), P("gx", "gy", "gz"))
    return jax.shard_map(
        functools.partial(on_device, counts),
        mesh=mesh,
        in_specs=placed,
        out_specs=(P(None, "gx", "gy", "gz"), P()),
        check_vma=False,
    )
```

```python
import functools

import jax
import jax.numpy as jnp
from jax import lax
from jax.experimental import pallas as pl
from jax.experimental.pallas import tpu as pltpu
from jax.sharding import PartitionSpec as P

BLOCK = 16
COARSE = 8
FLOOR_STIFFNESS = 0.05
MASS_TERM = 0.001
COUPLING = 2.5
RELAXATION = 0.6
KEEP = 1.0 - RELAXATION
DIAGONAL = 6.0 + 2.0 * COUPLING
OWN = 1.0 + COUPLING
CROSS = 0.25 * COUPLING
AXES = ("gx", "gy", "gz")
HALO = 4
EDGE = 2 * HALO
LANES = 128
YPAD = 8
MESH = pl.DeviceIdType.MESH
EXACT = lax.Precision.HIGHEST
NEAR = ((0, 1), (1, 1), (2, 1), (3, 1), (0, 2), (1, 2), (2, 2))
FAR = ((3, 2), (0, 3), (1, 3), (2, 3), (3, 3), (0, 4), (1, 4), (2, 4))
LAYERS = NEAR + FAR


def directions():
    out = []
    for dx in (-1, 0, 1):
        for dy in (-1, 0, 1):
            for dz in (-1, 0, 1):
                if (dx, dy, dz) != (0, 0, 0):
                    out.append((dx, dy, dz))
    return sorted(out, key=lambda d: -sum(abs(step) for step in d))


DIRECTIONS = directions()


UNROLL = 24


def by_two(low, high, body, carry):
    trips = -(-(high - low) // UNROLL)
    size = -(-(high - low) // trips)
    whole = (high - low) // size

    def several(trip, carry):
        for k in range(size):
            carry = body(low + size * trip + k, carry)
        return carry

    if whole > 1:
        carry = lax.fori_loop(0, whole, several, carry)
    else:
        carry = several(0, carry)
    for k in range(low + whole * size, high):
        carry = body(k, carry)
    return carry


def kernel(
    counts,
    extent,
    load_ref,
    damage_ref,
    out_ref,
    norms_ref,
    raw,
    stiff,
    harm,
    base,
    field_a,
    field_b,
    edge_base,
    edge_a,
    edge_b,
    sides,
    swung,
    relay,
    y_send,
    y_recv,
    xyn_send,
    xyn_recv,
    xy_send,
    xy_recv,
    p_all,
    q_send,
    q_all,
    py_send,
    py_recv,
    qy_send,
    qy_recv,
    coarse_send,
    coarse_recv,
    coarse_w,
    stack_w,
    spread_w,
    image_w,
    norm_send,
    norm_recv,
    amount,
    local_sem,
    halo_sem,
    coarse_sem,
    norm_sem,
    hello_sem,
):
    count_x, count_y, count_z = counts
    ex, ey, ez = extent
    cz = ez // BLOCK
    total = count_x * count_y * count_z
    wide_x = ex + 2 * HALO
    ypad = YPAD
    rows = ey + 2 * ypad
    wide_y = ey + 2 * HALO
    first_y = ypad - HALO
    me = tuple(lax.axis_index(axis) for axis in AXES)
    my_id = (me[0] * count_y + me[1]) * count_z + me[2]

    def place(index):
        return (
            index // (count_y * count_z),
            lax.rem(index // count_z, count_y),
            lax.rem(index, count_z),
        )

    harm_copy = pltpu.make_async_copy(damage_ref, harm, local_sem.at[0])
    load_copy = pltpu.make_async_copy(load_ref, raw, local_sem.at[1])
    harm_copy.start()
    load_copy.start()
    barrier = pltpu.get_barrier_semaphore()

    reach = -(-COARSE // cz)
    window = 2 * reach + 1

    def around(here, count):
        out = [here]
        for step in range(1, count):
            there = here + step
            out.append(jnp.where(there >= count, there - count, there))
        return out

    ring_x, ring_y, ring_z = (around(me[axis], counts[axis]) for axis in range(3))

    def peers(act):
        for dz in sorted(range(-reach, reach + 1), key=lambda step: -abs(step)):
            z = me[2] + dz

            @pl.when((z >= 0) & (z < count_z))
            def _():
                for x in reversed(ring_x):
                    for y in reversed(ring_y):
                        if dz != 0 or x is not me[0] or y is not me[1]:
                            act(x, y, z, dz)

    def greet(x, y, z, dz):
        pl.semaphore_signal(barrier, inc=1, device_id=(x, y, z), device_id_type=MESH)

    peers(greet)
    levels = jnp.minimum(me[2] + reach, count_z - 1) - jnp.maximum(me[2] - reach, 0) + 1

    def exists(dx, dy, dz):
        ok = None
        for axis, step in enumerate((dx, dy, dz)):
            if step == 0:
                continue
            here = me[axis] + step
            good = (here >= 0) & (here < counts[axis])
            ok = good if ok is None else ok & good
        return ok

    def block(x):
        return pl.ds((HALO + x) * rows + ypad, ey)

    for xs in range(2):

        @pl.when(jnp.logical_not(exists(2 * xs - 1, 0, 0)))
        def _():
            for part in range(HALO):
                for f in range(4):
                    x = part - HALO if xs == 0 else ex + part
                    base[f, block(x)] = jnp.zeros((ey, LANES), jnp.float32)

        for ys in range(2):

            @pl.when(jnp.logical_not(exists(2 * xs - 1, 2 * ys - 1, 0)))
            def _():
                xyn_recv[xs, ys] = jnp.zeros((len(NEAR), 2, LANES), jnp.float32)
                xy_recv[xs, ys] = jnp.zeros((len(LAYERS), HALO, LANES), jnp.float32)

    for ys in range(2):

        @pl.when(jnp.logical_not(exists(0, 2 * ys - 1, 0)))
        def _():
            y_recv[ys] = jnp.zeros((len(LAYERS), ex, LANES), jnp.float32)

    lane_own = lax.broadcasted_iota(jnp.int32, (ey, LANES), 1)
    lane = lax.broadcasted_iota(jnp.int32, (wide_y, LANES), 1)
    row_y = lax.broadcasted_iota(jnp.int32, (wide_y, LANES), 0)
    lower = lax.rem(lane, EDGE) < HALO
    at_y = me[1] * ey + row_y - HALO
    good_y = (at_y >= 0) & (at_y < ey * count_y)
    has_back, has_front = me[2] > 0, me[2] < count_z - 1
    upper_x = lax.rem(lane // (HALO * EDGE), 2) == 0
    high_z = lane >= LANES // 2
    good_x = (upper_x & (me[0] < count_x - 1)) | (~upper_x & (me[0] > 0))
    good_z = (high_z & (lower | has_front)) | (~high_z & (~lower | has_back))
    goods = (
        good_y & (~lower | has_back),
        good_y & (lower | has_front),
        good_y & good_x & good_z,
    )

    def fold(value):
        return jnp.sum(value.reshape(ey // 8, 8, LANES), axis=0)

    zero = jnp.zeros((8, LANES), jnp.float32)

    harm_copy.wait()
    load_copy.wait()

    def own_rows(x):
        return pl.ds(x * ey, ey)

    load_sum = zero
    stiff_sum = zero
    packed = [None] * 4
    for x in range(ex):
        level = 1.0 - harm[x].astype(jnp.float32) / 15.0
        g = level * level * (1.0 - FLOOR_STIFFNESS) + FLOOR_STIFFNESS
        inv = RELAXATION / (g * DIAGONAL + MASS_TERM)
        stiff[own_rows(x)] = g
        stiff_sum = stiff_sum + fold(g)
        values = []
        squared = None
        for c in range(3):
            load = raw[c, x]
            values.append(load * inv)
            squared = load * load if squared is None else squared + load * load
        load_sum = load_sum + fold(squared)
        values.append(g * inv)
        for f in range(4):
            base[f, block(x)] = values[f]
            moved = pltpu.roll(values[f], (EDGE * x + HALO) % LANES, 1)
            packed[f] = moved if x == 0 else jnp.where(lane_own // EDGE == x, moved, packed[f])
    for f in range(4):
        p_all[1, f, pl.ds(ypad, ey)] = packed[f]
        for phase in range(2):
            py_send[phase, 0, f] = packed[f][2 * phase : 2 * phase + 2]
            py_send[phase, 1, f] = packed[f][ey - 2 - 2 * phase : ey - 2 * phase]
    width = HALO * EDGE
    for xs in range(2):
        joined = None
        for f in range(4):
            shift = width * f - (0 if xs == 0 else (ex - HALO) * EDGE)
            moved = pltpu.roll(packed[f], shift % LANES, 1)
            joined = moved if f == 0 else jnp.where(lane_own // width == f, moved, joined)
        q_send[xs] = joined
        for phase in range(2):
            qy_send[phase, xs, 0] = joined[2 * phase : 2 * phase + 2]
            qy_send[phase, xs, 1] = joined[ey - 2 - 2 * phase : ey - 2 * phase]
    for side in range(2):
        for i, (f, layer) in enumerate(LAYERS):
            start = HALO * rows + ypad + (layer - 1 if side == 0 else ey - layer)
            for half in range(ex // 8):
                y_send[side, i, pl.ds(8 * half, 8)] = base[
                    f, pl.ds(start + 8 * half * rows, 8, stride=rows)
                ]
            for xs in range(2):
                x0 = 0 if xs == 0 else ex - HALO
                xy_send[xs, side, i] = base[f, pl.ds(start + x0 * rows, HALO, stride=rows)]
                if i < len(NEAR):
                    x0 = 0 if xs == 0 else ex - 2
                    xyn_send[xs, side, i] = base[f, pl.ds(start + x0 * rows, 2, stride=rows)]

    pl.semaphore_wait(barrier, levels * count_x * count_y - 1)

    def pieces(d, phase):
        dx, dy, dz = d
        xs, ys = (dx + 1) // 2, (dy + 1) // 2
        out = []
        near, far = pl.ds(0, len(NEAR)), pl.ds(len(NEAR), len(FAR))
        own = pl.ds(ypad, ey)
        edges, late = phase % 2 == 0, phase // 2
        if dy == 0:
            if late:
                return out
            if dz == 0 and not edges:
                for part in range(HALO):
                    src_x = part if dx < 0 else ex - HALO + part
                    dst_x = ex + part if dx < 0 else part - HALO
                    out.append((base.at[:, block(src_x)], base.at[:, block(dst_x)], 4 * ey))
            if dx == 0 and edges:
                out.append((p_all.at[1, :, own], p_all.at[1 - dz, :, own], 4 * ey))
            elif edges:
                out.append((q_send.at[xs], q_all.at[1 - xs, 1 - dz, own], ey))
            return out
        if edges:
            if dx == 0:
                out.append((py_send.at[late, ys], py_recv.at[late, 1 - ys, 1 - dz], 8))
            else:
                out.append((qy_send.at[late, xs, ys], qy_recv.at[late, 1 - xs, 1 - ys, 1 - dz], 2))
        elif dz == 0 and dx == 0:
            part = far if late else near
            size = len(FAR) if late else len(NEAR)
            out.append((y_send.at[ys, part], y_recv.at[1 - ys, part], size * ex))
        elif dz == 0 and not late:
            out.append((xyn_send.at[xs, ys], xyn_recv.at[1 - xs, 1 - ys], 2 * len(NEAR)))
        elif dz == 0:
            out.append((xy_send.at[xs, ys], xy_recv.at[1 - xs, 1 - ys], HALO * len(LAYERS)))
        return out

    odd = lax.rem(me[1], 2) == 1
    relayed = {
        1: odd & (me[1] + 2 < count_y),
        -1: jnp.logical_not(odd) & (me[1] >= 2),
    }
    relaying = {
        1: jnp.logical_not(odd) & (me[1] + 2 < count_y),
        -1: odd & (me[1] >= 3),
    }

    def far_copy(src, ys, device_y, final):
        return pltpu.make_async_remote_copy(
            src_ref=src,
            dst_ref=y_recv.at[1 - ys, pl.ds(len(NEAR), len(FAR))] if final else relay,
            send_sem=halo_sem.at[5 if final else 4],
            recv_sem=halo_sem.at[3 if final else 6],
            device_id=(me[0], device_y, me[2]),
            device_id_type=MESH,
        )

    def send_to_relay():
        for dy in (-1, 1):
            ys = (dy + 1) // 2

            @pl.when(relayed[dy])
            def _():
                far_copy(y_send.at[ys, pl.ds(len(NEAR), len(FAR))], ys, me[1] + 2 * dy, False).start()

    def pass_on():
        for dy in (-1, 1):

            @pl.when(relaying[dy])
            def _():
                wait_bytes(len(FAR) * ex, halo_sem.at[6])
                far_copy(relay, (1 - dy) // 2, me[1] + dy, True).start()

    def finish_relay():
        @pl.when(relaying[-1] | relaying[1])
        def _():
            wait_bytes(len(FAR) * ex, halo_sem.at[5])

    def start_sends(phase):
        ordered = []
        for turn_number in range(2):
            for number, d in enumerate(DIRECTIONS):
                if d[1] != 0:
                    ordered.append((number, d, odd == ((d[1] > 0) == (turn_number == 0))))
        ordered += [(number, d, None) for number, d in enumerate(DIRECTIONS) if d[1] == 0]
        for number, d, condition in ordered:
            parts = pieces(d, phase)
            if not parts:
                continue
            here = exists(*d)
            if condition is not None:
                here = here & condition
            if phase == 3 and d[0] == 0:
                here = here & jnp.logical_not(relayed[d[1]])

            @pl.when(here)
            def _():
                for src, dst, _ in parts:
                    pltpu.make_async_remote_copy(
                        src_ref=src,
                        dst_ref=dst,
                        send_sem=halo_sem.at[4],
                        recv_sem=halo_sem.at[phase],
                        device_id=tuple(me[axis] + d[axis] for axis in range(3)),
                        device_id_type=MESH,
                    ).start()

    start_sends(0)
    start_sends(1)
    send_to_relay()

    def wait_bytes(size, sem):
        span = amount.at[pl.ds(0, size)]
        pltpu.make_async_copy(span, span, sem).wait()

    sides_of = [
        (here > 0).astype(jnp.int32) + (here < count - 1).astype(jnp.int32)
        for here, count in zip(me, counts)
    ]
    most = [min(2, count - 1) for count in counts]

    def wait_halo(phases, sem):
        for number_x in range(min(1, most[0]), most[0] + 1):
            for number_y in range(min(1, most[1]), most[1] + 1):
                for number_z in range(min(1, most[2]), most[2] + 1):
                    have = (number_x, number_y, number_z)
                    size = 0
                    for d in DIRECTIONS:
                        if d == tuple(-abs(step) for step in d):
                            times = 1
                            for step, number in zip(d, have):
                                times *= number if step else 1
                            for phase in phases:
                                size += times * sum(part[2] for part in pieces(d, phase))

                    @pl.when(
                        (sides_of[0] == number_x)
                        & (sides_of[1] == number_y)
                        & (sides_of[2] == number_z)
                    )
                    def _():
                        wait_bytes(size, sem)

    rounds = []
    radius = reach
    while radius < count_z - 1:
        rounds.append(radius)
        radius *= 2

    def hello(number):
        for side, step in enumerate((-rounds[number], rounds[number])):

            @pl.when(exists(0, 0, step))
            def _():
                pl.semaphore_signal(
                    hello_sem.at[number, 1 - side],
                    inc=1,
                    device_id=(me[0], me[1], me[2] + step),
                    device_id_type=MESH,
                )

    def hear(number):
        for side, step in enumerate((-rounds[number], rounds[number])):

            @pl.when(exists(0, 0, step))
            def _():
                pl.semaphore_wait(hello_sem.at[number, side], 1)

    if rounds:
        hello(0)

    def unpack_main(phase):
        for side in range(2):
            for i, (f, layer) in enumerate(LAYERS):
                y = ypad - layer if side == 0 else ypad + ey + layer - 1
                if (i < len(NEAR)) == (phase == 0):
                    for half in range(ex // 8):
                        base[f, pl.ds((HALO + 8 * half) * rows + y, 8, stride=rows)] = y_recv[
                            side, i, pl.ds(8 * half, 8)
                        ]
                for xs in range(2):
                    if phase == 1:
                        x0 = 0 if xs == 0 else HALO + ex
                        base[f, pl.ds(x0 * rows + y, HALO, stride=rows)] = xy_recv[xs, side, i]
                    elif i < len(NEAR):
                        x0 = HALO - 2 if xs == 0 else HALO + ex
                        base[f, pl.ds(x0 * rows + y, 2, stride=rows)] = xyn_recv[xs, side, i]

    def unpack_edges(phase):
        for side in range(2):
            start = ypad - 2 - 2 * phase if side == 0 else ypad + ey + 2 * phase
            for dz in range(3):
                for f in range(4):
                    p_all[dz, f, pl.ds(start, 2)] = py_recv[phase, side, dz, f]
                for xs in range(2):
                    q_all[xs, dz, pl.ds(start, 2)] = qy_recv[phase, xs, side, dz]
        wide = pl.ds(first_y, wide_y)
        for f in range(4):
            back, here, front = (p_all[dz, f, wide] for dz in range(3))
            edge_base[f, 0, wide] = jnp.where(goods[0], jnp.where(lower, back, here), 0.0)
            edge_base[f, 1, wide] = jnp.where(goods[1], jnp.where(lower, here, front), 0.0)
        low, high = [], []
        for xs in range(2):
            back, here, front = (q_all[xs, dz, wide] for dz in range(3))
            low.append(jnp.where(lower, back, here))
            high.append(jnp.where(lower, here, front))
        for f in range(4):
            quarter = [
                pltpu.roll(value, (width * (k - f)) % LANES, 1)
                for k, value in enumerate((low[1], low[0], high[1], high[0]))
            ]
            merged = jnp.where(
                high_z,
                jnp.where(upper_x, quarter[2], quarter[3]),
                jnp.where(upper_x, quarter[0], quarter[1]),
            )
            edge_base[f, 2, wide] = jnp.where(goods[2], merged, 0.0)

    def at(p, dy=0, own=False):
        if own:
            return pl.ds(p * rows + ypad + dy, ey)
        return pl.ds(p * rows + first_y + dy, wide_y)

    outer = lax.broadcasted_iota(jnp.int32, (EDGE, LANES), 0) < HALO

    def take(ref, index, start, dy, mode):
        if mode == "wide":
            return ref[index + (pl.ds(start + first_y + dy, wide_y),)]
        if mode == "own":
            return ref[index + (pl.ds(start + ypad + dy, ey),)]
        low = ref[index + (pl.ds(start + first_y + dy, EDGE),)]
        high = ref[index + (pl.ds(start + ypad + ey - HALO + dy, EDGE),)]
        return jnp.where(outer, low, high)

    def put(ref, index, start, mode, value):
        if mode == "wide":
            ref[index + (pl.ds(start + first_y, wide_y),)] = value
        elif mode == "own":
            ref[index + (pl.ds(start + ypad, ey),)] = value
        else:
            ref[index + (pl.ds(start + first_y, HALO),)] = value[:HALO]
            ref[index + (pl.ds(start + ypad + ey, HALO),)] = value[HALO:]

    cell = lane // EDGE
    last_cell = cell == LANES // EDGE - 1
    first_cell = cell == 0
    half_cell = LANES // EDGE // 2

    def turn(value, step):
        return pltpu.roll(value, step % LANES, 1)

    def edge_shift(values, step):
        low, high, outer = values
        near = [turn(value, -step * EDGE) for value in values]
        half = LANES // 2
        if step > 0:
            far = turn(jnp.where(cell == half_cell, outer, low), half - EDGE)
            return [
                jnp.where(last_cell, near[2], near[0]),
                jnp.where(last_cell, far, near[1]),
                jnp.where(last_cell, near[1], jnp.where(cell == half_cell - 1, far, near[2])),
            ]
        far = turn(jnp.where(cell == half_cell - 1, outer, high), half + EDGE)
        return [
            jnp.where(first_cell, far, near[0]),
            jnp.where(first_cell, near[2], near[1]),
            jnp.where(first_cell, near[0], jnp.where(cell == half_cell, far, near[2])),
        ]

    def edge_stage(field, stage, sums=True):
        wide = pl.ds(first_y, wide_y)

        def load(c, oy):
            return [field[c, k, pl.ds(first_y + oy, wide_y)] for k in range(3)]

        centre = [load(c, 0) for c in range(3)]
        y_up = [load(c, 1) for c in range(3)]
        y_down = [load(c, -1) for c in range(3)]
        slope = [[CROSS * (y_up[c][k] - y_down[c][k]) for k in range(3)] for c in range(3)]
        used = range(3) if sums else (0, 2)
        x_up = {c: edge_shift(centre[c], 1) for c in used}
        x_down = {c: edge_shift(centre[c], -1) for c in used}
        ups, downs = [], []
        for k in range(3):
            tilt = [
                CROSS * (x_up[2][k] - x_down[2][k]),
                slope[2][k],
                CROSS * (x_up[0][k] - x_down[0][k]) + slope[1][k],
            ]
            mine = [centre[0][k], centre[1][k], OWN * centre[2][k]]
            ups.append([mine[c] + tilt[c] for c in range(3)])
            downs.append([mine[c] - tilt[c] for c in range(3)])
        front = lax.rem(lane, EDGE) == HALO
        for c in range(3):
            sides[stage, c, pl.ds(first_y, wide_y)] = jnp.where(front, ups[1][c], turn(downs[0][c], 2))
            sides[stage, c, pl.ds(rows + first_y, wide_y)] = jnp.where(
                front, turn(ups[2][c], LANES // 2), turn(downs[2][c], 2)
            )
        if not sums:
            return None
        slope_up, slope_down = [], []
        for c in range(2):
            for shifted, out in ((x_up, slope_up), (x_down, slope_down)):
                slot = 2 * c + (0 if out is slope_up else 1)
                for k in range(3):
                    swung[slot, k, wide] = shifted[c][k]
                out.append(
                    [
                        CROSS
                        * (
                            swung[slot, k, pl.ds(first_y + 1, wide_y)]
                            - swung[slot, k, pl.ds(first_y - 1, wide_y)]
                        )
                        for k in range(3)
                    ]
                )
        out = []
        for k in range(3):
            sum_x = [x_up[c][k] + x_down[c][k] for c in range(3)]
            sum_y = [y_up[c][k] + y_down[c][k] for c in range(3)]
            sum_z = [turn(ups[k][c], -1) + turn(downs[k][c], 1) for c in range(3)]
            out.append(
                [
                    OWN * sum_x[0] + sum_y[0] + (slope_up[1][k] - slope_down[1][k]) + sum_z[0],
                    sum_x[1] + OWN * sum_y[1] + (slope_up[0][k] - slope_down[0][k]) + sum_z[1],
                    sum_x[2] + sum_y[2] + sum_z[2],
                ]
            )
        return out

    def edge_sweep(source, target, stage):
        beside = edge_stage(source, stage)
        wide = pl.ds(first_y, wide_y)
        for k in range(3):
            share = edge_base[3, k, wide]
            for c in range(3):
                target[c, k, wide] = (
                    KEEP * source[c, k, wide] + edge_base[c, k, wide] + share * beside[k][c]
                )

    def neighbours(field, p, x, stage, mode="wide"):
        def load(c, ox, oy):
            return take(field, (c,), (p + ox) * rows, oy, mode)

        ring = (x + 2 * HALO) % wide_x
        outside = ring < 2 * HALO
        where_x = ring if outside else ring - 2 * HALO
        shift = (LANES - 1 - HALO - EDGE * where_x) % LANES
        centre = [load(c, 0, 0) for c in range(3)]
        x_up = [load(c, 1, 0) for c in range(3)]
        x_down = [load(c, -1, 0) for c in range(3)]
        y_up = [load(c, 0, 1) for c in range(3)]
        y_down = [load(c, 0, -1) for c in range(3)]
        slope = [CROSS * (y_up[c] - y_down[c]) for c in range(3)]
        corner = [
            CROSS * (load(c, 1, 1) - load(c, 1, -1)) - CROSS * (load(c, -1, 1) - load(c, -1, -1))
            for c in range(2)
        ]
        tilt = [
            CROSS * (x_up[2] - x_down[2]),
            slope[2],
            CROSS * (x_up[0] - x_down[0]) + slope[1],
        ]
        mine = [centre[0], centre[1], OWN * centre[2]]
        lanes = lax.broadcasted_iota(jnp.int32, centre[0].shape, 1)
        sum_z = []
        for c in range(3):
            end = pltpu.roll(take(sides, (stage, c), rows if outside else 0, 0, mode), shift, 1)
            up = jnp.where(lanes == LANES - 1, end, turn(mine[c] + tilt[c], -1))
            down = jnp.where(lanes == 0, end, turn(mine[c] - tilt[c], 1))
            sum_z.append(up + down)
        return [
            OWN * (x_up[0] + x_down[0]) + (y_up[0] + y_down[0]) + corner[1] + sum_z[0],
            (x_up[1] + x_down[1]) + OWN * (y_up[1] + y_down[1]) + corner[0] + sum_z[1],
            (x_up[2] + x_down[2]) + (y_up[2] + y_down[2]) + sum_z[2],
        ]

    def sweep(source, target, low, high, stage, mode="wide"):
        for x in range(low, high):
            p = x + HALO
            beside = neighbours(source, p, x, stage, mode)
            share = take(base, (3,), p * rows, 0, mode)
            for c in range(3):
                kept = KEEP * take(source, (c,), p * rows, 0, mode)
                fresh = kept + take(base, (c,), p * rows, 0, mode) + share * beside[c]
                put(target, (c,), p * rows, mode, fresh)

    def residual(field, x, stage):
        p = x + HALO
        beside = neighbours(field, p, x, stage, "own")
        g = stiff[own_rows(x)]
        heavy = g * DIAGONAL + MASS_TERM
        return [
            raw[c, x] - heavy * field[c, at(p, 0, True)] + g * beside[c] for c in range(3)
        ]

    wait_halo((0,), halo_sem.at[0])
    unpack_edges(0)
    edge_sweep(edge_base, edge_a, 0)
    edge_stage(edge_a, 1, False)
    greeted = min(1, len(rounds) - 1)
    for number in range(greeted):
        hear(number)
        hello(number + 1)
    pass_on()
    start_sends(2)
    start_sends(3)
    wait_halo((1,), halo_sem.at[1])
    unpack_main(0)
    sweep(base, field_a, -1, ex + 1, 0)

    def restrict(x, carry):
        left = residual(field_a, x, 1)
        return tuple(carry[c] + left[c] for c in range(3))

    sums = by_two(0, ex, restrict, (jnp.zeros((ey, LANES), jnp.float32),) * 3)
    sums = [fold(s) for s in sums] + [stiff_sum]
    stacked = jnp.concatenate([jnp.sum(s, axis=0, keepdims=True) for s in sums] + [zero[:4]], axis=0)
    source_lane = lax.broadcasted_iota(jnp.int32, (LANES, LANES), 0)
    target_lane = lax.broadcasted_iota(jnp.int32, (LANES, LANES), 1)
    gather = (source_lane // BLOCK == lax.rem(target_lane, cz)).astype(jnp.float32)
    grouped = jnp.dot(stacked, gather, precision=EXACT, preferred_element_type=jnp.float32)
    coarse_send[...] = grouped[:4]

    def coarse_copy(x, y, z, dz):
        return pltpu.make_async_remote_copy(
            src_ref=coarse_send,
            dst_ref=coarse_recv.at[reach - dz, me[0] * count_y + me[1]],
            send_sem=coarse_sem.at[0],
            recv_sem=coarse_sem.at[1],
            device_id=(x, y, z),
            device_id_type=MESH,
        )

    def coarse_wait():
        for number in range(1, window + 1):

            @pl.when(levels == number)
            def _():
                for k in range(2):
                    wait_bytes(4 * (number * count_x * count_y - 1), coarse_sem.at[k])

    peers(lambda x, y, z, dz: coarse_copy(x, y, z, dz).start())
    coarse_recv[reach, me[0] * count_y + me[1]] = grouped[:4]

    sweep(field_a, field_b, 0, ex, 1, "own")
    wait_halo((2,), halo_sem.at[2])
    unpack_edges(1)
    edge_sweep(edge_base, edge_a, 0)
    edge_sweep(edge_a, edge_b, 1)
    wait_halo((3,), halo_sem.at[3])
    unpack_main(1)
    for low, high in ((1 - HALO, -1), (ex + 1, ex + HALO - 1)):
        sweep(base, field_a, low, high, 0)
    sweep(base, field_a, -1, ex + 1, 0, "rim")
    for low, high in ((-2, 0), (ex, ex + 2)):
        sweep(field_a, field_b, low, high, 1)
    sweep(field_a, field_b, 0, ex, 1, "rim")
    wait_halo(range(4), halo_sem.at[4])
    finish_relay()
    coarse_wait()

    coarse_rows = -(-(count_y + 1) // 8) * 8
    lane_c = lax.broadcasted_iota(jnp.int32, (coarse_rows, LANES), 1)
    row_c = lax.broadcasted_iota(jnp.int32, (coarse_rows, LANES), 0)
    at_z = me[2] * cz - reach * cz + lane_c
    valid = (
        (row_c < count_y) & (at_z >= 0) & (at_z < cz * count_z) & (lane_c < window * cz)
    )
    slab = [[None] * 4 for _ in range(count_x)]
    for x in range(count_x):
        for c in range(4):
            value = None
            for w in range(window):
                column = jnp.concatenate(
                    [coarse_recv[w, x * count_y + y, c : c + 1] for y in range(count_y)]
                    + [jnp.zeros((coarse_rows - count_y, LANES), jnp.float32)],
                    axis=0,
                )
                value = column if value is None else jnp.where(lane_c // cz == w, column, value)
            slab[x][c] = jnp.where(valid, value, 0.0)
    mass = BLOCK**3 * MASS_TERM
    factor = [slab[x][3] * (BLOCK**2 / BLOCK**3) for x in range(count_x)]
    relax = [
        jnp.where(valid, RELAXATION / (factor[x] * DIAGONAL + mass), 0.0) for x in range(count_x)
    ]
    nothing = jnp.zeros((coarse_rows, LANES), jnp.float32)
    start_w = [[slab[x][c] * relax[x] for c in range(3)] for x in range(count_x)]
    share_w = [factor[x] * relax[x] for x in range(count_x)]
    w = start_w

    def y_shift(value, step):
        return pltpu.roll(value, step % coarse_rows, 0)

    for repeat in range(COARSE - 1):
        fresh = []
        for x in range(count_x):
            here = w[x]
            above = w[x + 1] if x + 1 < count_x else [nothing] * 3
            below = w[x - 1] if x > 0 else [nothing] * 3
            sum_x = [above[c] + below[c] for c in range(3)]
            diff_x = [above[c] - below[c] for c in range(3)]
            y_up = [y_shift(here[c], -1) for c in range(3)]
            y_down = [y_shift(here[c], 1) for c in range(3)]
            sum_y = [y_up[c] + y_down[c] for c in range(3)]
            diff_y = [y_up[c] - y_down[c] for c in range(3)]
            corner_x = y_shift(diff_x[1], -1) - y_shift(diff_x[1], 1)
            corner_y = y_shift(diff_x[0], -1) - y_shift(diff_x[0], 1)
            tilt = [CROSS * diff_x[2], CROSS * diff_y[2], CROSS * (diff_x[0] + diff_y[1])]
            own = [here[0], here[1], OWN * here[2]]
            sum_z = [turn(own[c] + tilt[c], -1) + turn(own[c] - tilt[c], 1) for c in range(3)]
            beside = [
                OWN * sum_x[0] + sum_y[0] + CROSS * corner_x + sum_z[0],
                sum_x[1] + OWN * sum_y[1] + CROSS * corner_y + sum_z[1],
                sum_x[2] + sum_y[2] + sum_z[2],
            ]
            fresh.append(
                [
                    KEEP * here[c] + start_w[x][c] + share_w[x] * beside[c]
                    for c in range(3)
                ]
            )
        w = fresh

    for x in range(count_x + 2):
        for c in range(3):
            inside = 1 <= x <= count_x
            coarse_w[x, c, pl.ds(0, 8)] = jnp.zeros((8, LANES), jnp.float32)
            coarse_w[x, c, pl.ds(8, coarse_rows)] = w[x - 1][c] if inside else nothing
    stack_w[pl.ds(24, 8)] = zero
    for xc in range(3):
        for c in range(3):
            stack_w[pl.ds(3 * (3 * xc + c), 3)] = coarse_w[me[0] + xc, c, pl.ds(7 + me[1], 3)]
    inner = lax.rem(target_lane, EDGE) < HALO
    first_cell_z, last_cell_z = reach * cz, (reach + 1) * cz - 1
    pick_low = jnp.where(inner, first_cell_z - 1, first_cell_z)
    pick_high = jnp.where(inner, last_cell_z, last_cell_z + 1)
    picks = (
        first_cell_z + target_lane // BLOCK,
        pick_low,
        pick_high,
        jnp.where(target_lane < LANES // 2, pick_low, pick_high),
    )
    widen = jnp.concatenate([(source_lane == pick).astype(jnp.float32) for pick in picks], axis=1)
    wide_all = jnp.dot(stack_w[...], widen, precision=EXACT, preferred_element_type=jnp.float32)

    def drawn(xc, c, k):
        parts = []
        for j in range(3):
            line = 3 * (3 * xc + c) + j
            piece = wide_all[line : line + 1, k * LANES : (k + 1) * LANES]
            parts.append(jnp.broadcast_to(piece, (wide_y, LANES)))
        return jnp.where(row_y < HALO, parts[0], jnp.where(row_y < HALO + ey, parts[1], parts[2]))

    wide = pl.ds(first_y, wide_y)
    for c in range(3):
        for xc in range(3):
            value = drawn(xc, c, 0)
            for plane in range(3):
                spread_w[c, pl.ds((3 * xc + plane) * rows + first_y, wide_y)] = value
        edge_a[c, 0, wide] = drawn(1, c, 1)
        edge_a[c, 1, wide] = drawn(1, c, 2)
        edge_a[c, 2, wide] = jnp.where(upper_x, drawn(2, c, 3), drawn(0, c, 3))
    beside = edge_stage(edge_a, 0)
    for k in range(3):
        share = edge_base[3, k, wide]
        for c in range(3):
            edge_b[c, k, wide] = (
                edge_b[c, k, wide] + KEEP * edge_a[c, k, wide] + share * beside[k][c]
            )
    edge_sweep(edge_b, edge_a, 1)
    edge_stage(edge_a, 2, False)
    for plane, x in ((1, -2), (2, -1), (3, 0), (4, ex // 2), (5, ex - 1), (6, ex), (7, ex + 1)):
        images = neighbours(spread_w, plane, x, 0)
        for c in range(3):
            image_w[c, at(plane)] = images[c]

    def correct(p, carry):
        kind = (
            jnp.int32(1)
            + jnp.int32(p >= HALO - 1)
            + jnp.int32(p >= HALO)
            + jnp.int32(p >= HALO + 1)
            + jnp.int32(p >= HALO + ex - 1)
            + jnp.int32(p >= HALO + ex)
            + jnp.int32(p >= HALO + ex + 1)
        )
        share = base[3, at(p)]
        for c in range(3):
            field_b[c, at(p)] = (
                field_b[c, at(p)] + KEEP * spread_w[c, at(kind)] + share * image_w[c, at(kind)]
            )
        return carry

    by_two(2, wide_x - 2, correct, 0)
    sweep(field_b, field_a, -1, ex + 1, 1)

    def squares(x, carry):
        left = residual(field_a, x, 2)
        for c in range(3):
            out_ref[c, x] = field_a[c, at(x + HALO, 0, True)]
        return carry + fold(sum(value * value for value in left))

    left_sum = by_two(0, ex, squares, zero)
    load_total = jnp.sum(jnp.sum(load_sum, axis=0, keepdims=True), axis=1, keepdims=True)
    left_total = jnp.sum(jnp.sum(left_sum, axis=0, keepdims=True), axis=1, keepdims=True)
    first = lax.broadcasted_iota(jnp.int32, (1, LANES), 1) == 0
    mine = jnp.where(first, load_total, left_total)
    norm_send[...] = mine

    for number in range(greeted, len(rounds)):
        if number > greeted:
            hello(number)
        hear(number)
    for x in reversed(ring_x):
        for z in reversed(ring_z):
            for y in reversed(ring_y):
                if x is not me[0] or y is not me[1] or z is not me[2]:
                    pltpu.make_async_remote_copy(
                        src_ref=norm_send,
                        dst_ref=norm_recv.at[my_id],
                        send_sem=norm_sem.at[0],
                        recv_sem=norm_sem.at[1],
                        device_id=(x, y, z),
                        device_id_type=MESH,
                    ).start()
    norm_recv[my_id] = mine
    others = norm_recv.at[pl.ds(0, total - 1)]
    for k in range(2):
        pltpu.make_async_copy(others, others, norm_sem.at[k]).wait()
    summed = jnp.sum(norm_recv[...], axis=0)
    nodes = 3 * ex * ey * ez * total
    norms_ref[...] = jnp.sqrt(summed / nodes)


def on_device(counts, right_side, damage):
    _, ex, ey, ez = right_side.shape
    assert ez == LANES and ex * EDGE == LANES and 2 * EDGE * EDGE == LANES
    assert ex % BLOCK == 0 and ey == BLOCK and ex == BLOCK
    cz = ez // BLOCK
    wide_x = ex + 2 * HALO
    rows = ey + 2 * YPAD
    flat = wide_x * rows
    total = counts[0] * counts[1] * counts[2]
    window = 2 * (-(-COARSE // cz)) + 1
    coarse_rows = -(-(counts[1] + 1) // 8) * 8
    rounds = 0
    while window // 2 << rounds < counts[2] - 1:
        rounds += 1
    f32 = jnp.float32

    def vmem(*shape):
        return pltpu.VMEM(shape + (LANES,), f32)

    dma = pltpu.SemaphoreType.DMA
    near, layers = len(NEAR), len(LAYERS)
    displacement, norms = pl.pallas_call(
        functools.partial(kernel, counts, (ex, ey, ez)),
        out_shape=(
            pltpu.VMEM(right_side.shape, f32),
            pltpu.VMEM((1, LANES), f32),
        ),
        in_specs=[pl.BlockSpec(memory_space=pl.ANY)] * 2,
        out_specs=(
            pl.BlockSpec(memory_space=pltpu.VMEM),
            pl.BlockSpec(memory_space=pltpu.VMEM),
        ),
        scratch_shapes=[
            vmem(3, ex, ey),
            vmem(ex * ey),
            pltpu.VMEM((ex, ey, LANES), jnp.int32),
            vmem(4, flat),
            vmem(3, flat),
            vmem(3, flat),
            vmem(4, 3, rows),
            vmem(3, 3, rows),
            vmem(3, 3, rows),
            vmem(3, 3, 2 * rows),
            vmem(4, 3, rows),
            vmem(len(FAR), ex),
            vmem(2, layers, ex),
            vmem(2, layers, ex),
            vmem(2, 2, near, 2),
            vmem(2, 2, near, 2),
            vmem(2, 2, layers, HALO),
            vmem(2, 2, layers, HALO),
            vmem(3, 4, rows),
            vmem(2, ey),
            vmem(2, 3, rows),
            vmem(2, 2, 4, 2),
            vmem(2, 2, 3, 4, 2),
            vmem(2, 2, 2, 2),
            vmem(2, 2, 2, 3, 2),
            vmem(4),
            vmem(window, counts[0] * counts[1], 4),
            vmem(counts[0] + 2, 3, 8 + coarse_rows),
            vmem(32),
            vmem(3, 9 * rows),
            vmem(3, 9 * rows),
            vmem(1),
            vmem(total, 1),
            vmem(4 * EDGE * LANES, 1),
            dma((2,)),
            dma((7,)),
            dma((2,)),
            dma((2,)),
            pltpu.SemaphoreType.REGULAR((max(1, rounds), 2)),
        ],
        compiler_params=pltpu.CompilerParams(collective_id=0, has_side_effects=True),
    )(right_side, damage)
    return displacement, norms[0, :2]


def solution(mesh):
    counts = tuple(mesh.shape[axis] for axis in AXES)
    placed = (P(None, "gx", "gy", "gz"), P("gx", "gy", "gz"))
    return jax.shard_map(
        functools.partial(on_device, counts),
        mesh=mesh,
        in_specs=placed,
        out_specs=(P(None, "gx", "gy", "gz"), P()),
        check_vma=False,
    )
```

```python
import functools

import jax
import jax.numpy as jnp
from jax import lax
from jax.experimental import pallas as pl
from jax.experimental.pallas import tpu as pltpu
from jax.sharding import PartitionSpec as P

BLOCK = 16
COARSE = 8
FLOOR_STIFFNESS = 0.05
MASS_TERM = 0.001
COUPLING = 2.5
RELAXATION = 0.6
KEEP = 1.0 - RELAXATION
DIAGONAL = 6.0 + 2.0 * COUPLING
OWN = 1.0 + COUPLING
CROSS = 0.25 * COUPLING
AXES = ("gx", "gy", "gz")
HALO = 4
EDGE = 2 * HALO
LANES = 128
YPAD = 8
MESH = pl.DeviceIdType.MESH
NEAR = ((0, 1), (1, 1), (2, 1), (3, 1), (0, 2), (1, 2), (2, 2))
FAR = ((3, 2), (0, 3), (1, 3), (2, 3), (3, 3), (0, 4), (1, 4), (2, 4))
LAYERS = NEAR + FAR


def directions():
    out = []
    for dx in (-1, 0, 1):
        for dy in (-1, 0, 1):
            for dz in (-1, 0, 1):
                if (dx, dy, dz) != (0, 0, 0):
                    out.append((dx, dy, dz))
    return sorted(out, key=lambda d: -sum(abs(step) for step in d))


DIRECTIONS = directions()


UNROLL = 24


def by_two(low, high, body, carry):
    trips = -(-(high - low) // UNROLL)
    size = -(-(high - low) // trips)
    whole = (high - low) // size

    def several(trip, carry):
        for k in range(size):
            carry = body(low + size * trip + k, carry)
        return carry

    if whole > 1:
        carry = lax.fori_loop(0, whole, several, carry)
    else:
        carry = several(0, carry)
    for k in range(low + whole * size, high):
        carry = body(k, carry)
    return carry


def kernel(
    counts,
    extent,
    load_ref,
    damage_ref,
    out_ref,
    norms_ref,
    raw,
    stiff,
    harm,
    base,
    field_a,
    field_b,
    edge_base,
    edge_a,
    edge_b,
    sides,
    swung,
    relay,
    y_send,
    y_recv,
    xyn_send,
    xyn_recv,
    xy_send,
    xy_recv,
    p_all,
    q_send,
    q_all,
    py_send,
    py_recv,
    qy_send,
    qy_recv,
    coarse_send,
    coarse_recv,
    coarse_w,
    stack_w,
    spread_w,
    image_w,
    norm_send,
    norm_recv,
    amount,
    local_sem,
    halo_sem,
    coarse_sem,
    norm_sem,
    hello_sem,
):
    count_x, count_y, count_z = counts
    ex, ey, ez = extent
    cz = ez // BLOCK
    total = count_x * count_y * count_z
    wide_x = ex + 2 * HALO
    ypad = YPAD
    rows = ey + 2 * ypad
    wide_y = ey + 2 * HALO
    first_y = ypad - HALO
    me = tuple(lax.axis_index(axis) for axis in AXES)
    my_id = (me[0] * count_y + me[1]) * count_z + me[2]

    def place(index):
        return (
            index // (count_y * count_z),
            lax.rem(index // count_z, count_y),
            lax.rem(index, count_z),
        )

    harm_copy = pltpu.make_async_copy(damage_ref, harm, local_sem.at[0])
    load_copy = pltpu.make_async_copy(load_ref, raw, local_sem.at[1])
    harm_copy.start()
    load_copy.start()
    barrier = pltpu.get_barrier_semaphore()

    reach = -(-COARSE // cz)
    window = 2 * reach + 1

    def around(here, count):
        out = [here]
        for step in range(1, count):
            there = here + step
            out.append(jnp.where(there >= count, there - count, there))
        return out

    ring_x, ring_y, ring_z = (around(me[axis], counts[axis]) for axis in range(3))

    def peers(act):
        for dz in sorted(range(-reach, reach + 1), key=lambda step: -abs(step)):
            z = me[2] + dz

            @pl.when((z >= 0) & (z < count_z))
            def _():
                for x in reversed(ring_x):
                    for y in reversed(ring_y):
                        if dz != 0 or x is not me[0] or y is not me[1]:
                            act(x, y, z, dz)

    def greet(x, y, z, dz):
        pl.semaphore_signal(barrier, inc=1, device_id=(x, y, z), device_id_type=MESH)

    peers(greet)
    levels = jnp.minimum(me[2] + reach, count_z - 1) - jnp.maximum(me[2] - reach, 0) + 1

    def exists(dx, dy, dz):
        ok = None
        for axis, step in enumerate((dx, dy, dz)):
            if step == 0:
                continue
            here = me[axis] + step
            good = (here >= 0) & (here < counts[axis])
            ok = good if ok is None else ok & good
        return ok

    def block(x):
        return pl.ds((HALO + x) * rows + ypad, ey)

    for xs in range(2):

        @pl.when(jnp.logical_not(exists(2 * xs - 1, 0, 0)))
        def _():
            for part in range(HALO):
                for f in range(4):
                    x = part - HALO if xs == 0 else ex + part
                    base[f, block(x)] = jnp.zeros((ey, LANES), jnp.float32)

        for ys in range(2):

            @pl.when(jnp.logical_not(exists(2 * xs - 1, 2 * ys - 1, 0)))
            def _():
                xyn_recv[xs, ys] = jnp.zeros((len(NEAR), 2, LANES), jnp.float32)
                xy_recv[xs, ys] = jnp.zeros((len(LAYERS), HALO, LANES), jnp.float32)

    for ys in range(2):

        @pl.when(jnp.logical_not(exists(0, 2 * ys - 1, 0)))
        def _():
            y_recv[ys] = jnp.zeros((len(LAYERS), ex, LANES), jnp.float32)

    lane_own = lax.broadcasted_iota(jnp.int32, (ey, LANES), 1)
    lane = lax.broadcasted_iota(jnp.int32, (wide_y, LANES), 1)
    row_y = lax.broadcasted_iota(jnp.int32, (wide_y, LANES), 0)
    lower = lax.rem(lane, EDGE) < HALO
    at_y = me[1] * ey + row_y - HALO
    good_y = (at_y >= 0) & (at_y < ey * count_y)
    has_back, has_front = me[2] > 0, me[2] < count_z - 1
    upper_x = lax.rem(lane // (HALO * EDGE), 2) == 0
    high_z = lane >= LANES // 2
    good_x = (upper_x & (me[0] < count_x - 1)) | (~upper_x & (me[0] > 0))
    good_z = (high_z & (lower | has_front)) | (~high_z & (~lower | has_back))
    goods = (
        good_y & (~lower | has_back),
        good_y & (lower | has_front),
        good_y & good_x & good_z,
    )

    def fold(value):
        return jnp.sum(value.reshape(ey // 8, 8, LANES), axis=0)

    zero = jnp.zeros((8, LANES), jnp.float32)

    def pick(values, chosen):
        parts, rest = [], values
        for _ in range(3):
            part = rest.astype(jnp.bfloat16).astype(jnp.float32)
            parts.append(part)
            rest = rest - part
        joined = jnp.concatenate(parts, axis=0).astype(jnp.bfloat16)
        out = jnp.dot(joined, chosen.astype(jnp.bfloat16), preferred_element_type=jnp.float32)
        height = values.shape[0]
        return out[:height] + out[height : 2 * height] + out[2 * height :]

    harm_copy.wait()
    load_copy.wait()

    def own_rows(x):
        return pl.ds(x * ey, ey)

    load_sum = zero
    stiff_sum = zero
    packed = [None] * 4
    for x in range(ex):
        level = 1.0 - harm[x].astype(jnp.float32) / 15.0
        g = level * level * (1.0 - FLOOR_STIFFNESS) + FLOOR_STIFFNESS
        inv = RELAXATION / (g * DIAGONAL + MASS_TERM)
        stiff[own_rows(x)] = g
        stiff_sum = stiff_sum + fold(g)
        values = []
        squared = None
        for c in range(3):
            load = raw[c, x]
            values.append(load * inv)
            squared = load * load if squared is None else squared + load * load
        load_sum = load_sum + fold(squared)
        values.append(g * inv)
        for f in range(4):
            base[f, block(x)] = values[f]
            moved = pltpu.roll(values[f], (EDGE * x + HALO) % LANES, 1)
            packed[f] = moved if x == 0 else jnp.where(lane_own // EDGE == x, moved, packed[f])
    for f in range(4):
        p_all[1, f, pl.ds(ypad, ey)] = packed[f]
        for phase in range(2):
            py_send[phase, 0, f] = packed[f][2 * phase : 2 * phase + 2]
            py_send[phase, 1, f] = packed[f][ey - 2 - 2 * phase : ey - 2 * phase]
    width = HALO * EDGE
    for xs in range(2):
        joined = None
        for f in range(4):
            shift = width * f - (0 if xs == 0 else (ex - HALO) * EDGE)
            moved = pltpu.roll(packed[f], shift % LANES, 1)
            joined = moved if f == 0 else jnp.where(lane_own // width == f, moved, joined)
        q_send[xs] = joined
        for phase in range(2):
            qy_send[phase, xs, 0] = joined[2 * phase : 2 * phase + 2]
            qy_send[phase, xs, 1] = joined[ey - 2 - 2 * phase : ey - 2 * phase]
    def pack_main(late):
        for side in range(2):
            for i, (f, layer) in enumerate(LAYERS):
                start = HALO * rows + ypad + (layer - 1 if side == 0 else ey - layer)
                if (i >= len(NEAR)) == late:
                    for half in range(ex // 8):
                        y_send[side, i, pl.ds(8 * half, 8)] = base[
                            f, pl.ds(start + 8 * half * rows, 8, stride=rows)
                        ]
                for xs in range(2):
                    if late:
                        x0 = 0 if xs == 0 else ex - HALO
                        xy_send[xs, side, i] = base[f, pl.ds(start + x0 * rows, HALO, stride=rows)]
                    elif i < len(NEAR):
                        x0 = 0 if xs == 0 else ex - 2
                        xyn_send[xs, side, i] = base[f, pl.ds(start + x0 * rows, 2, stride=rows)]

    pack_main(False)
    pl.semaphore_wait(barrier, levels * count_x * count_y - 1)

    def pieces(d, phase):
        dx, dy, dz = d
        xs, ys = (dx + 1) // 2, (dy + 1) // 2
        out = []
        near, far = pl.ds(0, len(NEAR)), pl.ds(len(NEAR), len(FAR))
        own = pl.ds(ypad, ey)
        edges, late = phase % 2 == 0, phase // 2
        if dy == 0:
            if late:
                return out
            if dz == 0 and not edges:
                for part in range(HALO):
                    src_x = part if dx < 0 else ex - HALO + part
                    dst_x = ex + part if dx < 0 else part - HALO
                    out.append((base.at[:, block(src_x)], base.at[:, block(dst_x)], 4 * ey))
            if dx == 0 and edges:
                out.append((p_all.at[1, :, own], p_all.at[1 - dz, :, own], 4 * ey))
            elif edges:
                out.append((q_send.at[xs], q_all.at[1 - xs, 1 - dz, own], ey))
            return out
        if edges:
            if dx == 0:
                out.append((py_send.at[late, ys], py_recv.at[late, 1 - ys, 1 - dz], 8))
            else:
                out.append((qy_send.at[late, xs, ys], qy_recv.at[late, 1 - xs, 1 - ys, 1 - dz], 2))
        elif dz == 0 and dx == 0:
            part = far if late else near
            size = len(FAR) if late else len(NEAR)
            out.append((y_send.at[ys, part], y_recv.at[1 - ys, part], size * ex))
        elif dz == 0 and not late:
            out.append((xyn_send.at[xs, ys], xyn_recv.at[1 - xs, 1 - ys], 2 * len(NEAR)))
        elif dz == 0:
            out.append((xy_send.at[xs, ys], xy_recv.at[1 - xs, 1 - ys], HALO * len(LAYERS)))
        return out

    odd = lax.rem(me[1], 2) == 1
    relayed = {
        1: odd & (me[1] + 2 < count_y),
        -1: jnp.logical_not(odd) & (me[1] >= 2),
    }
    relaying = {
        1: jnp.logical_not(odd) & (me[1] + 2 < count_y),
        -1: odd & (me[1] >= 3),
    }

    def far_copy(src, ys, device_y, final):
        return pltpu.make_async_remote_copy(
            src_ref=src,
            dst_ref=y_recv.at[1 - ys, pl.ds(len(NEAR), len(FAR))] if final else relay,
            send_sem=halo_sem.at[5 if final else 4],
            recv_sem=halo_sem.at[3 if final else 6],
            device_id=(me[0], device_y, me[2]),
            device_id_type=MESH,
        )

    def send_to_relay():
        for dy in (-1, 1):
            ys = (dy + 1) // 2

            @pl.when(relayed[dy])
            def _():
                far_copy(y_send.at[ys, pl.ds(len(NEAR), len(FAR))], ys, me[1] + 2 * dy, False).start()

    def pass_on():
        for dy in (-1, 1):

            @pl.when(relaying[dy])
            def _():
                wait_bytes(len(FAR) * ex, halo_sem.at[6])
                far_copy(relay, (1 - dy) // 2, me[1] + dy, True).start()

    def finish_relay():
        @pl.when(relaying[-1] | relaying[1])
        def _():
            wait_bytes(len(FAR) * ex, halo_sem.at[5])

    one_sided = (me[1] == 0) | (me[1] == count_y - 1)

    def start_sends(phase, only=None):
        ordered = []
        for turn_number in range(2):
            for number, d in enumerate(DIRECTIONS):
                if d[1] != 0:
                    ordered.append((number, d, odd == ((d[1] > 0) == (turn_number == 0))))
        ordered += [(number, d, None) for number, d in enumerate(DIRECTIONS) if d[1] == 0]
        for number, d, condition in ordered:
            parts = pieces(d, phase)
            if not parts:
                continue
            here = exists(*d) if only is None else exists(*d) & only
            if condition is not None:
                here = here & condition
            if phase == 3 and d[0] == 0:
                here = here & jnp.logical_not(relayed[d[1]])

            @pl.when(here)
            def _():
                for src, dst, _ in parts:
                    pltpu.make_async_remote_copy(
                        src_ref=src,
                        dst_ref=dst,
                        send_sem=halo_sem.at[4],
                        recv_sem=halo_sem.at[phase],
                        device_id=tuple(me[axis] + d[axis] for axis in range(3)),
                        device_id_type=MESH,
                    ).start()

    start_sends(0)
    start_sends(1)
    pack_main(True)
    send_to_relay()
    start_sends(2, one_sided)
    start_sends(3, one_sided)

    def wait_bytes(size, sem):
        span = amount.at[pl.ds(0, size)]
        pltpu.make_async_copy(span, span, sem).wait()

    sides_of = [
        (here > 0).astype(jnp.int32) + (here < count - 1).astype(jnp.int32)
        for here, count in zip(me, counts)
    ]
    most = [min(2, count - 1) for count in counts]

    def wait_halo(phases, sem):
        for number_x in range(min(1, most[0]), most[0] + 1):
            for number_y in range(min(1, most[1]), most[1] + 1):
                for number_z in range(min(1, most[2]), most[2] + 1):
                    have = (number_x, number_y, number_z)
                    size = 0
                    for d in DIRECTIONS:
                        if d == tuple(-abs(step) for step in d):
                            times = 1
                            for step, number in zip(d, have):
                                times *= number if step else 1
                            for phase in phases:
                                size += times * sum(part[2] for part in pieces(d, phase))

                    @pl.when(
                        (sides_of[0] == number_x)
                        & (sides_of[1] == number_y)
                        & (sides_of[2] == number_z)
                    )
                    def _():
                        wait_bytes(size, sem)

    rounds = []
    radius = reach
    while radius < count_z - 1:
        rounds.append(radius)
        radius *= 2

    def hello(number):
        for side, step in enumerate((-rounds[number], rounds[number])):

            @pl.when(exists(0, 0, step))
            def _():
                pl.semaphore_signal(
                    hello_sem.at[number, 1 - side],
                    inc=1,
                    device_id=(me[0], me[1], me[2] + step),
                    device_id_type=MESH,
                )

    def hear(number):
        for side, step in enumerate((-rounds[number], rounds[number])):

            @pl.when(exists(0, 0, step))
            def _():
                pl.semaphore_wait(hello_sem.at[number, side], 1)

    if rounds:
        hello(0)

    def unpack_main(phase):
        for side in range(2):
            for i, (f, layer) in enumerate(LAYERS):
                y = ypad - layer if side == 0 else ypad + ey + layer - 1
                if (i < len(NEAR)) == (phase == 0):
                    for half in range(ex // 8):
                        base[f, pl.ds((HALO + 8 * half) * rows + y, 8, stride=rows)] = y_recv[
                            side, i, pl.ds(8 * half, 8)
                        ]
                for xs in range(2):
                    if phase == 1:
                        x0 = 0 if xs == 0 else HALO + ex
                        base[f, pl.ds(x0 * rows + y, HALO, stride=rows)] = xy_recv[xs, side, i]
                    elif i < len(NEAR):
                        x0 = HALO - 2 if xs == 0 else HALO + ex
                        base[f, pl.ds(x0 * rows + y, 2, stride=rows)] = xyn_recv[xs, side, i]

    def unpack_edges(phase):
        for side in range(2):
            start = ypad - 2 - 2 * phase if side == 0 else ypad + ey + 2 * phase
            for dz in range(3):
                for f in range(4):
                    p_all[dz, f, pl.ds(start, 2)] = py_recv[phase, side, dz, f]
                for xs in range(2):
                    q_all[xs, dz, pl.ds(start, 2)] = qy_recv[phase, xs, side, dz]
        wide = pl.ds(first_y, wide_y)
        for f in range(4):
            back, here, front = (p_all[dz, f, wide] for dz in range(3))
            edge_base[f, 0, wide] = jnp.where(goods[0], jnp.where(lower, back, here), 0.0)
            edge_base[f, 1, wide] = jnp.where(goods[1], jnp.where(lower, here, front), 0.0)
        low, high = [], []
        for xs in range(2):
            back, here, front = (q_all[xs, dz, wide] for dz in range(3))
            low.append(jnp.where(lower, back, here))
            high.append(jnp.where(lower, here, front))
        for f in range(4):
            quarter = [
                pltpu.roll(value, (width * (k - f)) % LANES, 1)
                for k, value in enumerate((low[1], low[0], high[1], high[0]))
            ]
            merged = jnp.where(
                high_z,
                jnp.where(upper_x, quarter[2], quarter[3]),
                jnp.where(upper_x, quarter[0], quarter[1]),
            )
            edge_base[f, 2, wide] = jnp.where(goods[2], merged, 0.0)

    def at(p, dy=0, own=False):
        if own:
            return pl.ds(p * rows + ypad + dy, ey)
        return pl.ds(p * rows + first_y + dy, wide_y)

    outer = lax.broadcasted_iota(jnp.int32, (EDGE, LANES), 0) < HALO

    def take(ref, index, start, dy, mode):
        if mode == "wide":
            return ref[index + (pl.ds(start + first_y + dy, wide_y),)]
        if mode == "own":
            return ref[index + (pl.ds(start + ypad + dy, ey),)]
        low = ref[index + (pl.ds(start + first_y + dy, EDGE),)]
        high = ref[index + (pl.ds(start + ypad + ey - HALO + dy, EDGE),)]
        return jnp.where(outer, low, high)

    def put(ref, index, start, mode, value):
        if mode == "wide":
            ref[index + (pl.ds(start + first_y, wide_y),)] = value
        elif mode == "own":
            ref[index + (pl.ds(start + ypad, ey),)] = value
        else:
            ref[index + (pl.ds(start + first_y, HALO),)] = value[:HALO]
            ref[index + (pl.ds(start + ypad + ey, HALO),)] = value[HALO:]

    cell = lane // EDGE
    last_cell = cell == LANES // EDGE - 1
    first_cell = cell == 0
    half_cell = LANES // EDGE // 2

    def turn(value, step):
        return pltpu.roll(value, step % LANES, 1)

    def edge_shift(values, step):
        low, high, outer = values
        near = [turn(value, -step * EDGE) for value in values]
        half = LANES // 2
        if step > 0:
            far = turn(jnp.where(cell == half_cell, outer, low), half - EDGE)
            return [
                jnp.where(last_cell, near[2], near[0]),
                jnp.where(last_cell, far, near[1]),
                jnp.where(last_cell, near[1], jnp.where(cell == half_cell - 1, far, near[2])),
            ]
        far = turn(jnp.where(cell == half_cell - 1, outer, high), half + EDGE)
        return [
            jnp.where(first_cell, far, near[0]),
            jnp.where(first_cell, near[2], near[1]),
            jnp.where(first_cell, near[0], jnp.where(cell == half_cell, far, near[2])),
        ]

    def edge_stage(field, stage, sums=True):
        wide = pl.ds(first_y, wide_y)

        def load(c, oy):
            return [field[c, k, pl.ds(first_y + oy, wide_y)] for k in range(3)]

        centre = [load(c, 0) for c in range(3)]
        y_up = [load(c, 1) for c in range(3)]
        y_down = [load(c, -1) for c in range(3)]
        slope = [[CROSS * (y_up[c][k] - y_down[c][k]) for k in range(3)] for c in range(3)]
        used = range(3) if sums else (0, 2)
        x_up = {c: edge_shift(centre[c], 1) for c in used}
        x_down = {c: edge_shift(centre[c], -1) for c in used}
        ups, downs = [], []
        for k in range(3):
            tilt = [
                CROSS * (x_up[2][k] - x_down[2][k]),
                slope[2][k],
                CROSS * (x_up[0][k] - x_down[0][k]) + slope[1][k],
            ]
            mine = [centre[0][k], centre[1][k], OWN * centre[2][k]]
            ups.append([mine[c] + tilt[c] for c in range(3)])
            downs.append([mine[c] - tilt[c] for c in range(3)])
        front = lax.rem(lane, EDGE) == HALO
        for c in range(3):
            sides[stage, c, pl.ds(first_y, wide_y)] = jnp.where(front, ups[1][c], turn(downs[0][c], 2))
            sides[stage, c, pl.ds(rows + first_y, wide_y)] = jnp.where(
                front, turn(ups[2][c], LANES // 2), turn(downs[2][c], 2)
            )
        if not sums:
            return None
        slope_up, slope_down = [], []
        for c in range(2):
            for shifted, out in ((x_up, slope_up), (x_down, slope_down)):
                slot = 2 * c + (0 if out is slope_up else 1)
                for k in range(3):
                    swung[slot, k, wide] = shifted[c][k]
                out.append(
                    [
                        CROSS
                        * (
                            swung[slot, k, pl.ds(first_y + 1, wide_y)]
                            - swung[slot, k, pl.ds(first_y - 1, wide_y)]
                        )
                        for k in range(3)
                    ]
                )
        out = []
        for k in range(3):
            sum_x = [x_up[c][k] + x_down[c][k] for c in range(3)]
            sum_y = [y_up[c][k] + y_down[c][k] for c in range(3)]
            sum_z = [turn(ups[k][c], -1) + turn(downs[k][c], 1) for c in range(3)]
            out.append(
                [
                    OWN * sum_x[0] + sum_y[0] + (slope_up[1][k] - slope_down[1][k]) + sum_z[0],
                    sum_x[1] + OWN * sum_y[1] + (slope_up[0][k] - slope_down[0][k]) + sum_z[1],
                    sum_x[2] + sum_y[2] + sum_z[2],
                ]
            )
        return out

    def edge_sweep(source, target, stage):
        beside = edge_stage(source, stage)
        wide = pl.ds(first_y, wide_y)
        for k in range(3):
            share = edge_base[3, k, wide]
            for c in range(3):
                target[c, k, wide] = (
                    KEEP * source[c, k, wide] + edge_base[c, k, wide] + share * beside[k][c]
                )

    def neighbours(field, p, x, stage, mode="wide"):
        def load(c, ox, oy):
            return take(field, (c,), (p + ox) * rows, oy, mode)

        ring = (x + 2 * HALO) % wide_x
        outside = ring < 2 * HALO
        where_x = ring if outside else ring - 2 * HALO
        shift = (LANES - 1 - HALO - EDGE * where_x) % LANES
        centre = [load(c, 0, 0) for c in range(3)]
        x_up = [load(c, 1, 0) for c in range(3)]
        x_down = [load(c, -1, 0) for c in range(3)]
        y_up = [load(c, 0, 1) for c in range(3)]
        y_down = [load(c, 0, -1) for c in range(3)]
        slope = [CROSS * (y_up[c] - y_down[c]) for c in range(3)]
        corner = [
            CROSS * (load(c, 1, 1) - load(c, 1, -1)) - CROSS * (load(c, -1, 1) - load(c, -1, -1))
            for c in range(2)
        ]
        tilt = [
            CROSS * (x_up[2] - x_down[2]),
            slope[2],
            CROSS * (x_up[0] - x_down[0]) + slope[1],
        ]
        mine = [centre[0], centre[1], OWN * centre[2]]
        lanes = lax.broadcasted_iota(jnp.int32, centre[0].shape, 1)
        sum_z = []
        for c in range(3):
            end = pltpu.roll(take(sides, (stage, c), rows if outside else 0, 0, mode), shift, 1)
            up = jnp.where(lanes == LANES - 1, end, turn(mine[c] + tilt[c], -1))
            down = jnp.where(lanes == 0, end, turn(mine[c] - tilt[c], 1))
            sum_z.append(up + down)
        return [
            OWN * (x_up[0] + x_down[0]) + (y_up[0] + y_down[0]) + corner[1] + sum_z[0],
            (x_up[1] + x_down[1]) + OWN * (y_up[1] + y_down[1]) + corner[0] + sum_z[1],
            (x_up[2] + x_down[2]) + (y_up[2] + y_down[2]) + sum_z[2],
        ]

    def sweep(source, target, low, high, stage, mode="wide"):
        for x in range(low, high):
            p = x + HALO
            beside = neighbours(source, p, x, stage, mode)
            share = take(base, (3,), p * rows, 0, mode)
            for c in range(3):
                kept = KEEP * take(source, (c,), p * rows, 0, mode)
                fresh = kept + take(base, (c,), p * rows, 0, mode) + share * beside[c]
                put(target, (c,), p * rows, mode, fresh)

    def residual(field, x, stage):
        p = x + HALO
        beside = neighbours(field, p, x, stage, "own")
        g = stiff[own_rows(x)]
        heavy = g * DIAGONAL + MASS_TERM
        return [
            raw[c, x] - heavy * field[c, at(p, 0, True)] + g * beside[c] for c in range(3)
        ]

    wait_halo((0,), halo_sem.at[0])
    unpack_edges(0)
    edge_sweep(edge_base, edge_a, 0)
    edge_stage(edge_a, 1, False)
    greeted = min(1, len(rounds) - 1)
    for number in range(greeted):
        hear(number)
        hello(number + 1)
    pass_on()
    start_sends(2, jnp.logical_not(one_sided))
    start_sends(3, jnp.logical_not(one_sided))
    wait_halo((1,), halo_sem.at[1])
    unpack_main(0)
    sweep(base, field_a, -1, ex + 1, 0)

    def restrict(x, carry):
        left = residual(field_a, x, 1)
        return tuple(carry[c] + left[c] for c in range(3))

    sums = by_two(0, ex, restrict, (jnp.zeros((ey, LANES), jnp.float32),) * 3)
    sums = [fold(s) for s in sums] + [stiff_sum]
    stacked = jnp.concatenate([jnp.sum(s, axis=0, keepdims=True) for s in sums] + [zero[:4]], axis=0)
    source_lane = lax.broadcasted_iota(jnp.int32, (LANES, LANES), 0)
    target_lane = lax.broadcasted_iota(jnp.int32, (LANES, LANES), 1)
    gather = (source_lane // BLOCK == lax.rem(target_lane, cz)).astype(jnp.float32)
    grouped = pick(stacked, gather)
    coarse_send[...] = grouped[:4]

    def coarse_copy(x, y, z, dz):
        return pltpu.make_async_remote_copy(
            src_ref=coarse_send,
            dst_ref=coarse_recv.at[reach - dz, me[0] * count_y + me[1]],
            send_sem=coarse_sem.at[0],
            recv_sem=coarse_sem.at[1],
            device_id=(x, y, z),
            device_id_type=MESH,
        )

    def coarse_wait():
        for number in range(1, window + 1):

            @pl.when(levels == number)
            def _():
                for k in range(2):
                    wait_bytes(4 * (number * count_x * count_y - 1), coarse_sem.at[k])

    peers(lambda x, y, z, dz: coarse_copy(x, y, z, dz).start())
    coarse_recv[reach, me[0] * count_y + me[1]] = grouped[:4]

    sweep(field_a, field_b, 0, ex, 1, "own")
    wait_halo((2,), halo_sem.at[2])
    unpack_edges(1)
    edge_sweep(edge_base, edge_a, 0)
    edge_sweep(edge_a, edge_b, 1)
    wait_halo((3,), halo_sem.at[3])
    unpack_main(1)
    for low, high in ((1 - HALO, -1), (ex + 1, ex + HALO - 1)):
        sweep(base, field_a, low, high, 0)
    sweep(base, field_a, -1, ex + 1, 0, "rim")
    for low, high in ((-2, 0), (ex, ex + 2)):
        sweep(field_a, field_b, low, high, 1)
    sweep(field_a, field_b, 0, ex, 1, "rim")
    wait_halo(range(4), halo_sem.at[4])
    finish_relay()
    coarse_wait()

    coarse_rows = -(-(count_y + 1) // 8) * 8
    lane_c = lax.broadcasted_iota(jnp.int32, (coarse_rows, LANES), 1)
    row_c = lax.broadcasted_iota(jnp.int32, (coarse_rows, LANES), 0)
    at_z = me[2] * cz - reach * cz + lane_c
    valid = (
        (row_c < count_y) & (at_z >= 0) & (at_z < cz * count_z) & (lane_c < window * cz)
    )
    slab = [[None] * 4 for _ in range(count_x)]
    for x in range(count_x):
        for c in range(4):
            value = None
            for w in range(window):
                column = jnp.concatenate(
                    [coarse_recv[w, x * count_y + y, c : c + 1] for y in range(count_y)]
                    + [jnp.zeros((coarse_rows - count_y, LANES), jnp.float32)],
                    axis=0,
                )
                value = column if value is None else jnp.where(lane_c // cz == w, column, value)
            slab[x][c] = jnp.where(valid, value, 0.0)
    mass = BLOCK**3 * MASS_TERM
    factor = [slab[x][3] * (BLOCK**2 / BLOCK**3) for x in range(count_x)]
    relax = [
        jnp.where(valid, RELAXATION / (factor[x] * DIAGONAL + mass), 0.0) for x in range(count_x)
    ]
    nothing = jnp.zeros((coarse_rows, LANES), jnp.float32)
    start_w = [[slab[x][c] * relax[x] for c in range(3)] for x in range(count_x)]
    share_w = [factor[x] * relax[x] for x in range(count_x)]
    w = start_w

    def y_shift(value, step):
        return pltpu.roll(value, step % coarse_rows, 0)

    for repeat in range(COARSE - 1):
        fresh = []
        for x in range(count_x):
            here = w[x]
            above = w[x + 1] if x + 1 < count_x else [nothing] * 3
            below = w[x - 1] if x > 0 else [nothing] * 3
            sum_x = [above[c] + below[c] for c in range(3)]
            diff_x = [above[c] - below[c] for c in range(3)]
            y_up = [y_shift(here[c], -1) for c in range(3)]
            y_down = [y_shift(here[c], 1) for c in range(3)]
            sum_y = [y_up[c] + y_down[c] for c in range(3)]
            diff_y = [y_up[c] - y_down[c] for c in range(3)]
            corner_x = y_shift(diff_x[1], -1) - y_shift(diff_x[1], 1)
            corner_y = y_shift(diff_x[0], -1) - y_shift(diff_x[0], 1)
            tilt = [CROSS * diff_x[2], CROSS * diff_y[2], CROSS * (diff_x[0] + diff_y[1])]
            own = [here[0], here[1], OWN * here[2]]
            sum_z = [turn(own[c] + tilt[c], -1) + turn(own[c] - tilt[c], 1) for c in range(3)]
            beside = [
                OWN * sum_x[0] + sum_y[0] + CROSS * corner_x + sum_z[0],
                sum_x[1] + OWN * sum_y[1] + CROSS * corner_y + sum_z[1],
                sum_x[2] + sum_y[2] + sum_z[2],
            ]
            fresh.append(
                [
                    KEEP * here[c] + start_w[x][c] + share_w[x] * beside[c]
                    for c in range(3)
                ]
            )
        w = fresh

    for x in range(count_x + 2):
        for c in range(3):
            inside = 1 <= x <= count_x
            coarse_w[x, c, pl.ds(0, 8)] = jnp.zeros((8, LANES), jnp.float32)
            coarse_w[x, c, pl.ds(8, coarse_rows)] = w[x - 1][c] if inside else nothing
    stack_w[pl.ds(24, 8)] = zero
    for xc in range(3):
        for c in range(3):
            stack_w[pl.ds(3 * (3 * xc + c), 3)] = coarse_w[me[0] + xc, c, pl.ds(7 + me[1], 3)]
    inner = lax.rem(target_lane, EDGE) < HALO
    first_cell_z, last_cell_z = reach * cz, (reach + 1) * cz - 1
    pick_low = jnp.where(inner, first_cell_z - 1, first_cell_z)
    pick_high = jnp.where(inner, last_cell_z, last_cell_z + 1)
    picks = (
        first_cell_z + target_lane // BLOCK,
        pick_low,
        pick_high,
        jnp.where(target_lane < LANES // 2, pick_low, pick_high),
    )
    widen = jnp.concatenate([(source_lane == pick).astype(jnp.float32) for pick in picks], axis=1)
    wide_all = pick(stack_w[...], widen)

    def drawn(xc, c, k):
        parts = []
        for j in range(3):
            line = 3 * (3 * xc + c) + j
            piece = wide_all[line : line + 1, k * LANES : (k + 1) * LANES]
            parts.append(jnp.broadcast_to(piece, (wide_y, LANES)))
        return jnp.where(row_y < HALO, parts[0], jnp.where(row_y < HALO + ey, parts[1], parts[2]))

    wide = pl.ds(first_y, wide_y)
    for c in range(3):
        for xc in range(3):
            value = drawn(xc, c, 0)
            for plane in range(3):
                spread_w[c, pl.ds((3 * xc + plane) * rows + first_y, wide_y)] = value
        edge_a[c, 0, wide] = drawn(1, c, 1)
        edge_a[c, 1, wide] = drawn(1, c, 2)
        edge_a[c, 2, wide] = jnp.where(upper_x, drawn(2, c, 3), drawn(0, c, 3))
    beside = edge_stage(edge_a, 0)
    for k in range(3):
        share = edge_base[3, k, wide]
        for c in range(3):
            edge_b[c, k, wide] = (
                edge_b[c, k, wide] + KEEP * edge_a[c, k, wide] + share * beside[k][c]
            )
    edge_sweep(edge_b, edge_a, 1)
    edge_stage(edge_a, 2, False)
    for plane, x in ((1, -2), (2, -1), (3, 0), (4, ex // 2), (5, ex - 1), (6, ex), (7, ex + 1)):
        images = neighbours(spread_w, plane, x, 0)
        for c in range(3):
            image_w[c, at(plane)] = images[c]

    def correct(p, carry):
        kind = (
            jnp.int32(1)
            + jnp.int32(p >= HALO - 1)
            + jnp.int32(p >= HALO)
            + jnp.int32(p >= HALO + 1)
            + jnp.int32(p >= HALO + ex - 1)
            + jnp.int32(p >= HALO + ex)
            + jnp.int32(p >= HALO + ex + 1)
        )
        share = base[3, at(p)]
        for c in range(3):
            field_b[c, at(p)] = (
                field_b[c, at(p)] + KEEP * spread_w[c, at(kind)] + share * image_w[c, at(kind)]
            )
        return carry

    by_two(2, wide_x - 2, correct, 0)
    sweep(field_b, field_a, -1, ex + 1, 1)

    def squares(x, carry):
        left = residual(field_a, x, 2)
        for c in range(3):
            out_ref[c, x] = field_a[c, at(x + HALO, 0, True)]
        return carry + fold(sum(value * value for value in left))

    left_sum = by_two(0, ex, squares, zero)
    load_total = jnp.sum(jnp.sum(load_sum, axis=0, keepdims=True), axis=1, keepdims=True)
    left_total = jnp.sum(jnp.sum(left_sum, axis=0, keepdims=True), axis=1, keepdims=True)
    first = lax.broadcasted_iota(jnp.int32, (1, LANES), 1) == 0
    mine = jnp.where(first, load_total, left_total)
    norm_send[...] = mine

    for number in range(greeted, len(rounds)):
        if number > greeted:
            hello(number)
        hear(number)
    for x in reversed(ring_x):
        for z in reversed(ring_z):
            for y in reversed(ring_y):
                if x is not me[0] or y is not me[1] or z is not me[2]:
                    pltpu.make_async_remote_copy(
                        src_ref=norm_send,
                        dst_ref=norm_recv.at[my_id],
                        send_sem=norm_sem.at[0],
                        recv_sem=norm_sem.at[1],
                        device_id=(x, y, z),
                        device_id_type=MESH,
                    ).start()
    norm_recv[my_id] = mine
    others = norm_recv.at[pl.ds(0, total - 1)]
    for k in range(2):
        pltpu.make_async_copy(others, others, norm_sem.at[k]).wait()
    summed = jnp.sum(norm_recv[...], axis=0)
    nodes = 3 * ex * ey * ez * total
    norms_ref[...] = jnp.sqrt(summed / nodes)


def on_device(counts, right_side, damage):
    _, ex, ey, ez = right_side.shape
    assert ez == LANES and ex * EDGE == LANES and 2 * EDGE * EDGE == LANES
    assert ex % BLOCK == 0 and ey == BLOCK and ex == BLOCK
    cz = ez // BLOCK
    wide_x = ex + 2 * HALO
    rows = ey + 2 * YPAD
    flat = wide_x * rows
    total = counts[0] * counts[1] * counts[2]
    window = 2 * (-(-COARSE // cz)) + 1
    coarse_rows = -(-(counts[1] + 1) // 8) * 8
    rounds = 0
    while window // 2 << rounds < counts[2] - 1:
        rounds += 1
    f32 = jnp.float32

    def vmem(*shape):
        return pltpu.VMEM(shape + (LANES,), f32)

    dma = pltpu.SemaphoreType.DMA
    near, layers = len(NEAR), len(LAYERS)
    displacement, norms = pl.pallas_call(
        functools.partial(kernel, counts, (ex, ey, ez)),
        out_shape=(
            pltpu.VMEM(right_side.shape, f32),
            pltpu.VMEM((1, LANES), f32),
        ),
        in_specs=[pl.BlockSpec(memory_space=pl.ANY)] * 2,
        out_specs=(
            pl.BlockSpec(memory_space=pltpu.VMEM),
            pl.BlockSpec(memory_space=pltpu.VMEM),
        ),
        scratch_shapes=[
            vmem(3, ex, ey),
            vmem(ex * ey),
            pltpu.VMEM((ex, ey, LANES), jnp.int32),
            vmem(4, flat),
            vmem(3, flat),
            vmem(3, flat),
            vmem(4, 3, rows),
            vmem(3, 3, rows),
            vmem(3, 3, rows),
            vmem(3, 3, 2 * rows),
            vmem(4, 3, rows),
            vmem(len(FAR), ex),
            vmem(2, layers, ex),
            vmem(2, layers, ex),
            vmem(2, 2, near, 2),
            vmem(2, 2, near, 2),
            vmem(2, 2, layers, HALO),
            vmem(2, 2, layers, HALO),
            vmem(3, 4, rows),
            vmem(2, ey),
            vmem(2, 3, rows),
            vmem(2, 2, 4, 2),
            vmem(2, 2, 3, 4, 2),
            vmem(2, 2, 2, 2),
            vmem(2, 2, 2, 3, 2),
            vmem(4),
            vmem(window, counts[0] * counts[1], 4),
            vmem(counts[0] + 2, 3, 8 + coarse_rows),
            vmem(32),
            vmem(3, 9 * rows),
            vmem(3, 9 * rows),
            vmem(1),
            vmem(total, 1),
            vmem(4 * EDGE * LANES, 1),
            dma((2,)),
            dma((7,)),
            dma((2,)),
            dma((2,)),
            pltpu.SemaphoreType.REGULAR((max(1, rounds), 2)),
        ],
        compiler_params=pltpu.CompilerParams(collective_id=0, has_side_effects=True),
    )(right_side, damage)
    return displacement, norms[0, :2]


def solution(mesh):
    counts = tuple(mesh.shape[axis] for axis in AXES)
    placed = (P(None, "gx", "gy", "gz"), P("gx", "gy", "gz"))
    return jax.shard_map(
        functools.partial(on_device, counts),
        mesh=mesh,
        in_specs=placed,
        out_specs=(P(None, "gx", "gy", "gz"), P()),
        check_vma=False,
    )
```
